128 devices in a mesh: tp: 2 (over core), dp: 64 (over z, y, x).
Axes of the slice: x: 4, y: 4, z: 4, core: 2. Of those that a mesh axis runs over, the one named last changes fastest.
Arguments:
- token_ids: int32 [1024, 512], P('dp')
- embed_table: bfloat16 [50304, 512], P('tp')
- ln1_gain: bfloat16 [512], replicated
- ln1_bias: bfloat16 [512], replicated
- ln2_gain: bfloat16 [512], replicated
- ln2_bias: bfloat16 [512], replicated
- w_qkv: bfloat16 [512, 8, 3, 64], P(None, 'tp')
- b_qkv: bfloat16 [8, 3, 64], P('tp')
- w_dense: bfloat16 [8, 64, 512], P('tp')
- b_dense: bfloat16 [512], replicated
- w_fc1: bfloat16 [512, 2048], P(None, 'tp')
- b_fc1: bfloat16 [2048], P('tp')
- w_fc2: bfloat16 [2048, 512], P('tp')
- b_fc2: bfloat16 [512], replicated
- cotangent: bfloat16 [1024, 512, 512], P('dp')
Outputs:
- output 1: bfloat16 [1024, 512, 512], P('dp')
- output 2: float32 [50304, 512], P('tp', 'dp')
- output 3: float32 [512], P('dp')
- output 4: float32 [512], P('dp')
- output 5: float32 [512], P('dp')
- output 6: float32 [512], P('dp')
- output 7: float32 [512, 8, 3, 64], P('dp', 'tp')
- output 8: float32 [1536], P(('tp', 'dp'))
- output 9: float32 [8, 64, 512], P('tp', None, 'dp')
- output 10: float32 [512], P('dp')
- output 11: float32 [512, 2048], P('dp', 'tp')
- output 12: float32 [2048], P(('tp', 'dp'))
- output 13: float32 [2048, 512], P('tp', 'dp')
- output 14: float32 [512], P('dp')
All inputs are finite; a program needn't handle non-finite values.
Results may differ from the reference program's by a relative error of at most 0.00955545.
Values sent between devices are 32-bit elements.
A program may use at most 1 GiB of HBM per device.

```python
import jax
import jax.numpy as jnp
from jax import lax

VOCAB_SIZE = 50304
D_MODEL = 512
N_HEADS = 8
HEAD_DIM = 64
FF_DIM = 2048
SEQ_LEN = 512
BATCH_SEQS = 1024
ROT_DIM = HEAD_DIM // 4
EPS_NORM = 1e-5
ROPE_BASE = 10000.0


def setup_inputs(seed: int = 0) -> dict:
    key_list = jax.random.split(jax.random.key(seed), 16)
    base_ids = jax.random.randint(key_list[0], (BATCH_SEQS, SEQ_LEN), 0, VOCAB_SIZE, dtype=jnp.int32)
    shifts = jax.random.randint(key_list[1], (BATCH_SEQS, SEQ_LEN), 0, 8, dtype=jnp.int32)
    token_ids = jnp.right_shift(base_ids, shifts)
    token_ids = token_ids.at[0, 0].set(VOCAB_SIZE - 1).at[0, 1].set(0)
    d_scale = D_MODEL ** -0.5
    f_scale = FF_DIM ** -0.5

    def draw_normal(key_index, arr_shape, spread, offset):
        sample = jax.random.normal(key_list[key_index], arr_shape, jnp.float32) * spread + offset
        return sample.astype(jnp.bfloat16)

    return {
        'token_ids': token_ids,
        'embed_table': draw_normal(2, (VOCAB_SIZE, D_MODEL), 1.0, 0.0),
        'ln1_gain': draw_normal(3, (D_MODEL,), 0.6, 1.0),
        'ln1_bias': draw_normal(4, (D_MODEL,), 0.5, 0.0),
        'ln2_gain': draw_normal(5, (D_MODEL,), 0.6, 1.0),
        'ln2_bias': draw_normal(6, (D_MODEL,), 0.5, 0.0),
        'w_qkv': draw_normal(7, (D_MODEL, N_HEADS, 3, HEAD_DIM), d_scale, 0.0),
        'b_qkv': draw_normal(8, (N_HEADS, 3, HEAD_DIM), 0.5, 0.0),
        'w_dense': draw_normal(9, (N_HEADS, HEAD_DIM, D_MODEL), d_scale, 0.0),
        'b_dense': draw_normal(10, (D_MODEL,), 1.0, 0.0),
        'w_fc1': draw_normal(11, (D_MODEL, FF_DIM), d_scale, 0.0),
        'b_fc1': draw_normal(12, (FF_DIM,), 0.5, 0.0),
        'w_fc2': draw_normal(13, (FF_DIM, D_MODEL), f_scale, 0.0),
        'b_fc2': draw_normal(14, (D_MODEL,), 1.0, 0.0),
        'cotangent': draw_normal(15, (BATCH_SEQS, SEQ_LEN, D_MODEL), 1.0, 0.0),
    }


def to_bf16(tensor):
    return tensor.astype(jnp.bfloat16).astype(jnp.float32)


def rope_tables():
    half_rot = ROT_DIM // 2
    inv_freq = ROPE_BASE ** (-(jnp.arange(half_rot, dtype=jnp.float32) * 2.0) / ROT_DIM)
    angles = jnp.arange(SEQ_LEN, dtype=jnp.float32)[:, None] * inv_freq[None, :]
    angles = jnp.concatenate([angles, angles], axis=-1)
    return jnp.cos(angles)[:, None, :], jnp.sin(angles)[:, None, :]


def apply_rope(tensor, cos_table, sin_table):
    half_rot = ROT_DIM // 2
    rot_part = tensor[..., :ROT_DIM]
    turned = jnp.concatenate([-rot_part[..., half_rot:], rot_part[..., :half_rot]], axis=-1)
    return jnp.concatenate([rot_part * cos_table + turned * sin_table, tensor[..., ROT_DIM:]], axis=-1)


def layer_seq(x_seq, params):
    (ln1_gain, ln1_bias, ln2_gain, ln2_bias, w_qkv, b_qkv, w_dense, b_dense, w_fc1, b_fc1, w_fc2, b_fc2) = params
    mean_x = jnp.mean(x_seq, axis=-1, keepdims=True)
    centered = x_seq - mean_x
    normed = centered * lax.rsqrt(jnp.mean(centered * centered, axis=-1, keepdims=True) + EPS_NORM)
    hid_attn = to_bf16(normed * ln1_gain + ln1_bias)
    hid_mlp = to_bf16(normed * ln2_gain + ln2_bias)
    qkv_all = to_bf16(jnp.einsum('sd,dhjc->shjc', hid_attn, w_qkv) + b_qkv)
    cos_table, sin_table = rope_tables()
    queries = to_bf16(apply_rope(qkv_all[:, :, 0], cos_table, sin_table))
    keys_rot = to_bf16(apply_rope(qkv_all[:, :, 1], cos_table, sin_table))
    values = qkv_all[:, :, 2]
    scores = jnp.einsum('qhc,khc->hqk', queries, keys_rot) * HEAD_DIM ** -0.5
    causal = jnp.arange(SEQ_LEN)[:, None] >= jnp.arange(SEQ_LEN)[None, :]
    probs_low = to_bf16(jax.nn.softmax(jnp.where(causal[None], scores, -1e30), axis=-1))
    context = to_bf16(jnp.einsum('hqk,khc->qhc', probs_low, values))
    attn_out = jnp.einsum('qhc,hcd->qd', context, w_dense) + b_dense
    pre_act = to_bf16(jnp.dot(hid_mlp, w_fc1, preferred_element_type=jnp.float32) + b_fc1)
    gelu_out = to_bf16(jax.nn.gelu(pre_act, approximate=False))
    mlp_out = jnp.dot(gelu_out, w_fc2, preferred_element_type=jnp.float32) + b_fc2
    return to_bf16(x_seq + attn_out + mlp_out)


def reference(token_ids, embed_table, ln1_gain, ln1_bias, ln2_gain, ln2_bias, w_qkv, b_qkv, w_dense, b_dense, w_fc1, b_fc1, w_fc2, b_fc2, cotangent):
    params = tuple(item.astype(jnp.float32) for item in (ln1_gain, ln1_bias, ln2_gain, ln2_bias, w_qkv, b_qkv, w_dense, b_dense, w_fc1, b_fc1, w_fc2, b_fc2))
    tokens = jnp.take(embed_table, token_ids, axis=0)
    zero_grads = tuple(jnp.zeros_like(item) for item in params)
    zero_embed = jnp.zeros((VOCAB_SIZE, D_MODEL), jnp.float32)

    def scan_step(carry, inputs):
        grad_acc, embed_acc = carry
        tok_seq, ids_seq, cot_seq = inputs
        out_seq, vjp_pull = jax.vjp(layer_seq, tok_seq.astype(jnp.float32), params)
        grad_x, grad_params = vjp_pull(cot_seq.astype(jnp.float32))
        grad_acc = tuple(acc_item + new_item for acc_item, new_item in zip(grad_acc, grad_params))
        embed_acc = embed_acc.at[ids_seq].add(grad_x)
        return (grad_acc, embed_acc), out_seq.astype(jnp.bfloat16)

    (grads, d_embed), layer_out = lax.scan(scan_step, (zero_grads, zero_embed), (tokens, token_ids, cotangent))
    (d_ln1_gain, d_ln1_bias, d_ln2_gain, d_ln2_bias, d_w_qkv, d_b_qkv, d_w_dense, d_b_dense, d_w_fc1, d_b_fc1, d_w_fc2, d_b_fc2) = grads
    return (layer_out, d_embed, d_ln1_gain, d_ln1_bias, d_ln2_gain, d_ln2_bias, d_w_qkv, d_b_qkv.reshape(-1), d_w_dense, d_b_dense, d_w_fc1, d_b_fc1, d_w_fc2, d_b_fc2)
```

```python
import functools
import math
import jax
import jax.numpy as jnp
from jax import lax
from jax.experimental import pallas as pl
from jax.experimental.pallas import tpu as pltpu
from jax.sharding import PartitionSpec as P

F32, BF16 = jnp.float32, jnp.bfloat16
NN = (((1,), (0,)), ((), ()))
NT = (((1,), (1,)), ((), ()))
TN = (((0,), (0,)), ((), ()))
S, D, FF, HEADS, HD = 512, 512, 2048, 8, 64
PAIR, HALF, PAIRS, FF_STEPS, ROT_HALF = 2 * HD, S // 2, HEADS // 2, FF // S, HD // 8
EPS, ROPE_BASE = 1e-5, 10000.0
LOG2E = 1.4426950408889634
SQRT_HALF, INV_SQRT_2PI = 0.7071067811865476, 0.3989422804014327
ERF_P = 0.35
ERF_C = (0.19746628636396, 0.19745311511580, 0.18590938935029, 0.15467161331132, 0.16294620242859,
         -0.014553608641014, 0.20121223107286, -0.085106053125625)
RB = 64
VMEM_LIMIT = 67_000_000
ROW, LANES, RING = 8, 128, 4
PAD = 25600
COLOR = PAD // 2
WIDE, EXTRA = 3072, 128
GCOLS = WIDE + EXTRA
MESH = pl.DeviceIdType.MESH
CHUNKS = (5, 3)


def dot(a, b, dims=NN):
    return lax.dot_general(a, b, dims, preferred_element_type=F32)


def rnd(v):
    return v.astype(BF16).astype(F32)


def gelu_parts(a):
    t = 1.0 / (1.0 + (ERF_P * SQRT_HALF) * jnp.abs(a))
    r = 0.5 * ERF_C[-1]
    for c in ERF_C[-2::-1]:
        r = r * t + 0.5 * c
    e = jnp.exp2(a * a * (-0.5 * LOG2E))
    q = r * t * e
    phi = jnp.where(a < 0, q, 1.0 - q)
    return a * phi, phi + a * e * INV_SQRT_2PI


def block(i, n):
    return slice(i * n, i * n + n)


def row_sums(v):
    return jnp.sum(v.reshape(RB // ROW, ROW, v.shape[-1]), axis=0)


def row_loop(body):
    @pl.loop(0, S // RB)
    def _(i):
        body(pl.ds(pl.multiple_of(i * RB, RB), RB))


def wcol(half, part, width):
    return slice(half * WIDE + part, half * WIDE + part + width)


def layer_kernel(carry, z_ref, xo_ref, xp_ref, cot_ref, vec_ref, bqkv_ref, bfc1_ref, rope_ref,
                 qo_ref, do_ref, fo_ref, to_ref, rp_ref, fp_ref, *refs):
    carried, refs = refs[:carry], refs[carry:]
    out_ref, gx_refs, (gw_ref, gs_ref, gb1_ref), refs = refs[0], refs[1:1 + RING], refs[1 + RING:RING + RING], refs[RING + RING:]
    (wqkv, wd, w1, w2, n_scr, inv_scr, x_scr, acc_scr, dh2_scr, a_scr, g_scr, h1_scr, h2_scr, h1t_scr, h2t_scr, cott_scr,
     dctx_scr, ctx_scr, u_scr, da_scr, qkv_scr, dqkv_scr) = refs

    @pl.when(pl.program_id(0) == 0)
    def _():
        if carried:
            for src, dst in zip(carried, (gw_ref, gs_ref, gb1_ref)):
                pltpu.sync_copy(src, dst)
        else:
            for dst in (gw_ref, gs_ref, gb1_ref):
                dst[...] = jnp.zeros_like(dst)
        for j in range(3):
            wqkv[block(2 * j, HALF), :] = qo_ref[block(j, HALF), :]
            wqkv[block(2 * j + 1, HALF), :] = rp_ref[block(j, HALF), :].astype(BF16)
        wd[:HALF, :] = do_ref[...]
        wd[HALF:, :] = rp_ref[block(3, HALF), :].astype(BF16)
        n = FF // 2
        w2[:n, :] = to_ref[...]
        w2[n:, :] = rp_ref[2 * S:, :].astype(BF16)
        w1[:, :n] = fo_ref[...]
        w1[:, n:] = fp_ref[...].astype(BF16)

    cot = cot_ref[0]
    g1, b1, g2, b2, bo = (vec_ref[i:i + 1, :] for i in range(5))

    def norm(rows):
        x = xo_ref[0, rows, :].astype(F32) + xp_ref[0, rows, :]
        x_scr[rows, :] = x
        cen = x - jnp.mean(x, axis=-1, keepdims=True)
        inv = lax.rsqrt(jnp.mean(cen * cen, axis=-1, keepdims=True) + EPS)
        n = cen * inv
        n_scr[rows, :] = n
        inv_scr[rows, :] = inv
        h1_scr[rows, :] = (n * g1 + b1).astype(BF16)
        h2_scr[rows, :] = (n * g2 + b2).astype(BF16)
        gs_ref[4] += row_sums(cot_ref[0, rows, :].astype(F32))
    row_loop(norm)

    h1t_scr[...] = h1_scr[...].T
    h2t_scr[...] = h2_scr[...].T
    cott_scr[...] = cot.T

    h1 = h1_scr[...]
    for p in range(PAIRS):
        for j in range(3):
            v = dot(h1, wqkv[block(j * PAIRS + p, PAIR), :], NT) + bqkv_ref[j:j + 1, block(p, PAIR)]
            v = v.astype(BF16)
            if j < 2:
                v = v.astype(F32)
                v = (v * rope_ref[0] + pltpu.roll(v, PAIR - ROT_HALF, 1) * rope_ref[1]
                     + pltpu.roll(v, ROT_HALF, 1) * rope_ref[2]).astype(BF16)
            qkv_scr[j, :, block(p, PAIR)] = v
    dctx_scr[...] = dot(cot, wd[...], NT).astype(BF16)

    lane = lax.broadcasted_iota(jnp.int32, (S, PAIR), 1)
    causal = lax.broadcasted_iota(jnp.int32, (HALF, HALF), 0) >= lax.broadcasted_iota(jnp.int32, (HALF, HALF), 1)
    zero = jnp.zeros((S, PAIR), BF16)

    def plus(lst, i, v):
        lst[i] = v if i not in lst else lst[i] + v

    for p in range(PAIRS):
        cs = block(p, PAIR)
        qp, kp, vp = (qkv_scr[j, :, cs] for j in range(3))
        dcp = dctx_scr[:, cs]
        ctx, dq, dk, dv = {}, {}, {}, {}
        for mine in (lane < HD, lane >= HD):
            qm, km, vm, dcm = (jnp.where(mine, w, zero) for w in (qp, kp, vp, dcp))
            for qb in range(2):
                kl = HALF * (qb + 1)
                qs = block(qb, HALF)
                s = dot(qm[qs], kp[:kl], NT)
                diag = jnp.where(causal, s[:, kl - HALF:], -1e30)
                s = jnp.concatenate([s[:, :HALF], diag], axis=1) if qb else diag
                e = jnp.exp2((s - jnp.max(s, axis=-1, keepdims=True)) * (HD ** -0.5 * LOG2E))
                pr = e * (1.0 / jnp.sum(e, axis=-1, keepdims=True))
                pb = pr.astype(BF16)
                plus(ctx, qb, dot(pb, vm[:kl]))
                dp = rnd(dot(dcm[qs], vp[:kl], NT))
                ds = (pr * (dp - jnp.sum(pr * dp, axis=-1, keepdims=True))).astype(BF16)
                plus(dq, qb, dot(ds, km[:kl]))
                dkb = dot(ds, qm[qs], TN)
                dvb = dot(pb, dcm[qs], TN)
                for kb in range(qb + 1):
                    plus(dk, kb, dkb[block(kb, HALF)])
                    plus(dv, kb, dvb[block(kb, HALF)])
        for b in range(2):
            bs = block(b, HALF)
            ctx_scr[bs, cs] = ctx[b].astype(BF16)
            for j, g in enumerate((dq[b], dk[b])):
                g = rnd(g * HD ** -0.5)
                spun = g * rope_ref[3, bs]
                dqkv_scr[j, bs, cs] = (g * rope_ref[0, bs] + pltpu.roll(spun, PAIR - ROT_HALF, 1) * rope_ref[4, bs]
                                       + pltpu.roll(spun, ROT_HALF, 1) * rope_ref[5, bs]).astype(BF16)
            dqkv_scr[2, bs, cs] = dv[b].astype(BF16)

    acc_scr[...] = dot(ctx_scr[...], wd[...])
    dh2_scr[...] = jnp.zeros_like(dh2_scr)
    h2 = h2_scr[...]
    for c in range(FF_STEPS):
        cs = block(c, S)
        a_scr[...] = dot(h2, w1[:, cs]) + bfc1_ref[:, cs]
        g_scr[...] = dot(cot, w2[cs, :], NT)

        def act(rows, cs=cs):
            u, gp = gelu_parts(rnd(a_scr[rows, :]))
            da = (rnd(g_scr[rows, :]) * gp).astype(BF16)
            u_scr[rows, :] = u.astype(BF16)
            da_scr[rows, :] = da
            gb1_ref[:, cs] += row_sums(da.astype(F32))
        row_loop(act)

        u, da = u_scr[...], da_scr[...]
        acc_scr[...] += dot(u, w2[cs, :])
        dh2_scr[...] += dot(da, w1[:, cs], NT)
        half, part = c // 2, 2 * S + c % 2 * S
        gw_ref[:, wcol(half, part, S)] += dot(h2t_scr[...], da)
        gw_ref[:, wcol(half, part + 2 * S, S)] += dot(cott_scr[...], u)

    for half in range(2):
        hs = block(half, HALF)
        for j in range(3):
            gw_ref[:, wcol(half, j * HALF, HALF)] += dot(h1t_scr[...], dqkv_scr[j, :, hs])
        gw_ref[:, wcol(half, 3 * HALF, HALF)] += dot(cott_scr[...], ctx_scr[:, hs])
    a_scr[...] = sum(dot(dqkv_scr[j], wqkv[block(j, S), :]) for j in range(3))
    z = z_ref[0]

    def back(rows):
        n = n_scr[rows, :]
        d1, d2 = rnd(a_scr[rows, :]), rnd(dh2_scr[rows, :])
        for i, v in zip((0, 1, 2, 3, 5, 6, 7), (d1 * n, d1, d2 * n, d2, *(dqkv_scr[j, rows, :].astype(F32) for j in range(3)))):
            gs_ref[i] += row_sums(v)
        gn = d1 * g1 + d2 * g2
        g_scr[rows, :] = cot_ref[0, rows, :].astype(F32) + inv_scr[rows, :] * (
            gn - jnp.mean(gn, axis=-1, keepdims=True) - n * jnp.mean(gn * n, axis=-1, keepdims=True))
        for k, ref in enumerate(gx_refs):
            ref[rows, :] = g_scr[rows, pl.ds(pl.multiple_of((z + k) % RING * LANES, LANES), LANES)]
        out_ref[0, rows, :] = rnd(x_scr[rows, :] + (acc_scr[rows, :] + bo))
    row_loop(back)


def rope_consts():
    inv_freq = ROPE_BASE ** (-jnp.arange(ROT_HALF, dtype=F32) / ROT_HALF)
    ang = jnp.arange(S, dtype=F32)[:, None] * inv_freq[None, :]
    cos, sin = jnp.cos(ang), jnp.sin(ang)
    one, zero = jnp.ones_like(cos), jnp.zeros_like(cos)
    keep, none = jnp.ones((S, HD - 2 * ROT_HALF), F32), jnp.zeros((S, HD - 2 * ROT_HALF), F32)
    parts = ((cos, cos, keep), (-sin, zero, none), (zero, sin, none), (sin, sin, none), (one, zero, none), (zero, -one, none))
    return jnp.stack([jnp.concatenate(p + p, axis=1) for p in parts])


def layer_call(first, count, carried, z, *args):
    vm, hbm = pl.BlockSpec(memory_space=pltpu.VMEM), pl.BlockSpec(memory_space=pl.ANY)
    seq = pl.BlockSpec((1, S, D), lambda i, _: (i + first, 0, 0))
    table, low = pltpu.VMEM((S, D), F32), pltpu.VMEM((S, D), BF16)
    return pl.pallas_call(
        functools.partial(layer_kernel, len(carried)),
        grid_spec=pltpu.PrefetchScalarGridSpec(
            num_scalar_prefetch=1, grid=(count,),
            in_specs=[seq] * 3 + [vm] * (len(args) - 3) + [hbm] * len(carried),
            out_specs=[pl.BlockSpec((1, S, D), lambda i, _: (i, 0, 0))] + [pl.BlockSpec((S, LANES), lambda i, _: (i, 0))] * RING + [vm] * 3,
            scratch_shapes=[pltpu.VMEM((3 * S, D), BF16), low, pltpu.VMEM((D, FF), BF16), pltpu.VMEM((FF, D), BF16), table,
                            pltpu.VMEM((S, 1), F32)] + [table] * 5 + [low] * 9 + [pltpu.VMEM((3, S, D), BF16)] * 2),
        out_shape=[jax.ShapeDtypeStruct((count, S, D), F32)] + [jax.ShapeDtypeStruct((count * S, LANES), F32)] * RING
        + [jax.ShapeDtypeStruct((D, 2 * WIDE), F32), jax.ShapeDtypeStruct((ROW, ROW, D), F32), jax.ShapeDtypeStruct((ROW, FF), F32)],
        compiler_params=pltpu.CompilerParams(dimension_semantics=("arbitrary",), vmem_limit_bytes=VMEM_LIMIT),
        cost_estimate=pl.CostEstimate(flops=count * 30_000_000_000, bytes_accessed=60_000_000, transcendentals=0),
        name="layer",
    )(z, *args, *carried)


def merge_kernel(firsts, half, core_ref, *refs):
    i = pl.program_id(0)
    for src, (own, first, count) in zip(refs[:-1], firsts):
        at = i - first - half * jnp.where(own, core_ref[0], 1 - core_ref[0])

        @pl.when((at >= 0) & (at < count))
        def _():
            refs[-1][...] = src[...].astype(BF16)


def merge_call(core, owns, others):
    counts = [v.shape[0] for v in owns]
    half = sum(counts)
    firsts = [(own, sum(counts[:j]), n) for own in (True, False) for j, n in enumerate(counts)]

    def spec(own, first, count):
        return pl.BlockSpec((1, S, D), lambda i, c: (
            jnp.clip(i - first - half * (c[0] if own else 1 - c[0]), 0, count - 1), 0, 0))
    return pl.pallas_call(
        functools.partial(merge_kernel, firsts, half),
        grid_spec=pltpu.PrefetchScalarGridSpec(
            num_scalar_prefetch=1, grid=(2 * half,), in_specs=[spec(*f) for f in firsts],
            out_specs=pl.BlockSpec((1, S, D), lambda i, c: (i, 0, 0))),
        out_shape=jax.ShapeDtypeStruct((2 * half, S, D), BF16),
        name="merge",
    )(core.reshape(1).astype(jnp.int32), *owns, *others)


STEPS, UNROLL = 8, 8
STEP = PAD // STEPS


def table_kernel(half, ids_ref, *refs):
    rows, (out_ref, acc, acc2, stage, sem) = refs[:-5], refs[-5:]

    @pl.loop(0, acc.shape[0] // LANES)
    def _(j):
        for a in (acc, acc2):
            a[pl.ds(pl.multiple_of(j * LANES, LANES), LANES), :] = jnp.zeros((LANES, LANES), F32)
    start = 0
    for even, odd in zip(rows[::2], rows[1::2]):
        count = even.shape[0]

        @pl.loop(0, count // UNROLL)
        def _(g, start=start, count=count, even=even, odd=odd):
            t0 = pl.multiple_of(g * UNROLL, UNROLL)
            for j in range(UNROLL):
                for a, src, base in ((acc, even, start), (acc2, odd, start + count)):
                    row = pl.ds(ids_ref[base + t0 + j], 1)
                    a[row, :] += src[pl.ds(t0 + j, 1), :]
        start += 2 * count
    copies = []
    for i in range(2 * STEPS):
        h, c, slot = i // STEPS, i % STEPS, i % 2
        if i > 1:
            copies[i - 2].wait()

        @pl.loop(0, STEP // LANES, unroll=5)
        def _(b):
            at = pl.ds(pl.multiple_of(h * half + c * STEP + b * LANES, ROW), LANES)
            stage[slot, :, pl.ds(pl.multiple_of(b * LANES, LANES), LANES)] = (acc[at, :] + acc2[at, :]).T
        copies.append(pltpu.make_async_copy(stage.at[slot], out_ref.at[h, :, pl.ds(c * STEP, STEP)], sem.at[slot]))
        copies[i].start()
    for c in copies[-2:]:
        c.wait()


def table_call(ids, rows, half):
    return pl.pallas_call(
        functools.partial(table_kernel, half),
        grid_spec=pltpu.PrefetchScalarGridSpec(
            num_scalar_prefetch=1, grid=(), in_specs=[pl.BlockSpec(memory_space=pltpu.VMEM)] * len(rows),
            out_specs=pl.BlockSpec(memory_space=pl.ANY),
            scratch_shapes=[pltpu.VMEM((half + PAD, LANES), F32)] * 2 + [pltpu.VMEM((2, LANES, STEP), F32), pltpu.SemaphoreType.DMA((2,))]),
        out_shape=jax.ShapeDtypeStruct((2, LANES, PAD), F32),
        compiler_params=pltpu.CompilerParams(vmem_limit_bytes=VMEM_LIMIT),
        cost_estimate=pl.CostEstimate(flops=4_000_000_000, bytes_accessed=34_000_000, transcendentals=0),
        name="table",
    )(ids, *rows)


def cut(lo, n):
    first = n // (2 * LANES) * LANES
    return (lo, first), (lo + first, n - first)


def over(lead, body, at=()):
    if not lead:
        return body(at)

    @pl.loop(0, lead[0])
    def _(i):
        over(lead[1:], body, at + (i,))


def add_into(dst, srcs, lead, lo, n):
    def body(at):
        v = dst[at + (slice(None), pl.ds(lo, n))]
        for s in srcs:
            v = v + s[at + (slice(None), pl.ds(0, n))]
        dst[at + (slice(None), pl.ds(lo, n))] = v
    over(lead, body)


def tail_kernel(t_ref, g_ref, e_ref, oute_ref, outw_ref, *scratch):
    tsum, tpeer, gsum, gpeer, send, recv, local = scratch[:7]
    bufs = list(scratch[7:])
    core, dp = lax.axis_index('tp'), lax.axis_index('dp')
    pos = {'z': dp // (RING * RING), 'y': dp // RING % RING, 'x': dp % RING}
    stride = {'z': RING * RING, 'y': RING, 'x': 1}

    def shift(axis, k):
        return (pos[axis] + k) % RING

    def device(axis, k):
        return (core, dp + (shift(axis, k) - pos[axis]) * stride[axis])
    peer = (1 - core, dp)

    barrier = pltpu.get_barrier_semaphore()
    near = [peer] + [device(axis, k) for axis in 'zyx' for k in (1, RING - 1)]
    for who in near:
        pl.semaphore_signal(barrier, inc=1, device_id=who, device_id_type=MESH)
    pl.semaphore_wait(barrier, len(near))

    used = [0, 0]

    def remote(src, dst, who):
        i = used[0]
        used[0] += 1
        c = pltpu.make_async_remote_copy(src, dst, send.at[i], recv.at[i], device_id=who, device_id_type=MESH)
        c.start()
        return c

    def load(src, dst):
        i = used[1]
        used[1] += 1
        c = pltpu.make_async_copy(src, dst, local.at[i])
        c.start()
        return c
    sent = []

    full = pl.ds(0, COLOR)
    rest = pl.ds(COLOR, COLOR)
    wide, extra, far = pl.ds(0, WIDE), pl.ds(WIDE, EXTRA), pl.ds(WIDE, WIDE)
    every = slice(None)
    views = {
        'a': ('y', lambda i: (i, every, every, full)),
        'b': ('x', lambda i: (every, i, every, rest)),
        'g': ('z', lambda i: (i, every, every, every, wide)),
    }
    pend = {}
    pend['e'] = [remote(e_ref.at[1], gpeer.at[every, every, every, every, extra], peer),
                 load(e_ref.at[0], gsum.at[every, every, every, every, extra])]
    for k in (2, 1, RING - 1, 0):
        for name, (axis, view) in views.items():
            at = view(shift(axis, k))
            if name == 'g':
                there = at[:-1] + (far,)
                pend[name, k] = [remote(g_ref.at[there], gpeer.at[at], peer), load(g_ref.at[at], gsum.at[at])]
            else:
                pend[name, k] = [remote(t_ref.at[(1,) + at], tpeer.at[at], peer), load(t_ref.at[(0,) + at], tsum.at[at])]

    def arrive(key):
        out, here = pend[key]
        sent.append(out)
        out.wait_recv()
        here.wait()

    def ready(name, k):
        arrive((name, k))
        axis, _ = views[name]
        i = shift(axis, k)
        if name == 'a':
            add_into(tsum.at[i], [tpeer.at[i]], (RING,), 0, COLOR)
        elif name == 'b':
            add_into(tsum.at[:, i, :, rest], [tpeer.at[:, i, :, rest]], (RING,), 0, COLOR)
        else:
            add_into(gsum.at[i], [gpeer.at[i]], (RING, RING), 0, GCOLS)

    class Stage:
        def __init__(self, axis, piece, lead, lo, n, need=None):
            self.axis, self.piece, self.lead, self.lo, self.n, self.need = axis, piece, lead, lo, n, need
            self.halves = cut(lo, n)
            self.near = [bufs.pop(0), bufs.pop(0)]
            self.last = [bufs.pop(0), bufs.pop(0)]

        def view(self, k, lo, n):
            return self.piece(shift(self.axis, k)).at[(every,) * (len(self.lead) + 1) + (pl.ds(lo, n),)]

        def want(self, k):
            if self.need:
                ready(self.need, k)

        def first(self):
            self.want(2)
            self.c1 = [remote(self.view(2, *self.halves[s]), self.near[s], device(self.axis, k))
                       for s, k in enumerate((1, RING - 1))]

        def second(self):
            self.want(1)
            self.want(RING - 1)
            self.c2 = []
            for s, k in enumerate((1, RING - 1)):
                self.c1[s].wait_recv()
                add_into(self.piece(shift(self.axis, k)), [self.near[s]], self.lead, *self.halves[s])
                self.c2.append(remote(self.view(k, self.lo, self.n), self.last[s], device(self.axis, k)))

        def finish(self):
            self.want(0)
            for c in self.c2:
                c.wait_recv()
            add_into(self.piece(shift(self.axis, 0)), self.last, self.lead, self.lo, self.n)
            sent.extend(self.c1 + self.c2)

    py, px, pz = pos['y'], pos['x'], pos['z']
    one, two = (RING,), (RING, RING)
    a1 = Stage('y', lambda i: tsum.at[i], one, 0, COLOR, 'a')
    b1 = Stage('x', lambda i: tsum.at[:, i], one, COLOR, COLOR, 'b')
    g1 = Stage('z', lambda i: gsum.at[i], two, 0, GCOLS, 'g')
    a2 = Stage('x', lambda i: tsum.at[py, i], (), 0, COLOR)
    b2 = Stage('y', lambda i: tsum.at[i, px], (), COLOR, COLOR)
    (c0, cn), (d0, dn) = cut(0, GCOLS)
    c1 = Stage('y', lambda i: gsum.at[pz, i], one, c0, cn)
    d1 = Stage('x', lambda i: gsum.at[pz, :, i], one, d0, dn)
    c2 = Stage('x', lambda i: gsum.at[pz, py, i], (), c0, cn)
    d2 = Stage('y', lambda i: gsum.at[pz, i, px], (), d0, dn)

    a1.first()
    b1.first()
    arrive('e')
    g1.first()
    for phase in ('second', 'finish'):
        for s in (a1, b1, g1):
            getattr(s, phase)()
            if phase == 'finish':
                for t in {a1: (a2,), b1: (b2,), g1: (c1, d1)}[s]:
                    t.first()
    for s in (a2, b2, c1, d1):
        s.second()
    for s in (a2, b2):
        s.finish()
    oute_ref[...] = tsum[py, px, :, 0:oute_ref.shape[1]]
    for s, t in ((c1, c2), (d1, d2)):
        s.finish()
        t.first()
    for s in (c2, d2):
        s.second()
    for s in (c2, d2):
        s.finish()
    outw_ref[...] = gsum[pz, py, px]
    for c in sent:
        c.wait_send()


def tail_call(t, g, e, rows):
    def ring_bufs(lead, n):
        (_, p), (_, q) = cut(0, n)
        return [pltpu.VMEM(lead + (ROW, w), F32) for w in (p, q, n, n)]
    (_, cn), (_, dn) = cut(0, GCOLS)
    one, two, three = (RING,), (RING,) * 2, (RING,) * 3
    bufs = sum((ring_bufs(*b) for b in ((one, COLOR), (one, COLOR), (two, GCOLS), ((), COLOR), ((), COLOR),
                                        (one, cn), (one, dn), ((), cn), ((), dn))), [])
    dma = pltpu.SemaphoreType.DMA
    hbm = pl.BlockSpec(memory_space=pl.ANY)
    vm = pl.BlockSpec(memory_space=pltpu.VMEM)
    return pl.pallas_call(
        tail_kernel,
        in_specs=[hbm] * 3, out_specs=[vm] * 2,
        out_shape=[jax.ShapeDtypeStruct((ROW, rows), F32), jax.ShapeDtypeStruct((ROW, GCOLS), F32)],
        scratch_shapes=[pltpu.VMEM(two + (ROW, PAD), F32)] * 2 + [pltpu.VMEM(three + (ROW, GCOLS), F32)] * 2
        + [dma((64,)), dma((64,)), dma((16,))] + bufs,
        compiler_params=pltpu.CompilerParams(collective_id=0, has_side_effects=True, vmem_limit_bytes=VMEM_LIMIT),
        name="tail",
    )(t, g, e)


def solution(mesh):
    tp, dp, no = 'tp', 'dp', None
    one, vec_dp, both = P(no), P(dp), P((tp, dp))
    arg_specs = (P(dp, no), P(tp, no), one, one, one, one, P(no, tp, no, no), P(tp, no, no), P(tp, no, no), one, P(no, tp), P(tp), P(tp, no), one, P(dp, no, no))
    out_specs = (P(dp, no, no), P(tp, dp), vec_dp, vec_dp, vec_dp, vec_dp, P(dp, tp, no, no), both, P(tp, no, dp), vec_dp, P(dp, tp), both, P(tp, dp), vec_dp)
    chips = mesh.shape[dp]
    plane = chips // RING

    def swap(v):
        return lax.ppermute(v, tp, [(0, 1), (1, 0)])

    def z_shift(v, k):
        return lax.ppermute(v, dp, [(i, (i + k * plane) % chips) for i in range(chips)]) if k else v

    def device_step(token_ids, embed_table, ln1_gain, ln1_bias, ln2_gain, ln2_bias, w_qkv, b_qkv, w_dense, b_dense, w_fc1, b_fc1, w_fc2, b_fc2, cotangent):
        core = lax.axis_index(tp)
        z = (lax.axis_index(dp) // plane).reshape(1)
        vocab_local = embed_table.shape[0]
        seqs = token_ids.shape[0] // 2
        f = lambda v: v.astype(F32)

        wq_own = w_qkv.transpose(2, 1, 3, 0).reshape(3 * HALF, D)
        wd_own = w_dense.reshape(HALF, D)
        rows_peer = swap(f(jnp.concatenate([wq_own, wd_own, w_fc2], axis=0)))
        fc1_peer = swap(f(w_fc1))
        b_peer = swap(f(jnp.concatenate([b_qkv.reshape(-1), b_fc1])))
        bqkv = jnp.concatenate([f(b_qkv), b_peer[:b_qkv.size].reshape(b_qkv.shape)], axis=0).transpose(1, 0, 2).reshape(3, D)
        bfc1 = jnp.concatenate([f(b_fc1), b_peer[b_qkv.size:]]).reshape(1, FF)
        vec = jnp.stack([f(ln1_gain), f(ln1_bias), f(ln2_gain), f(ln2_bias), f(b_dense) + f(b_fc2)])

        def lookup(ids):
            local = ids - core * vocab_local
            ok = (local >= 0) & (local < vocab_local)
            got = jnp.take(embed_table, jnp.where(ok, local, 0), axis=0)
            return jnp.where(ok[..., None], got, jnp.zeros_like(got))

        ids_own = lax.dynamic_slice_in_dim(token_ids, core * seqs, seqs, 0)
        ids_peer = lax.dynamic_slice_in_dim(token_ids, (1 - core) * seqs, seqs, 0)
        cot = lax.dynamic_slice_in_dim(cotangent, core * seqs, seqs, 0)
        x_peer = swap(f(lookup(ids_peer)))
        x_own = lookup(ids_own)
        flat = ids_own.reshape(-1)
        ids_z = [z_shift(flat, k) for k in range(RING)]

        args = (x_own, x_peer, cot, vec, bqkv, bfc1, rope_consts(), wq_own, wd_own, w_fc1, w_fc2, rows_peer, fc1_peer)
        carried, owns, others, rows, row_ids, first = (), [], [], [], [], 0
        for count in CHUNKS:
            out, *gx_carried = layer_call(first, count, carried, z, *args)
            gx, carried = gx_carried[:RING], gx_carried[RING:]
            owns.append(out)
            others.append(swap(out))
            rows += [z_shift(gx[k], k) for k in range(RING)]
            row_ids += [ids_z[k][first * S:(first + count) * S] for k in range(RING)]
            first += count
        grad_w, grad_s, grad_b1 = carried
        layer_out = merge_call(core, owns, others)

        ids = jnp.concatenate(row_ids) - core * vocab_local
        dense = table_call(jnp.where(ids < 0, ids + 2 * vocab_local, ids), rows, vocab_local)

        small = jnp.sum(grad_s, axis=1)
        norms = small[:5].reshape(5, chips, ROW).transpose(1, 0, 2).reshape(chips, 5 * ROW)
        grad_bq = small[5:].reshape(3, 2, PAIRS, HD).transpose(1, 2, 0, 3).reshape(2, chips, -1)
        grad_bf = jnp.sum(grad_b1, axis=0).reshape(2, chips, -1)
        extra = jnp.concatenate([jnp.stack([norms, norms]), grad_bq, grad_bf], axis=2)
        ends = (5 * ROW, 5 * ROW + grad_bq.shape[2], extra.shape[2])
        extra = jnp.pad(extra[:, :, None, :], ((0, 0), (0, 0), (0, ROW - 1), (0, EXTRA - ends[2])))
        ring3 = (RING,) * 3
        sum_embed, total = tail_call(dense.reshape(2, RING, RING, ROW, PAD), grad_w.reshape(ring3 + (ROW, 2 * WIDE)),
                                     extra.reshape((2,) + ring3 + (ROW, EXTRA)), vocab_local)
        qkv, wide = 3 * HALF, 4 * HALF
        sum_wqkv = total[:, :qkv].reshape(ROW, 3, PAIRS, HD).transpose(0, 2, 1, 3)
        sum_wdense = total[:, qkv:wide].reshape(ROW, PAIRS, HD).transpose(1, 2, 0)
        sum_wfc1, sum_wfc2 = total[:, wide:2 * wide], total[:, 2 * wide:WIDE].T
        last = total[0, WIDE:]
        n1g, n1b, n2g, n2b, bias = last[:ends[0]].reshape(5, ROW)
        return (layer_out, sum_embed.T, n1g, n1b, n2g, n2b, sum_wqkv, last[ends[0]:ends[1]], sum_wdense, bias, sum_wfc1,
                last[ends[1]:ends[2]], sum_wfc2, bias)

    return jax.shard_map(device_step, mesh=mesh, in_specs=arg_specs, out_specs=out_specs, check_vma=False)
```

```python
import functools
import math
import jax
import jax.numpy as jnp
from jax import lax
from jax.experimental import pallas as pl
from jax.experimental.pallas import tpu as pltpu
from jax.sharding import PartitionSpec as P

F32, BF16 = jnp.float32, jnp.bfloat16
NN = (((1,), (0,)), ((), ()))
NT = (((1,), (1,)), ((), ()))
TN = (((0,), (0,)), ((), ()))
S, D, FF, HEADS, HD = 512, 512, 2048, 8, 64
PAIR, HALF, PAIRS, FF_STEPS, ROT_HALF = 2 * HD, S // 2, HEADS // 2, FF // S, HD // 8
EPS, ROPE_BASE = 1e-5, 10000.0
LOG2E = 1.4426950408889634
SQRT_HALF, INV_SQRT_2PI = 0.7071067811865476, 0.3989422804014327
ERF_P = 0.35
ERF_C = (0.19746628636396, 0.19745311511580, 0.18590938935029, 0.15467161331132, 0.16294620242859,
         -0.014553608641014, 0.20121223107286, -0.085106053125625)
RB = 128
VMEM_LIMIT = 67_000_000
ROW, LANES, RING = 8, 128, 4
PAD = 25600
COLOR = PAD // 2
WIDE, EXTRA = 3072, 128
GCOLS = WIDE + EXTRA
MESH = pl.DeviceIdType.MESH


def dot(a, b, dims=NN):
    return lax.dot_general(a, b, dims, preferred_element_type=F32)


def rnd(v):
    return v.astype(BF16).astype(F32)


def gelu_parts(a):
    t = 1.0 / (1.0 + (ERF_P * SQRT_HALF) * jnp.abs(a))
    r = 0.5 * ERF_C[-1]
    for c in ERF_C[-2::-1]:
        r = r * t + 0.5 * c
    e = jnp.exp2(a * a * (-0.5 * LOG2E))
    q = r * t * e
    phi = jnp.where(a < 0, q, 1.0 - q)
    return a * phi, phi + a * e * INV_SQRT_2PI


def block(i, n):
    return slice(i * n, i * n + n)


def row_sums(v):
    return jnp.sum(v.reshape(RB // ROW, ROW, v.shape[-1]), axis=0)


def row_loop(body):
    @pl.loop(0, S // RB)
    def _(i):
        body(pl.ds(pl.multiple_of(i * RB, RB), RB))


def wcol(half, part, width):
    return slice(half * WIDE + part, half * WIDE + part + width)


def layer_kernel(xo_ref, xp_ref, cot_ref, vec_ref, bqkv_ref, bfc1_ref, rope_ref, qo_ref, do_ref, fo_ref, to_ref, rp_ref, fp_ref,
                 out_ref, rows_ref, gw_ref, gs_ref, gb1_ref,
                 wqkv, wd, w1, w2, n_scr, inv_scr, x_scr, acc_scr, dh2_scr, a_scr, g_scr, h1_scr, h2_scr, h1t_scr, h2t_scr, cott_scr,
                 dctx_scr, ctx_scr, u_scr, da_scr, qkv_scr, dqkv_scr,
                 gx_buf, out_buf, peer_buf, own_low, peer_low, gx_send, gx_recv, gx_local, out_send, out_recv, own_sem, peer_sem, init_sem):
    step, last = pl.program_id(0), pl.num_programs(0) - 1
    slot = step % 2
    core, chip = lax.axis_index('tp'), lax.axis_index('dp')
    chips = lax.axis_size('dp')
    plane = chips // RING
    z, peer = chip // plane, (1 - core, chip)

    def z_device(k):
        return (core, (chip + k * plane) % chips)

    @pl.when(step == 0)
    def _():
        barrier = pltpu.get_barrier_semaphore()
        near = [peer] + [z_device(k) for k in range(1, RING)]
        for who in near:
            pl.semaphore_signal(barrier, inc=1, device_id=who, device_id_type=MESH)
        pl.semaphore_wait(barrier, len(near))
        for dst in (gw_ref, gs_ref, gb1_ref):
            dst[...] = jnp.zeros_like(dst)
        n = FF // 2
        moves = [(qo_ref.at[block(j, HALF)], wqkv.at[block(2 * j, HALF)]) for j in range(3)]
        moves += [(do_ref, wd.at[:HALF]), (to_ref, w2.at[:n]), (fo_ref, w1.at[:, :n])]
        tables = (n_scr, x_scr, acc_scr, dh2_scr, a_scr, g_scr)
        parts = [rp_ref.at[block(i, S)] for i in range(RING)] + [fp_ref.at[:, block(i, S)] for i in range(2)]
        copies = [pltpu.make_async_copy(src, dst, init_sem.at[i]) for i, (src, dst) in enumerate(moves + list(zip(parts, tables)))]
        for c in copies:
            c.start()
        for c in copies:
            c.wait()
        for j in range(3):
            wqkv[block(2 * j + 1, HALF), :] = tables[j // 2][block(j % 2, HALF), :].astype(BF16)
        wd[HALF:, :] = tables[1][HALF:, :].astype(BF16)
        for i in range(2):
            w2[block(2 + i, S), :] = tables[2 + i][...].astype(BF16)
            w1[:, block(2 + i, S)] = tables[RING + i][...].astype(BF16)

    def gx_copy(at, k):
        rows = pl.ds(pl.multiple_of(at * S, S), S)
        src, dst = gx_buf.at[at % 2, k], rows_ref.at[k, rows]
        if k:
            return pltpu.make_async_remote_copy(src, dst, gx_send.at[at % 2, k], gx_recv.at[at, k], device_id=z_device(k), device_id_type=MESH)
        return pltpu.make_async_copy(src, dst, gx_local.at[at % 2])

    def out_copy(at):
        return pltpu.make_async_remote_copy(out_buf.at[at % 2], peer_buf.at[at], out_send.at[at % 2], out_recv.at[at], device_id=peer, device_id_type=MESH)

    def own_store(at):
        return pltpu.make_async_copy(own_low.at[at % 2], out_ref.at[core * (last + 1) + at], own_sem.at[at % 2])

    def peer_store(at):
        return pltpu.make_async_copy(peer_low.at[at % 2], out_ref.at[(1 - core) * (last + 1) + at], peer_sem.at[at % 2])

    def drain(at):
        gx_copy(at, 0).wait()
        for k in range(1, RING):
            gx_copy(at, k).wait_send()
        out_copy(at).wait_send()
        own_store(at).wait()

    def take_peer(at):
        out_copy(at).wait_recv()

        @pl.when(at > 1)
        def _():
            peer_store(at - 2).wait()
        peer_low[at % 2] = peer_buf[at].astype(BF16)
        peer_store(at).start()

    @pl.when(step > 1)
    def _():
        drain(step - 2)

    cot = cot_ref[0]
    g1, b1, g2, b2, bo = (vec_ref[i:i + 1, :] for i in range(5))

    def norm(rows):
        x = xo_ref[0, rows, :].astype(F32) + xp_ref[0, rows, :]
        x_scr[rows, :] = x
        cen = x - jnp.mean(x, axis=-1, keepdims=True)
        inv = lax.rsqrt(jnp.mean(cen * cen, axis=-1, keepdims=True) + EPS)
        n = cen * inv
        n_scr[rows, :] = n
        inv_scr[rows, :] = inv
        h1_scr[rows, :] = (n * g1 + b1).astype(BF16)
        h2_scr[rows, :] = (n * g2 + b2).astype(BF16)
        gs_ref[4] += row_sums(cot_ref[0, rows, :].astype(F32))
    row_loop(norm)

    h1t_scr[...] = h1_scr[...].T
    h2t_scr[...] = h2_scr[...].T
    cott_scr[...] = cot.T

    h1 = h1_scr[...]
    for p in range(PAIRS):
        for j in range(3):
            v = dot(h1, wqkv[block(j * PAIRS + p, PAIR), :], NT) + bqkv_ref[j:j + 1, block(p, PAIR)]
            v = v.astype(BF16)
            if j < 2:
                v = v.astype(F32)
                v = (v * rope_ref[0] + pltpu.roll(v, PAIR - ROT_HALF, 1) * rope_ref[1]
                     + pltpu.roll(v, ROT_HALF, 1) * rope_ref[2]).astype(BF16)
            qkv_scr[j, :, block(p, PAIR)] = v
    dctx_scr[...] = dot(cot, wd[...], NT).astype(BF16)

    lane = lax.broadcasted_iota(jnp.int32, (S, PAIR), 1)
    causal = lax.broadcasted_iota(jnp.int32, (HALF, HALF), 0) >= lax.broadcasted_iota(jnp.int32, (HALF, HALF), 1)
    zero = jnp.zeros((S, PAIR), BF16)

    def plus(lst, i, v):
        lst[i] = v if i not in lst else lst[i] + v

    for p in range(PAIRS):
        cs = block(p, PAIR)
        qp, kp, vp = (qkv_scr[j, :, cs] for j in range(3))
        dcp = dctx_scr[:, cs]
        ctx, dq, dk, dv = {}, {}, {}, {}
        for mine in (lane < HD, lane >= HD):
            qm, km, vm, dcm = (jnp.where(mine, w, zero) for w in (qp, kp, vp, dcp))
            for qb in range(2):
                kl = HALF * (qb + 1)
                qs = block(qb, HALF)
                s = dot(qm[qs], kp[:kl], NT)
                diag = jnp.where(causal, s[:, kl - HALF:], -1e30)
                s = jnp.concatenate([s[:, :HALF], diag], axis=1) if qb else diag
                e = jnp.exp2((s - jnp.max(s, axis=-1, keepdims=True)) * (HD ** -0.5 * LOG2E))
                pr = e * (1.0 / jnp.sum(e, axis=-1, keepdims=True))
                pb = pr.astype(BF16)
                plus(ctx, qb, dot(pb, vm[:kl]))
                dp = rnd(dot(dcm[qs], vp[:kl], NT))
                ds = (pr * (dp - jnp.sum(pr * dp, axis=-1, keepdims=True))).astype(BF16)
                plus(dq, qb, dot(ds, km[:kl]))
                dkb = dot(ds, qm[qs], TN)
                dvb = dot(pb, dcm[qs], TN)
                for kb in range(qb + 1):
                    plus(dk, kb, dkb[block(kb, HALF)])
                    plus(dv, kb, dvb[block(kb, HALF)])
        for b in range(2):
            bs = block(b, HALF)
            ctx_scr[bs, cs] = ctx[b].astype(BF16)
            for j, g in enumerate((dq[b], dk[b])):
                g = rnd(g * HD ** -0.5)
                spun = g * rope_ref[3, bs]
                dqkv_scr[j, bs, cs] = (g * rope_ref[0, bs] + pltpu.roll(spun, PAIR - ROT_HALF, 1) * rope_ref[4, bs]
                                       + pltpu.roll(spun, ROT_HALF, 1) * rope_ref[5, bs]).astype(BF16)
            dqkv_scr[2, bs, cs] = dv[b].astype(BF16)

    acc_scr[...] = dot(ctx_scr[...], wd[...])
    dh2_scr[...] = jnp.zeros_like(dh2_scr)
    h2 = h2_scr[...]
    for c in range(FF_STEPS):
        cs = block(c, S)
        a_scr[...] = dot(h2, w1[:, cs]) + bfc1_ref[:, cs]
        g_scr[...] = dot(cot, w2[cs, :], NT)

        def act(rows, cs=cs):
            u, gp = gelu_parts(rnd(a_scr[rows, :]))
            da = (rnd(g_scr[rows, :]) * gp).astype(BF16)
            u_scr[rows, :] = u.astype(BF16)
            da_scr[rows, :] = da
            gb1_ref[:, cs] += row_sums(da.astype(F32))
        row_loop(act)

        u, da = u_scr[...], da_scr[...]
        acc_scr[...] += dot(u, w2[cs, :])
        dh2_scr[...] += dot(da, w1[:, cs], NT)
        half, part = c // 2, 2 * S + c % 2 * S
        gw_ref[:, wcol(half, part, S)] += dot(h2t_scr[...], da)
        gw_ref[:, wcol(half, part + 2 * S, S)] += dot(cott_scr[...], u)

    for half in range(2):
        hs = block(half, HALF)
        for j in range(3):
            gw_ref[:, wcol(half, j * HALF, HALF)] += dot(h1t_scr[...], dqkv_scr[j, :, hs])
        gw_ref[:, wcol(half, 3 * HALF, HALF)] += dot(cott_scr[...], ctx_scr[:, hs])
    a_scr[...] = sum(dot(dqkv_scr[j], wqkv[block(j, S), :]) for j in range(3))

    def back(rows):
        n = n_scr[rows, :]
        d1, d2 = rnd(a_scr[rows, :]), rnd(dh2_scr[rows, :])
        for i, v in zip((0, 1, 2, 3, 5, 6, 7), (d1 * n, d1, d2 * n, d2, *(dqkv_scr[j, rows, :].astype(F32) for j in range(3)))):
            gs_ref[i] += row_sums(v)
        gn = d1 * g1 + d2 * g2
        g_scr[rows, :] = cot_ref[0, rows, :].astype(F32) + inv_scr[rows, :] * (
            gn - jnp.mean(gn, axis=-1, keepdims=True) - n * jnp.mean(gn * n, axis=-1, keepdims=True))
        for k in range(RING):
            gx_buf[slot, k, rows, :] = g_scr[rows, pl.ds(pl.multiple_of((z + k) % RING * LANES, LANES), LANES)]
        low = (x_scr[rows, :] + (acc_scr[rows, :] + bo)).astype(BF16)
        own_low[slot, rows, :] = low
        out_buf[slot, rows, :] = low.astype(F32)
    row_loop(back)
    for k in range(RING):
        gx_copy(step, k).start()
    out_copy(step).start()
    own_store(step).start()

    @pl.when(step > 0)
    def _():
        take_peer(step - 1)

    @pl.when(step == last)
    def _():
        take_peer(step)
        for at in (step - 1, step):
            drain(at)
            peer_store(at).wait()

        @pl.loop(0, last + 1)
        def _(at):
            for k in range(1, RING):
                gx_copy(at, k).wait_recv()


def rope_consts():
    inv_freq = ROPE_BASE ** (-jnp.arange(ROT_HALF, dtype=F32) / ROT_HALF)
    ang = jnp.arange(S, dtype=F32)[:, None] * inv_freq[None, :]
    cos, sin = jnp.cos(ang), jnp.sin(ang)
    one, zero = jnp.ones_like(cos), jnp.zeros_like(cos)
    keep, none = jnp.ones((S, HD - 2 * ROT_HALF), F32), jnp.zeros((S, HD - 2 * ROT_HALF), F32)
    parts = ((cos, cos, keep), (-sin, zero, none), (zero, sin, none), (sin, sin, none), (one, zero, none), (zero, -one, none))
    return jnp.stack([jnp.concatenate(p + p, axis=1) for p in parts])


def layer_call(*args):
    count = args[0].shape[0]
    vm, hbm = pl.BlockSpec(memory_space=pltpu.VMEM), pl.BlockSpec(memory_space=pl.ANY)
    seq = pl.BlockSpec((1, S, D), lambda i: (i, 0, 0))
    table, low, dma = pltpu.VMEM((S, D), F32), pltpu.VMEM((S, D), BF16), pltpu.SemaphoreType.DMA
    return pl.pallas_call(
        layer_kernel,
        grid=(count,),
        in_specs=[seq] * 3 + [vm] * 4 + [hbm] * (len(args) - 7),
        out_specs=[hbm] * 2 + [vm] * 3,
        out_shape=[jax.ShapeDtypeStruct((2 * count, S, D), BF16), jax.ShapeDtypeStruct((RING, count * S, LANES), F32),
                   jax.ShapeDtypeStruct((D, 2 * WIDE), F32), jax.ShapeDtypeStruct((ROW, ROW, D), F32), jax.ShapeDtypeStruct((ROW, FF), F32)],
        scratch_shapes=[pltpu.VMEM((3 * S, D), BF16), low, pltpu.VMEM((D, FF), BF16), pltpu.VMEM((FF, D), BF16), table,
                        pltpu.VMEM((S, 1), F32)] + [table] * 5 + [low] * 9 + [pltpu.VMEM((3, S, D), BF16)] * 2
        + [pltpu.VMEM((2, RING, S, LANES), F32), pltpu.VMEM((2, S, D), F32), pltpu.VMEM((count, S, D), F32)]
        + [pltpu.VMEM((2, S, D), BF16)] * 2
        + [dma((2, RING)), dma((count, RING)), dma((2,)), dma((2,)), dma((count,)), dma((2,)), dma((2,)), dma((16,))],
        compiler_params=pltpu.CompilerParams(dimension_semantics=("arbitrary",), collective_id=1, has_side_effects=True,
                                             vmem_limit_bytes=VMEM_LIMIT),
        cost_estimate=pl.CostEstimate(flops=count * 30_000_000_000, bytes_accessed=60_000_000, transcendentals=0),
        name="layer",
    )(*args)


STEPS, UNROLL = 8, 8
STEP = PAD // STEPS


def table_kernel(half, ids_ref, rows_ref, out_ref, acc, acc2, stage, sem):
    @pl.loop(0, acc.shape[0] // LANES)
    def _(j):
        for a in (acc, acc2):
            a[pl.ds(pl.multiple_of(j * LANES, LANES), LANES), :] = jnp.zeros((LANES, LANES), F32)
    count = rows_ref.shape[1]
    for k in range(0, RING, 2):
        @pl.loop(0, count // UNROLL)
        def _(g):
            t0 = pl.multiple_of(g * UNROLL, UNROLL)
            for j in range(UNROLL):
                for a, src in ((acc, k), (acc2, k + 1)):
                    row = pl.ds(ids_ref[src * count + t0 + j], 1)
                    a[row, :] += rows_ref[src, pl.ds(t0 + j, 1), :]
    copies = []
    for i in range(2 * STEPS):
        h, c, slot = i // STEPS, i % STEPS, i % 2
        if i > 1:
            copies[i - 2].wait()

        @pl.loop(0, STEP // LANES, unroll=5)
        def _(b):
            at = pl.ds(pl.multiple_of(h * half + c * STEP + b * LANES, ROW), LANES)
            stage[slot, :, pl.ds(pl.multiple_of(b * LANES, LANES), LANES)] = (acc[at, :] + acc2[at, :]).T
        copies.append(pltpu.make_async_copy(stage.at[slot], out_ref.at[h, :, pl.ds(c * STEP, STEP)], sem.at[slot]))
        copies[i].start()
    for c in copies[-2:]:
        c.wait()


def table_call(ids, rows, half):
    return pl.pallas_call(
        functools.partial(table_kernel, half),
        grid_spec=pltpu.PrefetchScalarGridSpec(
            num_scalar_prefetch=1, grid=(), in_specs=[pl.BlockSpec(memory_space=pltpu.VMEM)],
            out_specs=pl.BlockSpec(memory_space=pl.ANY),
            scratch_shapes=[pltpu.VMEM((half + PAD, LANES), F32)] * 2 + [pltpu.VMEM((2, LANES, STEP), F32), pltpu.SemaphoreType.DMA((2,))]),
        out_shape=jax.ShapeDtypeStruct((2, LANES, PAD), F32),
        compiler_params=pltpu.CompilerParams(vmem_limit_bytes=VMEM_LIMIT),
        cost_estimate=pl.CostEstimate(flops=4_000_000_000, bytes_accessed=34_000_000, transcendentals=0),
        name="table",
    )(ids, rows)


def cut(lo, n):
    first = n // (2 * LANES) * LANES
    return (lo, first), (lo + first, n - first)


def over(lead, body, at=()):
    if not lead:
        return body(at)

    @pl.loop(0, lead[0])
    def _(i):
        over(lead[1:], body, at + (i,))


def add_into(dst, srcs, lead, lo, n):
    def body(at):
        v = dst[at + (slice(None), pl.ds(lo, n))]
        for s in srcs:
            v = v + s[at + (slice(None), pl.ds(0, n))]
        dst[at + (slice(None), pl.ds(lo, n))] = v
    over(lead, body)


def tail_kernel(t_ref, g_ref, e_ref, oute_ref, outw_ref, *scratch):
    tsum, tpeer, gsum, gpeer, send, recv, local = scratch[:7]
    bufs = list(scratch[7:])
    core, dp = lax.axis_index('tp'), lax.axis_index('dp')
    pos = {'z': dp // (RING * RING), 'y': dp // RING % RING, 'x': dp % RING}
    stride = {'z': RING * RING, 'y': RING, 'x': 1}

    def shift(axis, k):
        return (pos[axis] + k) % RING

    def device(axis, k):
        return (core, dp + (shift(axis, k) - pos[axis]) * stride[axis])
    peer = (1 - core, dp)

    barrier = pltpu.get_barrier_semaphore()
    near = [peer] + [device(axis, k) for axis in 'zyx' for k in (1, RING - 1)]
    for who in near:
        pl.semaphore_signal(barrier, inc=1, device_id=who, device_id_type=MESH)
    pl.semaphore_wait(barrier, len(near))

    used = [0, 0]

    def remote(src, dst, who):
        i = used[0]
        used[0] += 1
        c = pltpu.make_async_remote_copy(src, dst, send.at[i], recv.at[i], device_id=who, device_id_type=MESH)
        c.start()
        return c

    def load(src, dst):
        i = used[1]
        used[1] += 1
        c = pltpu.make_async_copy(src, dst, local.at[i])
        c.start()
        return c
    sent = []

    full = pl.ds(0, COLOR)
    rest = pl.ds(COLOR, COLOR)
    wide, extra, far = pl.ds(0, WIDE), pl.ds(WIDE, EXTRA), pl.ds(WIDE, WIDE)
    every = slice(None)
    views = {
        'a': ('y', lambda i: (i, every, every, full)),
        'b': ('x', lambda i: (every, i, every, rest)),
        'g': ('z', lambda i: (i, every, every, every, wide)),
    }
    pend = {}
    pend['e'] = [remote(e_ref.at[1], gpeer.at[every, every, every, every, extra], peer),
                 load(e_ref.at[0], gsum.at[every, every, every, every, extra])]
    for k in (2, 1, RING - 1, 0):
        for name, (axis, view) in views.items():
            at = view(shift(axis, k))
            if name == 'g':
                there = at[:-1] + (far,)
                pend[name, k] = [remote(g_ref.at[there], gpeer.at[at], peer), load(g_ref.at[at], gsum.at[at])]
            else:
                pend[name, k] = [remote(t_ref.at[(1,) + at], tpeer.at[at], peer), load(t_ref.at[(0,) + at], tsum.at[at])]

    def arrive(key):
        out, here = pend[key]
        sent.append(out)
        out.wait_recv()
        here.wait()

    def ready(name, k):
        arrive((name, k))
        axis, _ = views[name]
        i = shift(axis, k)
        if name == 'a':
            add_into(tsum.at[i], [tpeer.at[i]], (RING,), 0, COLOR)
        elif name == 'b':
            add_into(tsum.at[:, i, :, rest], [tpeer.at[:, i, :, rest]], (RING,), 0, COLOR)
        else:
            add_into(gsum.at[i], [gpeer.at[i]], (RING, RING), 0, GCOLS)

    class Stage:
        def __init__(self, axis, piece, lead, lo, n, need=None):
            self.axis, self.piece, self.lead, self.lo, self.n, self.need = axis, piece, lead, lo, n, need
            self.halves = cut(lo, n)
            self.near = [bufs.pop(0), bufs.pop(0)]
            self.last = [bufs.pop(0), bufs.pop(0)]

        def view(self, k, lo, n):
            return self.piece(shift(self.axis, k)).at[(every,) * (len(self.lead) + 1) + (pl.ds(lo, n),)]

        def want(self, k):
            if self.need:
                ready(self.need, k)

        def first(self):
            self.want(2)
            self.c1 = [remote(self.view(2, *self.halves[s]), self.near[s], device(self.axis, k))
                       for s, k in enumerate((1, RING - 1))]

        def second(self):
            self.want(1)
            self.want(RING - 1)
            self.c2 = []
            for s, k in enumerate((1, RING - 1)):
                self.c1[s].wait_recv()
                add_into(self.piece(shift(self.axis, k)), [self.near[s]], self.lead, *self.halves[s])
                self.c2.append(remote(self.view(k, self.lo, self.n), self.last[s], device(self.axis, k)))

        def finish(self):
            self.want(0)
            for c in self.c2:
                c.wait_recv()
            add_into(self.piece(shift(self.axis, 0)), self.last, self.lead, self.lo, self.n)
            sent.extend(self.c1 + self.c2)

    py, px, pz = pos['y'], pos['x'], pos['z']
    one, two = (RING,), (RING, RING)
    a1 = Stage('y', lambda i: tsum.at[i], one, 0, COLOR, 'a')
    b1 = Stage('x', lambda i: tsum.at[:, i], one, COLOR, COLOR, 'b')
    g1 = Stage('z', lambda i: gsum.at[i], two, 0, GCOLS, 'g')
    a2 = Stage('x', lambda i: tsum.at[py, i], (), 0, COLOR)
    b2 = Stage('y', lambda i: tsum.at[i, px], (), COLOR, COLOR)
    (c0, cn), (d0, dn) = cut(0, GCOLS)
    c1 = Stage('y', lambda i: gsum.at[pz, i], one, c0, cn)
    d1 = Stage('x', lambda i: gsum.at[pz, :, i], one, d0, dn)
    c2 = Stage('x', lambda i: gsum.at[pz, py, i], (), c0, cn)
    d2 = Stage('y', lambda i: gsum.at[pz, i, px], (), d0, dn)

    a1.first()
    b1.first()
    arrive('e')
    g1.first()
    for phase in ('second', 'finish'):
        for s in (a1, b1, g1):
            getattr(s, phase)()
            if phase == 'finish':
                for t in {a1: (a2,), b1: (b2,), g1: (c1, d1)}[s]:
                    t.first()
    for s in (a2, b2, c1, d1):
        s.second()
    for s in (a2, b2):
        s.finish()
    oute_ref[...] = tsum[py, px, :, 0:oute_ref.shape[1]]
    for s, t in ((c1, c2), (d1, d2)):
        s.finish()
        t.first()
    for s in (c2, d2):
        s.second()
    for s in (c2, d2):
        s.finish()
    outw_ref[...] = gsum[pz, py, px]
    for c in sent:
        c.wait_send()


def tail_call(t, g, e, rows):
    def ring_bufs(lead, n):
        (_, p), (_, q) = cut(0, n)
        return [pltpu.VMEM(lead + (ROW, w), F32) for w in (p, q, n, n)]
    (_, cn), (_, dn) = cut(0, GCOLS)
    one, two, three = (RING,), (RING,) * 2, (RING,) * 3
    bufs = sum((ring_bufs(*b) for b in ((one, COLOR), (one, COLOR), (two, GCOLS), ((), COLOR), ((), COLOR),
                                        (one, cn), (one, dn), ((), cn), ((), dn))), [])
    dma = pltpu.SemaphoreType.DMA
    hbm = pl.BlockSpec(memory_space=pl.ANY)
    vm = pl.BlockSpec(memory_space=pltpu.VMEM)
    return pl.pallas_call(
        tail_kernel,
        in_specs=[hbm] * 3, out_specs=[vm] * 2,
        out_shape=[jax.ShapeDtypeStruct((ROW, rows), F32), jax.ShapeDtypeStruct((ROW, GCOLS), F32)],
        scratch_shapes=[pltpu.VMEM(two + (ROW, PAD), F32)] * 2 + [pltpu.VMEM(three + (ROW, GCOLS), F32)] * 2
        + [dma((64,)), dma((64,)), dma((16,))] + bufs,
        compiler_params=pltpu.CompilerParams(collective_id=0, has_side_effects=True, vmem_limit_bytes=VMEM_LIMIT),
        name="tail",
    )(t, g, e)


def solution(mesh):
    tp, dp, no = 'tp', 'dp', None
    one, vec_dp, both = P(no), P(dp), P((tp, dp))
    arg_specs = (P(dp, no), P(tp, no), one, one, one, one, P(no, tp, no, no), P(tp, no, no), P(tp, no, no), one, P(no, tp), P(tp), P(tp, no), one, P(dp, no, no))
    out_specs = (P(dp, no, no), P(tp, dp), vec_dp, vec_dp, vec_dp, vec_dp, P(dp, tp, no, no), both, P(tp, no, dp), vec_dp, P(dp, tp), both, P(tp, dp), vec_dp)
    chips = mesh.shape[dp]
    plane = chips // RING

    def swap(v):
        return lax.ppermute(v, tp, [(0, 1), (1, 0)])

    def z_shift(v, k):
        return lax.ppermute(v, dp, [(i, (i + k * plane) % chips) for i in range(chips)]) if k else v

    def device_step(token_ids, embed_table, ln1_gain, ln1_bias, ln2_gain, ln2_bias, w_qkv, b_qkv, w_dense, b_dense, w_fc1, b_fc1, w_fc2, b_fc2, cotangent):
        core = lax.axis_index(tp)
        vocab_local = embed_table.shape[0]
        seqs = token_ids.shape[0] // 2
        f = lambda v: v.astype(F32)

        wq_own = w_qkv.transpose(2, 1, 3, 0).reshape(3 * HALF, D)
        wd_own = w_dense.reshape(HALF, D)
        rows_peer = swap(f(jnp.concatenate([wq_own, wd_own, w_fc2], axis=0)))
        fc1_peer = swap(f(w_fc1))
        b_peer = swap(f(jnp.concatenate([b_qkv.reshape(-1), b_fc1])))
        bqkv = jnp.concatenate([f(b_qkv), b_peer[:b_qkv.size].reshape(b_qkv.shape)], axis=0).transpose(1, 0, 2).reshape(3, D)
        bfc1 = jnp.concatenate([f(b_fc1), b_peer[b_qkv.size:]]).reshape(1, FF)
        vec = jnp.stack([f(ln1_gain), f(ln1_bias), f(ln2_gain), f(ln2_bias), f(b_dense) + f(b_fc2)])

        def lookup(ids):
            local = ids - core * vocab_local
            ok = (local >= 0) & (local < vocab_local)
            got = jnp.take(embed_table, jnp.where(ok, local, 0), axis=0)
            return jnp.where(ok[..., None], got, jnp.zeros_like(got))

        ids_own = lax.dynamic_slice_in_dim(token_ids, core * seqs, seqs, 0)
        ids_peer = lax.dynamic_slice_in_dim(token_ids, (1 - core) * seqs, seqs, 0)
        cot = lax.dynamic_slice_in_dim(cotangent, core * seqs, seqs, 0)
        x_peer = swap(f(lookup(ids_peer)))
        x_own = lookup(ids_own)
        flat = ids_own.reshape(-1)
        ids = jnp.concatenate([z_shift(flat, k) for k in range(RING)]) - core * vocab_local

        args = (x_own, x_peer, cot, vec, bqkv, bfc1, rope_consts(), wq_own, wd_own, w_fc1, w_fc2, rows_peer, fc1_peer)
        layer_out, rows, grad_w, grad_s, grad_b1 = layer_call(*args)

        dense = table_call(jnp.where(ids < 0, ids + 2 * vocab_local, ids), rows, vocab_local)

        small = jnp.sum(grad_s, axis=1)
        norms = small[:5].reshape(5, chips, ROW).transpose(1, 0, 2).reshape(chips, 5 * ROW)
        grad_bq = small[5:].reshape(3, 2, PAIRS, HD).transpose(1, 2, 0, 3).reshape(2, chips, -1)
        grad_bf = jnp.sum(grad_b1, axis=0).reshape(2, chips, -1)
        extra = jnp.concatenate([jnp.stack([norms, norms]), grad_bq, grad_bf], axis=2)
        ends = (5 * ROW, 5 * ROW + grad_bq.shape[2], extra.shape[2])
        extra = jnp.pad(extra[:, :, None, :], ((0, 0), (0, 0), (0, ROW - 1), (0, EXTRA - ends[2])))
        ring3 = (RING,) * 3
        sum_embed, total = tail_call(dense.reshape(2, RING, RING, ROW, PAD), grad_w.reshape(ring3 + (ROW, 2 * WIDE)),
                                     extra.reshape((2,) + ring3 + (ROW, EXTRA)), vocab_local)
        qkv, wide = 3 * HALF, 4 * HALF
        sum_wqkv = total[:, :qkv].reshape(ROW, 3, PAIRS, HD).transpose(0, 2, 1, 3)
        sum_wdense = total[:, qkv:wide].reshape(ROW, PAIRS, HD).transpose(1, 2, 0)
        sum_wfc1, sum_wfc2 = total[:, wide:2 * wide], total[:, 2 * wide:WIDE].T
        last = total[0, WIDE:]
        n1g, n1b, n2g, n2b, bias = last[:ends[0]].reshape(5, ROW)
        return (layer_out, sum_embed.T, n1g, n1b, n2g, n2b, sum_wqkv, last[ends[0]:ends[1]], sum_wdense, bias, sum_wfc1,
                last[ends[1]:ends[2]], sum_wfc2, bias)

    return jax.shard_map(device_step, mesh=mesh, in_specs=arg_specs, out_specs=out_specs, check_vma=False)
```

```python
import functools
import math
import jax
import jax.numpy as jnp
from jax import lax
from jax.experimental import pallas as pl
from jax.experimental.pallas import tpu as pltpu
from jax.sharding import PartitionSpec as P

F32, BF16 = jnp.float32, jnp.bfloat16
NN = (((1,), (0,)), ((), ()))
NT = (((1,), (1,)), ((), ()))
TN = (((0,), (0,)), ((), ()))
S, D, FF, HEADS, HD = 512, 512, 2048, 8, 64
PAIR, HALF, PAIRS, FF_STEPS, ROT_HALF = 2 * HD, S // 2, HEADS // 2, FF // S, HD // 8
EPS, ROPE_BASE = 1e-5, 10000.0
LOG2E = 1.4426950408889634
SQRT_HALF, INV_SQRT_2PI = 0.7071067811865476, 0.3989422804014327
ERF_P = 0.35
ERF_C = (0.19746628636396, 0.19745311511580, 0.18590938935029, 0.15467161331132, 0.16294620242859,
         -0.014553608641014, 0.20121223107286, -0.085106053125625)
RB = 128
VMEM_LIMIT = 67_000_000
ROW, LANES, RING = 8, 128, 4
PAD = 25600
COLOR = PAD // 2
WIDE, EXTRA = 3072, 128
GCOLS = WIDE + EXTRA
MESH = pl.DeviceIdType.MESH


def dot(a, b, dims=NN):
    return lax.dot_general(a, b, dims, preferred_element_type=F32)


def rnd(v):
    return v.astype(BF16).astype(F32)


def gelu_parts(a):
    t = 1.0 / (1.0 + (ERF_P * SQRT_HALF) * jnp.abs(a))
    r = 0.5 * ERF_C[-1]
    for c in ERF_C[-2::-1]:
        r = r * t + 0.5 * c
    e = jnp.exp2(a * a * (-0.5 * LOG2E))
    q = r * t * e
    phi = jnp.where(a < 0, q, 1.0 - q)
    return a * phi, phi + a * e * INV_SQRT_2PI


def block(i, n):
    return slice(i * n, i * n + n)


def row_sums(v):
    return jnp.sum(v.reshape(v.shape[0] // ROW, ROW, v.shape[1]), axis=0)


def wcol(half, part, width):
    return slice(half * WIDE + part, half * WIDE + part + width)


def layer_kernel(xo_ref, xp_ref, cot_ref, vec_ref, bqkv_ref, bfc1_ref, rope_ref, qo_ref, do_ref, fo_ref, to_ref, rp_ref, fp_ref,
                 out_ref, rows_ref, gw_ref, gs_ref, gb1_ref,
                 wqkv, wd, w1, w2, n_scr, acc_scr, dh2_scr, dh1_scr, inv_scr, h1_scr, h2_scr, h1t_scr, h2t_scr, cott_scr, dctx_scr, ctx_scr,
                 qkv_scr, dqkv_scr, s_scr, dp_scr, pb_scr, ds_scr, a_scr, du_scr, u_scr, da_scr, dk_scr, dv_scr,
                 gx_buf, out_buf, peer_buf, own_low, peer_low, gx_send, gx_recv, gx_local, out_send, out_recv, own_sem, peer_sem, init_sem):
    step, last = pl.program_id(0), pl.num_programs(0) - 1
    slot = step % 2
    core, chip = lax.axis_index('tp'), lax.axis_index('dp')
    chips = lax.axis_size('dp')
    plane = chips // RING
    z, peer = chip // plane, (1 - core, chip)

    def z_device(k):
        return (core, (chip + k * plane) % chips)

    @pl.when(step == 0)
    def _():
        barrier = pltpu.get_barrier_semaphore()
        near = [peer] + [z_device(k) for k in range(1, RING)]
        for who in near:
            pl.semaphore_signal(barrier, inc=1, device_id=who, device_id_type=MESH)
        pl.semaphore_wait(barrier, len(near))
        for dst in (gw_ref, gs_ref, gb1_ref):
            dst[...] = jnp.zeros_like(dst)
        n = FF // 2
        moves = [(qo_ref.at[block(j, HALF)], wqkv.at[block(2 * j, HALF)]) for j in range(3)]
        moves += [(do_ref, wd.at[:HALF]), (to_ref, w2.at[:n]), (fo_ref, w1.at[:, :n])]
        tables = (n_scr, acc_scr, dh2_scr, dh1_scr, s_scr.at[0], s_scr.at[1])
        parts = [rp_ref.at[block(i, S)] for i in range(RING)] + [fp_ref.at[:, block(i, S)] for i in range(2)]
        copies = [pltpu.make_async_copy(src, dst, init_sem.at[i]) for i, (src, dst) in enumerate(moves + list(zip(parts, tables)))]
        for c in copies:
            c.start()
        for c in copies:
            c.wait()
        for j in range(3):
            wqkv[block(2 * j + 1, HALF), :] = tables[j // 2][block(j % 2, HALF), :].astype(BF16)
        wd[HALF:, :] = tables[1][HALF:, :].astype(BF16)
        for i in range(2):
            w2[block(2 + i, S), :] = tables[2 + i][...].astype(BF16)
            w1[:, block(2 + i, S)] = tables[RING + i][...].astype(BF16)

    def gx_copy(at, k):
        rows = pl.ds(pl.multiple_of(at * S, S), S)
        src, dst = gx_buf.at[at % 2, k], rows_ref.at[k, rows]
        if k:
            return pltpu.make_async_remote_copy(src, dst, gx_send.at[at % 2, k], gx_recv.at[at, k], device_id=z_device(k), device_id_type=MESH)
        return pltpu.make_async_copy(src, dst, gx_local.at[at % 2])

    def out_copy(at):
        return pltpu.make_async_remote_copy(out_buf.at[at % 2], peer_buf.at[at], out_send.at[at % 2], out_recv.at[at], device_id=peer, device_id_type=MESH)

    def own_store(at):
        return pltpu.make_async_copy(own_low.at[at % 2], out_ref.at[core * (last + 1) + at], own_sem.at[at % 2])

    def peer_store(at):
        return pltpu.make_async_copy(peer_low.at[at % 2], out_ref.at[(1 - core) * (last + 1) + at], peer_sem.at[at % 2])

    def drain(at):
        gx_copy(at, 0).wait()
        for k in range(1, RING):
            gx_copy(at, k).wait_send()
        out_copy(at).wait_send()
        own_store(at).wait()

    def take_peer(at):
        out_copy(at).wait_recv()

        @pl.when(at > 1)
        def _():
            peer_store(at - 2).wait()
        peer_low[at % 2] = peer_buf[at].astype(BF16)
        peer_store(at).start()

    @pl.when(step > 1)
    def _():
        drain(step - 2)

    cot = cot_ref[0]
    g1, b1, g2, b2, bo = (vec_ref[i:i + 1, :] for i in range(5))

    dctx_scr[...] = dot(cot, wd[...], NT).astype(BF16)
    cott_scr[...] = cot.T
    x = xo_ref[0].astype(F32) + xp_ref[0]
    cen = x - jnp.mean(x, axis=-1, keepdims=True)
    inv = lax.rsqrt(jnp.mean(cen * cen, axis=-1, keepdims=True) + EPS)
    n = cen * inv
    n_scr[...] = n
    inv_scr[...] = inv
    h1_scr[...] = (n * g1 + b1).astype(BF16)
    h2_scr[...] = (n * g2 + b2).astype(BF16)
    gs_ref[4] += row_sums(cot.astype(F32))
    h1t_scr[...] = h1_scr[...].T
    h2t_scr[...] = h2_scr[...].T
    h1, h2 = h1_scr[...], h2_scr[...]

    for p in range(PAIRS):
        for j in range(3):
            v = dot(h1, wqkv[block(j * PAIRS + p, PAIR), :], NT) + bqkv_ref[j:j + 1, block(p, PAIR)]
            v = v.astype(BF16)
            if j < 2:
                v = v.astype(F32)
                v = (v * rope_ref[0] + pltpu.roll(v, PAIR - ROT_HALF, 1) * rope_ref[1]
                     + pltpu.roll(v, ROT_HALF, 1) * rope_ref[2]).astype(BF16)
            qkv_scr[j, :, block(p, PAIR)] = v

    lane = lax.broadcasted_iota(jnp.int32, (HALF, PAIR), 1)
    causal = lax.broadcasted_iota(jnp.int32, (HALF, HALF), 0) >= lax.broadcasted_iota(jnp.int32, (HALF, HALF), 1)
    heads = (lane < HD, lane >= HD)
    zero = jnp.zeros((HALF, PAIR), BF16)

    def only(v, hh):
        return jnp.concatenate([jnp.where(heads[hh], v[block(i, HALF)], zero) for i in range(v.shape[0] // HALF)], axis=0)

    def rope_back(g, rows):
        g = rnd(g * HD ** -0.5)
        return (g * rope_ref[0, rows] + pltpu.roll(g * rope_ref[1, rows], ROT_HALF, 1)
                + pltpu.roll(g * rope_ref[2, rows], PAIR - ROT_HALF, 1)).astype(BF16)

    class Attention:
        def __init__(self, i):
            p, self.qb = i // 2, i % 2
            self.n, self.slot, self.lanes, self.rows = HALF * (self.qb + 1), self.qb, block(p, PAIR), block(self.qb, HALF)

        def operands(self):
            q, dc = qkv_scr[0, self.rows, self.lanes], dctx_scr[self.rows, self.lanes]
            return q, dc, qkv_scr[1, :self.n, self.lanes], qkv_scr[2, :self.n, self.lanes]

        def one(self):
            q, dc, k, v = self.operands()
            for hh in range(2):
                at = (self.slot, block(hh, HALF), slice(self.n))
                s_scr[at] = dot(only(q, hh), k, NT)
                dp_scr[at] = dot(only(dc, hh), v, NT).astype(BF16)

        def two(self):
            for hh in range(2):
                at = (self.slot, block(hh, HALF), slice(self.n))
                s = s_scr[at]
                diag = jnp.where(causal, s[:, self.n - HALF:], -1e30)
                s = jnp.concatenate([s[:, :HALF], diag], axis=1) if self.qb else diag
                e = jnp.exp2((s - jnp.max(s, axis=-1, keepdims=True)) * (HD ** -0.5 * LOG2E))
                pr = e * (1.0 / jnp.sum(e, axis=-1, keepdims=True))
                pb_scr[at] = pr.astype(BF16)
                dp = dp_scr[at].astype(F32)
                ds_scr[at] = (pr * (dp - jnp.sum(pr * dp, axis=-1, keepdims=True))).astype(BF16)

        def three(self):
            q, dc, k, v = self.operands()
            pb, ds = pb_scr[self.slot, :, :self.n], ds_scr[self.slot, :, :self.n]
            rows, lanes = self.rows, self.lanes
            ctx_scr[rows, lanes] = sum(dot(pb[block(hh, HALF)], only(v, hh)) for hh in range(2)).astype(BF16)
            dqkv_scr[0, rows, lanes] = rope_back(sum(dot(ds[block(hh, HALF)], only(k, hh)) for hh in range(2)), rows)
            dk = dot(ds, jnp.concatenate([only(q, hh) for hh in range(2)], axis=0), TN)
            dv = dot(pb, jnp.concatenate([only(dc, hh) for hh in range(2)], axis=0), TN)
            if not self.qb:
                dk_scr[...] = dk
                dv_scr[...] = dv
                return
            for b in range(2):
                at = block(b, HALF)
                gk, gv = (dk[at], dv[at]) if b else (dk[at] + dk_scr[...], dv[at] + dv_scr[...])
                dqkv_scr[1, at, lanes] = rope_back(gk, at)
                dqkv_scr[2, at, lanes] = gv.astype(BF16)

    class Mlp:
        def __init__(self, i):
            self.i, self.slot, self.cols = i, i % 2, block(i, HALF)

        def one(self):
            a_scr[self.slot] = dot(h2, w1[:, self.cols]) + bfc1_ref[:, self.cols]
            du_scr[self.slot] = dot(cot, w2[self.cols, :], NT).astype(BF16)

        def two(self):
            u, gp = gelu_parts(rnd(a_scr[self.slot]))
            da = (du_scr[self.slot].astype(F32) * gp).astype(BF16)
            u_scr[self.slot] = u.astype(BF16)
            da_scr[self.slot] = da
            gb1_ref[:, self.cols] += row_sums(da.astype(F32))

        def three(self):
            u, da = u_scr[self.slot], da_scr[self.slot]
            m, d = dot(u, w2[self.cols, :]), dot(da, w1[:, self.cols], NT)
            acc_scr[...] = acc_scr[...] + m if self.i else m
            dh2_scr[...] = dh2_scr[...] + d if self.i else d
            half, part = self.i // RING, 2 * S + self.i % RING * HALF
            gw_ref[:, wcol(half, part, HALF)] += dot(h2t_scr[...], da)
            gw_ref[:, wcol(half, part + 2 * S, HALF)] += dot(cott_scr[...], u)

    units = [u for i in range(2 * PAIRS) for u in (Attention(i), Mlp(i))]
    units[0].one()
    for i, u in enumerate(units):
        if i + 1 < len(units):
            units[i + 1].one()
        u.two()
        if i:
            units[i - 1].three()
    units[-1].three()

    dh1_scr[...] = sum(dot(dqkv_scr[j], wqkv[block(j, S), :]) for j in range(3))
    acc_scr[...] += dot(ctx_scr[...], wd[...])
    for half in range(2):
        hs = block(half, HALF)
        for j in range(3):
            gw_ref[:, wcol(half, j * HALF, HALF)] += dot(h1t_scr[...], dqkv_scr[j, :, hs])
        gw_ref[:, wcol(half, 3 * HALF, HALF)] += dot(cott_scr[...], ctx_scr[:, hs])

    n = n_scr[...]
    d1, d2 = rnd(dh1_scr[...]), rnd(dh2_scr[...])
    for i, v in zip((0, 1, 2, 3, 5, 6, 7), (d1 * n, d1, d2 * n, d2, *(dqkv_scr[j].astype(F32) for j in range(3)))):
        gs_ref[i] += row_sums(v)
    gn = d1 * g1 + d2 * g2
    s_scr[0] = cot.astype(F32) + inv_scr[...] * (
        gn - jnp.mean(gn, axis=-1, keepdims=True) - n * jnp.mean(gn * n, axis=-1, keepdims=True))
    low = (xo_ref[0].astype(F32) + xp_ref[0] + (acc_scr[...] + bo)).astype(BF16)
    own_low[slot] = low
    out_buf[slot] = low.astype(F32)
    for k in range(RING):
        gx_buf[slot, k] = s_scr[0, :, pl.ds(pl.multiple_of((z + k) % RING * LANES, LANES), LANES)]
    for k in range(RING):
        gx_copy(step, k).start()
    out_copy(step).start()
    own_store(step).start()

    @pl.when(step > 0)
    def _():
        take_peer(step - 1)

    @pl.when(step == last)
    def _():
        take_peer(step)
        for at in (step - 1, step):
            drain(at)
            peer_store(at).wait()

        @pl.loop(0, last + 1)
        def _(at):
            for k in range(1, RING):
                gx_copy(at, k).wait_recv()


def rope_consts():
    lane = lax.broadcasted_iota(jnp.int32, (S, PAIR), 1) % HD
    inv_freq = ROPE_BASE ** (-(lane % ROT_HALF).astype(F32) / ROT_HALF)
    ang = lax.broadcasted_iota(F32, (S, PAIR), 0) * inv_freq
    sin, low, rot = jnp.sin(ang), lane < ROT_HALF, lane < 2 * ROT_HALF
    return jnp.stack([jnp.where(rot, jnp.cos(ang), 1.0), jnp.where(low, -sin, 0.0), jnp.where(rot & ~low, sin, 0.0)])


def layer_call(*args):
    count = args[0].shape[0]
    vm, hbm = pl.BlockSpec(memory_space=pltpu.VMEM), pl.BlockSpec(memory_space=pl.ANY)
    seq = pl.BlockSpec((1, S, D), lambda i: (i, 0, 0))
    own_seq = pl.BlockSpec((1, S, D), lambda i: (lax.axis_index('tp') * count + i, 0, 0))
    dma = pltpu.SemaphoreType.DMA

    def table(*lead):
        return pltpu.VMEM(lead + (S, D), F32)

    def low(*lead):
        return pltpu.VMEM(lead + (S, D), BF16)
    thin, thin_low, small = pltpu.VMEM((2, S, HALF), F32), pltpu.VMEM((2, S, HALF), BF16), pltpu.VMEM((HALF, PAIR), F32)
    return pl.pallas_call(
        layer_kernel,
        grid=(count,),
        in_specs=[seq, seq, own_seq] + [vm] * 4 + [hbm] * (len(args) - 7),
        out_specs=[hbm] * 2 + [vm] * 3,
        out_shape=[jax.ShapeDtypeStruct((2 * count, S, D), BF16), jax.ShapeDtypeStruct((RING, count * S, LANES), F32),
                   jax.ShapeDtypeStruct((D, 2 * WIDE), F32), jax.ShapeDtypeStruct((ROW, ROW, D), F32), jax.ShapeDtypeStruct((ROW, FF), F32)],
        scratch_shapes=[pltpu.VMEM((3 * S, D), BF16), low(), pltpu.VMEM((D, FF), BF16), pltpu.VMEM((FF, D), BF16)] + [table()] * 4
        + [pltpu.VMEM((S, 1), F32)] + [low()] * 7 + [low(3)] * 2 + [table(2)] + [low(2)] * 3 + [thin] + [thin_low] * 3 + [small] * 2
        + [pltpu.VMEM((2, RING, S, LANES), F32), table(2), table(count)] + [low(2)] * 2
        + [dma((2, RING)), dma((count, RING)), dma((2,)), dma((2,)), dma((count,)), dma((2,)), dma((2,)), dma((16,))],
        compiler_params=pltpu.CompilerParams(dimension_semantics=("arbitrary",), collective_id=1, has_side_effects=True,
                                             vmem_limit_bytes=VMEM_LIMIT),
        cost_estimate=pl.CostEstimate(flops=count * 30_000_000_000, bytes_accessed=60_000_000, transcendentals=0),
        name="layer",
    )(*args)


STEPS, UNROLL = 8, 8
STEP = PAD // STEPS


def table_kernel(half, ids_ref, rows_ref, lo_ref, out_ref, lo_out_ref, acc, acc2, stage, lo_buf, sem, lo_in, lo_sent):
    @pl.loop(0, acc.shape[0] // LANES)
    def _(j):
        for a in (acc, acc2):
            a[pl.ds(pl.multiple_of(j * LANES, LANES), LANES), :] = jnp.zeros((LANES, LANES), F32)
    count, blocks = rows_ref.shape[1], lo_ref.shape[0]
    part = RING // 2 * count // blocks
    per = count // part

    def lo_load(i):
        return pltpu.make_async_copy(lo_ref.at[i], lo_buf.at[i % 2], lo_in.at[i % 2])

    def lo_store(i):
        return pltpu.make_async_copy(lo_buf.at[i % 2], lo_out_ref.at[i], lo_sent.at[i % 2])
    lo_load(0).start()

    @pl.loop(0, blocks)
    def _(i):
        lo_load(i).wait()
        lo_store(i).start()

        @pl.when(i > 0)
        def _():
            lo_store(i - 1).wait()

        @pl.when(i + 1 < blocks)
        def _():
            lo_load(i + 1).start()
        k, first = i // per * 2, i % per * part

        @pl.loop(0, part // UNROLL)
        def _(g):
            t0 = pl.multiple_of(first + g * UNROLL, UNROLL)
            for j in range(UNROLL):
                for a, src in ((acc, k), (acc2, k + 1)):
                    row = pl.ds(ids_ref[src * count + t0 + j], 1)
                    a[row, :] += rows_ref[src, pl.ds(t0 + j, 1), :]
    lo_store(blocks - 1).wait()
    copies = []
    for i in range(2 * STEPS):
        h, c, slot = i // STEPS, i % STEPS, i % 2
        if i > 1:
            copies[i - 2].wait()

        @pl.loop(0, STEP // LANES, unroll=5)
        def _(b):
            at = pl.ds(pl.multiple_of(h * half + c * STEP + b * LANES, ROW), LANES)
            stage[slot, :, pl.ds(pl.multiple_of(b * LANES, LANES), LANES)] = (acc[at, :] + acc2[at, :]).T
        copies.append(pltpu.make_async_copy(stage.at[slot], out_ref.at[h, :, pl.ds(c * STEP, STEP)], sem.at[slot]))
        copies[i].start()
    for c in copies[-2:]:
        c.wait()


def table_call(ids, rows, lo, half):
    hbm, dma = pl.BlockSpec(memory_space=pl.ANY), pltpu.SemaphoreType.DMA((2,))
    return pl.pallas_call(
        functools.partial(table_kernel, half),
        grid_spec=pltpu.PrefetchScalarGridSpec(
            num_scalar_prefetch=1, grid=(), in_specs=[pl.BlockSpec(memory_space=pltpu.VMEM), hbm], out_specs=[hbm] * 2,
            scratch_shapes=[pltpu.VMEM((half + PAD, LANES), F32)] * 2 + [pltpu.VMEM((2, LANES, STEP), F32), pltpu.VMEM((2, S, D), BF16)]
            + [dma] * 3),
        out_shape=[jax.ShapeDtypeStruct((2, LANES, PAD), F32), jax.ShapeDtypeStruct(lo.shape, lo.dtype)],
        compiler_params=pltpu.CompilerParams(vmem_limit_bytes=VMEM_LIMIT),
        cost_estimate=pl.CostEstimate(flops=4_000_000_000, bytes_accessed=34_000_000, transcendentals=0),
        name="table",
    )(ids, rows, lo)


def cut(lo, n):
    first = n // (2 * LANES) * LANES
    return (lo, first), (lo + first, n - first)


def over(lead, body, at=()):
    if not lead:
        return body(at)

    @pl.loop(0, lead[0])
    def _(i):
        over(lead[1:], body, at + (i,))


def add_into(dst, srcs, lead, lo, n):
    def body(at):
        v = dst[at + (slice(None), pl.ds(lo, n))]
        for s in srcs:
            v = v + s[at + (slice(None), pl.ds(0, n))]
        dst[at + (slice(None), pl.ds(lo, n))] = v
    over(lead, body)


def tail_kernel(t_ref, g_ref, e_ref, oute_ref, outw_ref, *scratch):
    tsum, tpeer, gsum, gpeer, send, recv, local = scratch[:7]
    bufs = list(scratch[7:])
    core, dp = lax.axis_index('tp'), lax.axis_index('dp')
    pos = {'z': dp // (RING * RING), 'y': dp // RING % RING, 'x': dp % RING}
    stride = {'z': RING * RING, 'y': RING, 'x': 1}

    def shift(axis, k):
        return (pos[axis] + k) % RING

    def device(axis, k):
        return (core, dp + (shift(axis, k) - pos[axis]) * stride[axis])
    peer = (1 - core, dp)

    barrier = pltpu.get_barrier_semaphore()
    near = [peer] + [device(axis, k) for axis in 'zyx' for k in (1, RING - 1)]
    for who in near:
        pl.semaphore_signal(barrier, inc=1, device_id=who, device_id_type=MESH)
    pl.semaphore_wait(barrier, len(near))

    used = [0, 0]

    def remote(src, dst, who):
        i = used[0]
        used[0] += 1
        c = pltpu.make_async_remote_copy(src, dst, send.at[i], recv.at[i], device_id=who, device_id_type=MESH)
        c.start()
        return c

    def load(src, dst):
        i = used[1]
        used[1] += 1
        c = pltpu.make_async_copy(src, dst, local.at[i])
        c.start()
        return c
    sent = []

    full = pl.ds(0, COLOR)
    rest = pl.ds(COLOR, COLOR)
    wide, extra, far = pl.ds(0, WIDE), pl.ds(WIDE, EXTRA), pl.ds(WIDE, WIDE)
    every = slice(None)
    views = {
        'a': ('y', lambda i: (i, every, every, full)),
        'b': ('x', lambda i: (every, i, every, rest)),
        'g': ('z', lambda i: (i, every, every, every, wide)),
    }
    pend = {}
    pend['e'] = [remote(e_ref.at[1], gpeer.at[every, every, every, every, extra], peer),
                 load(e_ref.at[0], gsum.at[every, every, every, every, extra])]
    for k in (2, 1, RING - 1, 0):
        for name, (axis, view) in views.items():
            at = view(shift(axis, k))
            if name == 'g':
                there = at[:-1] + (far,)
                pend[name, k] = [remote(g_ref.at[there], gpeer.at[at], peer), load(g_ref.at[at], gsum.at[at])]
            else:
                pend[name, k] = [remote(t_ref.at[(1,) + at], tpeer.at[at], peer), load(t_ref.at[(0,) + at], tsum.at[at])]

    def arrive(key):
        out, here = pend[key]
        sent.append(out)
        out.wait_recv()
        here.wait()

    def ready(name, k):
        arrive((name, k))
        axis, _ = views[name]
        i = shift(axis, k)
        if name == 'a':
            add_into(tsum.at[i], [tpeer.at[i]], (RING,), 0, COLOR)
        elif name == 'b':
            add_into(tsum.at[:, i, :, rest], [tpeer.at[:, i, :, rest]], (RING,), 0, COLOR)
        else:
            add_into(gsum.at[i], [gpeer.at[i]], (RING, RING), 0, GCOLS)

    class Stage:
        def __init__(self, axis, piece, lead, lo, n, need=None):
            self.axis, self.piece, self.lead, self.lo, self.n, self.need = axis, piece, lead, lo, n, need
            self.halves = cut(lo, n)
            self.near = [bufs.pop(0), bufs.pop(0)]
            self.last = [bufs.pop(0), bufs.pop(0)]

        def view(self, k, lo, n):
            return self.piece(shift(self.axis, k)).at[(every,) * (len(self.lead) + 1) + (pl.ds(lo, n),)]

        def want(self, k):
            if self.need:
                ready(self.need, k)

        def first(self):
            self.want(2)
            self.c1 = [remote(self.view(2, *self.halves[s]), self.near[s], device(self.axis, k))
                       for s, k in enumerate((1, RING - 1))]

        def second(self):
            self.want(1)
            self.want(RING - 1)
            self.c2 = []
            for s, k in enumerate((1, RING - 1)):
                self.c1[s].wait_recv()
                add_into(self.piece(shift(self.axis, k)), [self.near[s]], self.lead, *self.halves[s])
                self.c2.append(remote(self.view(k, self.lo, self.n), self.last[s], device(self.axis, k)))

        def finish(self):
            self.want(0)
            for c in self.c2:
                c.wait_recv()
            add_into(self.piece(shift(self.axis, 0)), self.last, self.lead, self.lo, self.n)
            sent.extend(self.c1 + self.c2)

    py, px, pz = pos['y'], pos['x'], pos['z']
    one, two = (RING,), (RING, RING)
    a1 = Stage('y', lambda i: tsum.at[i], one, 0, COLOR, 'a')
    b1 = Stage('x', lambda i: tsum.at[:, i], one, COLOR, COLOR, 'b')
    g1 = Stage('z', lambda i: gsum.at[i], two, 0, GCOLS, 'g')
    a2 = Stage('x', lambda i: tsum.at[py, i], (), 0, COLOR)
    b2 = Stage('y', lambda i: tsum.at[i, px], (), COLOR, COLOR)
    (c0, cn), (d0, dn) = cut(0, GCOLS)
    c1 = Stage('y', lambda i: gsum.at[pz, i], one, c0, cn)
    d1 = Stage('x', lambda i: gsum.at[pz, :, i], one, d0, dn)
    c2 = Stage('x', lambda i: gsum.at[pz, py, i], (), c0, cn)
    d2 = Stage('y', lambda i: gsum.at[pz, i, px], (), d0, dn)

    a1.first()
    b1.first()
    arrive('e')
    g1.first()
    for phase in ('second', 'finish'):
        for s in (a1, b1, g1):
            getattr(s, phase)()
            if phase == 'finish':
                for t in {a1: (a2,), b1: (b2,), g1: (c1, d1)}[s]:
                    t.first()
    for s in (a2, b2, c1, d1):
        s.second()
    for s in (a2, b2):
        s.finish()
    oute_ref[...] = tsum[py, px, :, 0:oute_ref.shape[1]]
    for s, t in ((c1, c2), (d1, d2)):
        s.finish()
        t.first()
    for s in (c2, d2):
        s.second()
    for s in (c2, d2):
        s.finish()
    outw_ref[...] = gsum[pz, py, px]
    for c in sent:
        c.wait_send()


def tail_call(t, g, e, rows):
    def ring_bufs(lead, n):
        (_, p), (_, q) = cut(0, n)
        return [pltpu.VMEM(lead + (ROW, w), F32) for w in (p, q, n, n)]
    (_, cn), (_, dn) = cut(0, GCOLS)
    one, two, three = (RING,), (RING,) * 2, (RING,) * 3
    bufs = sum((ring_bufs(*b) for b in ((one, COLOR), (one, COLOR), (two, GCOLS), ((), COLOR), ((), COLOR),
                                        (one, cn), (one, dn), ((), cn), ((), dn))), [])
    dma = pltpu.SemaphoreType.DMA
    hbm = pl.BlockSpec(memory_space=pl.ANY)
    vm = pl.BlockSpec(memory_space=pltpu.VMEM)
    return pl.pallas_call(
        tail_kernel,
        in_specs=[hbm] * 3, out_specs=[vm] * 2,
        out_shape=[jax.ShapeDtypeStruct((ROW, rows), F32), jax.ShapeDtypeStruct((ROW, GCOLS), F32)],
        scratch_shapes=[pltpu.VMEM(two + (ROW, PAD), F32)] * 2 + [pltpu.VMEM(three + (ROW, GCOLS), F32)] * 2
        + [dma((64,)), dma((64,)), dma((16,))] + bufs,
        compiler_params=pltpu.CompilerParams(collective_id=0, has_side_effects=True, vmem_limit_bytes=VMEM_LIMIT),
        name="tail",
    )(t, g, e)


def solution(mesh):
    tp, dp, no = 'tp', 'dp', None
    one, vec_dp, both = P(no), P(dp), P((tp, dp))
    arg_specs = (P(dp, no), P(tp, no), one, one, one, one, P(no, tp, no, no), P(tp, no, no), P(tp, no, no), one, P(no, tp), P(tp), P(tp, no), one, P(dp, no, no))
    out_specs = (P(dp, no, no), P(tp, dp), vec_dp, vec_dp, vec_dp, vec_dp, P(dp, tp, no, no), both, P(tp, no, dp), vec_dp, P(dp, tp), both, P(tp, dp), vec_dp)
    chips = mesh.shape[dp]
    plane = chips // RING

    def swap(v):
        return lax.ppermute(v, tp, [(0, 1), (1, 0)])

    def z_shift(v, k):
        return lax.ppermute(v, dp, [(i, (i + k * plane) % chips) for i in range(chips)]) if k else v

    def device_step(token_ids, embed_table, ln1_gain, ln1_bias, ln2_gain, ln2_bias, w_qkv, b_qkv, w_dense, b_dense, w_fc1, b_fc1, w_fc2, b_fc2, cotangent):
        core = lax.axis_index(tp)
        vocab_local = embed_table.shape[0]
        seqs = token_ids.shape[0] // 2
        f = lambda v: v.astype(F32)

        wq_own = w_qkv.transpose(2, 1, 3, 0).reshape(3 * HALF, D)
        wd_own = w_dense.reshape(HALF, D)
        rows_peer = swap(f(jnp.concatenate([wq_own, wd_own, w_fc2], axis=0)))
        fc1_peer = swap(f(w_fc1))
        b_peer = swap(f(jnp.concatenate([b_qkv.reshape(-1), b_fc1])))
        bqkv = jnp.concatenate([f(b_qkv), b_peer[:b_qkv.size].reshape(b_qkv.shape)], axis=0).transpose(1, 0, 2).reshape(3, D)
        bfc1 = jnp.concatenate([f(b_fc1), b_peer[b_qkv.size:]]).reshape(1, FF)
        vec = jnp.stack([f(ln1_gain), f(ln1_bias), f(ln2_gain), f(ln2_bias), f(b_dense) + f(b_fc2)])

        def lookup(ids):
            local = ids - core * vocab_local
            ok = (local >= 0) & (local < vocab_local)
            got = jnp.take(embed_table, jnp.where(ok, local, 0), axis=0)
            return jnp.where(ok[..., None], got, jnp.zeros_like(got))

        ids_own = lax.dynamic_slice_in_dim(token_ids, core * seqs, seqs, 0)
        ids_peer = lax.dynamic_slice_in_dim(token_ids, (1 - core) * seqs, seqs, 0)
        x_peer = swap(f(lookup(ids_peer)))
        x_own = lookup(ids_own)
        flat = ids_own.reshape(-1)
        ids = jnp.concatenate([z_shift(flat, k) for k in range(RING)]) - core * vocab_local

        args = (x_own, x_peer, cotangent, vec, bqkv, bfc1, rope_consts(), wq_own, wd_own, w_fc1, w_fc2, rows_peer, fc1_peer)
        layer_out, rows, grad_w, grad_s, grad_b1 = layer_call(*args)

        dense, layer_out = table_call(jnp.where(ids < 0, ids + 2 * vocab_local, ids), rows, layer_out, vocab_local)

        small = jnp.sum(grad_s, axis=1)
        norms = small[:5].reshape(5, chips, ROW).transpose(1, 0, 2).reshape(chips, 5 * ROW)
        grad_bq = small[5:].reshape(3, 2, PAIRS, HD).transpose(1, 2, 0, 3).reshape(2, chips, -1)
        grad_bf = jnp.sum(grad_b1, axis=0).reshape(2, chips, -1)
        extra = jnp.concatenate([jnp.stack([norms, norms]), grad_bq, grad_bf], axis=2)
        ends = (5 * ROW, 5 * ROW + grad_bq.shape[2], extra.shape[2])
        extra = jnp.pad(extra[:, :, None, :], ((0, 0), (0, 0), (0, ROW - 1), (0, EXTRA - ends[2])))
        ring3 = (RING,) * 3
        sum_embed, total = tail_call(dense.reshape(2, RING, RING, ROW, PAD), grad_w.reshape(ring3 + (ROW, 2 * WIDE)),
                                     extra.reshape((2,) + ring3 + (ROW, EXTRA)), vocab_local)
        qkv, wide = 3 * HALF, 4 * HALF
        sum_wqkv = total[:, :qkv].reshape(ROW, 3, PAIRS, HD).transpose(0, 2, 1, 3)
        sum_wdense = total[:, qkv:wide].reshape(ROW, PAIRS, HD).transpose(1, 2, 0)
        sum_wfc1, sum_wfc2 = total[:, wide:2 * wide], total[:, 2 * wide:WIDE].T
        last = total[0, WIDE:]
        n1g, n1b, n2g, n2b, bias = last[:ends[0]].reshape(5, ROW)
        return (layer_out, sum_embed.T, n1g, n1b, n2g, n2b, sum_wqkv, last[ends[0]:ends[1]], sum_wdense, bias, sum_wfc1,
                last[ends[1]:ends[2]], sum_wfc2, bias)

    return jax.shard_map(device_step, mesh=mesh, in_specs=arg_specs, out_specs=out_specs, check_vma=False)
```

```python
import functools
import math
import jax
import jax.numpy as jnp
from jax import lax
from jax.experimental import pallas as pl
from jax.experimental.pallas import tpu as pltpu
from jax.sharding import PartitionSpec as P

F32, BF16 = jnp.float32, jnp.bfloat16
NN = (((1,), (0,)), ((), ()))
NT = (((1,), (1,)), ((), ()))
TN = (((0,), (0,)), ((), ()))
S, D, FF, HEADS, HD = 512, 512, 2048, 8, 64
PAIR, HALF, PAIRS, FF_STEPS, ROT_HALF = 2 * HD, S // 2, HEADS // 2, FF // S, HD // 8
EPS, ROPE_BASE = 1e-5, 10000.0
LOG2E = 1.4426950408889634
SQRT_HALF, INV_SQRT_2PI = 0.7071067811865476, 0.3989422804014327
RB = 128
VMEM_LIMIT = 67_000_000
ROW, LANES, RING = 8, 128, 4
PAD = 25600
COLOR = PAD // 2
PARTS = 2
WIDE, EXTRA = 3072, 128
GCOLS = WIDE + EXTRA
MESH = pl.DeviceIdType.MESH


def dot(a, b, dims=NN):
    return lax.dot_general(a, b, dims, preferred_element_type=F32)


def rnd(v):
    return v.astype(BF16).astype(F32)


def gelu_parts(a):
    phi = 0.5 + 0.5 * lax.erf(a * SQRT_HALF)
    return a * phi, phi + a * jnp.exp2(a * a * (-0.5 * LOG2E)) * INV_SQRT_2PI


def block(i, n):
    return slice(i * n, i * n + n)


def row_sums(v):
    return jnp.sum(v.reshape(v.shape[0] // ROW, ROW, v.shape[1]), axis=0)


def wcol(half, part, width):
    return slice(half * WIDE + part, half * WIDE + part + width)


def look_up_kernel(codes_ref, table_ref, peer_ref, own_ref, table, sem):
    step = pl.program_id(0)
    half = pl.num_programs(0) * S

    @pl.when(step == 0)
    def _():
        rows = table_ref.shape[0]
        load = pltpu.make_async_copy(table_ref, table.at[:rows], sem)
        load.start()
        table[rows:, :] = jnp.zeros((ROW, D), BF16)
        load.wait()
    sub = lax.broadcasted_iota(jnp.int32, (ROW, D), 0)

    def look_up(first):
        got = jnp.zeros((ROW, D), F32)
        for j in range(ROW):
            at = codes_ref[first + j]
            rows = table[pl.ds(pl.multiple_of(at & -ROW, ROW), ROW), :].astype(F32)
            got = jnp.where(sub == j, pltpu.roll(rows, (j - at) & (ROW - 1), 0), got)
        return got

    for k, dst in enumerate((own_ref, peer_ref)):
        @pl.loop(0, S // ROW, unroll=2)
        def _(g):
            t0 = pl.multiple_of(g * ROW, ROW)
            dst[0, pl.ds(t0, ROW), :] = look_up(k * half + step * S + t0).astype(dst.dtype)


def look_up_call(codes, table):
    seqs = codes.size // (2 * S)
    seq = pl.BlockSpec((1, S, D), lambda i, _: (i, 0, 0))
    return pl.pallas_call(
        look_up_kernel,
        grid_spec=pltpu.PrefetchScalarGridSpec(
            num_scalar_prefetch=1, grid=(seqs,), in_specs=[pl.BlockSpec(memory_space=pl.ANY)], out_specs=[seq] * 2,
            scratch_shapes=[pltpu.VMEM((table.shape[0] + ROW, D), BF16), pltpu.SemaphoreType.DMA]),
        out_shape=[jax.ShapeDtypeStruct((seqs, S, D), t) for t in (F32, BF16)],
        compiler_params=pltpu.CompilerParams(dimension_semantics=("arbitrary",), vmem_limit_bytes=VMEM_LIMIT),
        cost_estimate=pl.CostEstimate(flops=40_000_000_000, bytes_accessed=40_000_000, transcendentals=0),
        name="look_up",
    )(codes, table)


def layer_kernel(xo_ref, cot_ref, vec_ref, bo_ref, bp_ref, rope_ref, xs_ref, qo_ref, do_ref, fo_ref, to_ref, rp_ref, fp_ref,
                 out_ref, rows_ref, xin_ref, gw_out, gs_ref, gb1_ref,
                 gw_ref, wqkv, wd, w1, w2, n_scr, acc_scr, dh2_scr, dh1_scr, inv_scr, h1_scr, h2_scr, h1t_scr, h2t_scr, cott_scr, dctx_scr, ctx_scr,
                 qkv_scr, dqkv_scr, s_scr, dp_scr, pb_scr, ds_scr, a_scr, du_scr, u_scr, da_scr, dk_scr, dv_scr,
                 xp_buf, gx_buf, out_buf, peer_buf, own_low, peer_low, x_send, x_recv, x_load, gx_send, gx_recv, gx_local, out_send, out_recv, own_sem, peer_sem, init_sem):
    step, last = pl.program_id(0), pl.num_programs(0) - 1
    slot = step % 2
    core, chip = lax.axis_index('tp'), lax.axis_index('dp')
    chips = lax.axis_size('dp')
    plane = chips // RING
    z, peer = chip // plane, (1 - core, chip)

    def z_device(k):
        return (core, (chip + k * plane) % chips)

    def x_copy(at):
        return pltpu.make_async_remote_copy(xs_ref.at[at], xin_ref.at[at], x_send.at[at], x_recv.at[at], device_id=peer, device_id_type=MESH)

    def x_take(at):
        return pltpu.make_async_copy(xin_ref.at[at], xp_buf.at[at % 2], x_load.at[at % 2])

    @pl.when(step == 0)
    def _():
        barrier = pltpu.get_barrier_semaphore()
        near = [peer] + [z_device(k) for k in range(1, RING)]
        for who in near:
            pl.semaphore_signal(barrier, inc=1, device_id=who, device_id_type=MESH)
        pl.semaphore_wait(barrier, len(near))

        @pl.loop(0, last + 1)
        def _(at):
            x_copy(at).start()
        for dst in (gw_ref, gs_ref, gb1_ref):
            dst[...] = jnp.zeros_like(dst)
        n = FF // 2
        moves = [(qo_ref.at[block(j, HALF)], wqkv.at[block(2 * j, HALF)]) for j in range(3)]
        moves += [(do_ref, wd.at[:HALF]), (to_ref, w2.at[:n]), (fo_ref, w1.at[:, :n])]
        tables = (n_scr, acc_scr, dh2_scr, dh1_scr, s_scr.at[0], s_scr.at[1])
        parts = [rp_ref.at[block(i, S)] for i in range(RING)] + [fp_ref.at[:, block(i, S)] for i in range(2)]
        copies = [pltpu.make_async_copy(src, dst, init_sem.at[i]) for i, (src, dst) in enumerate(moves + list(zip(parts, tables)))]
        for c in copies:
            c.start()
        for c in copies:
            c.wait()
        for j in range(3):
            wqkv[block(2 * j + 1, HALF), :] = tables[j // 2][block(j % 2, HALF), :].astype(BF16)
        wd[HALF:, :] = tables[1][HALF:, :].astype(BF16)
        for i in range(2):
            w2[block(2 + i, S), :] = tables[2 + i][...].astype(BF16)
            w1[:, block(2 + i, S)] = tables[RING + i][...].astype(BF16)

        x_copy(0).wait_recv()
        x_take(0).start()

    x_take(step).wait()

    @pl.when(step < last)
    def _():
        x_copy(step + 1).wait_recv()
        x_take(step + 1).start()

    def gx_copy(at, k):
        rows = pl.ds(pl.multiple_of(at * S, S), S)
        src, dst = gx_buf.at[at % 2, k], rows_ref.at[k, rows]
        if k:
            return pltpu.make_async_remote_copy(src, dst, gx_send.at[at % 2, k], gx_recv.at[at, k], device_id=z_device(k), device_id_type=MESH)
        return pltpu.make_async_copy(src, dst, gx_local.at[at % 2])

    def out_copy(at):
        return pltpu.make_async_remote_copy(out_buf.at[at % 2], peer_buf.at[at], out_send.at[at % 2], out_recv.at[at], device_id=peer, device_id_type=MESH)

    def own_store(at):
        return pltpu.make_async_copy(own_low.at[at % 2], out_ref.at[core * (last + 1) + at], own_sem.at[at % 2])

    def peer_store(at):
        return pltpu.make_async_copy(peer_low.at[at % 2], out_ref.at[(1 - core) * (last + 1) + at], peer_sem.at[at % 2])

    def drain(at):
        gx_copy(at, 0).wait()
        for k in range(1, RING):
            gx_copy(at, k).wait_send()
        out_copy(at).wait_send()
        own_store(at).wait()

    def take_peer(at):
        out_copy(at).wait_recv()

        @pl.when(at > 1)
        def _():
            peer_store(at - 2).wait()
        peer_low[at % 2] = peer_buf[at].astype(BF16)
        peer_store(at).start()

    @pl.when(step > 1)
    def _():
        drain(step - 2)

    cot = cot_ref[0]
    g1, b1, g2, b2, bd, bf = (vec_ref[i:i + 1, :].astype(F32) for i in range(6))
    bo = bd + bf

    def bias(row, i, n):
        width = HALF if row < 3 else FF // 2
        src, i = (bo_ref, i) if i < width // n else (bp_ref, i - width // n)
        return src[row:row + 1, block(i, n)]

    dctx_scr[...] = dot(cot, wd[...], NT).astype(BF16)
    cott_scr[...] = cot.T
    x = xo_ref[0].astype(F32) + xp_buf[slot]
    cen = x - jnp.mean(x, axis=-1, keepdims=True)
    inv = lax.rsqrt(jnp.mean(cen * cen, axis=-1, keepdims=True) + EPS)
    n = cen * inv
    n_scr[...] = n
    inv_scr[...] = inv
    h1_scr[...] = (n * g1 + b1).astype(BF16)
    h2_scr[...] = (n * g2 + b2).astype(BF16)
    gs_ref[4] += row_sums(cot.astype(F32))
    h1t_scr[...] = h1_scr[...].T
    h2t_scr[...] = h2_scr[...].T
    h1, h2 = h1_scr[...], h2_scr[...]

    for p in range(PAIRS):
        for j in range(3):
            v = dot(h1, wqkv[block(j * PAIRS + p, PAIR), :], NT) + bias(j, p, PAIR)
            v = v.astype(BF16)
            if j < 2:
                v = v.astype(F32)
                v = (v * rope_ref[0] + pltpu.roll(v, PAIR - ROT_HALF, 1) * rope_ref[1]
                     + pltpu.roll(v, ROT_HALF, 1) * rope_ref[2]).astype(BF16)
            qkv_scr[j, :, block(p, PAIR)] = v

    lane = lax.broadcasted_iota(jnp.int32, (HALF, PAIR), 1)
    causal = lax.broadcasted_iota(jnp.int32, (HALF, HALF), 0) >= lax.broadcasted_iota(jnp.int32, (HALF, HALF), 1)
    heads = (lane < HD, lane >= HD)
    zero = jnp.zeros((HALF, PAIR), BF16)

    def only(v, hh):
        return jnp.concatenate([jnp.where(heads[hh], v[block(i, HALF)], zero) for i in range(v.shape[0] // HALF)], axis=0)

    def rope_back(g, rows):
        g = rnd(g * HD ** -0.5)
        return (g * rope_ref[0, rows] + pltpu.roll(g * rope_ref[1, rows], ROT_HALF, 1)
                + pltpu.roll(g * rope_ref[2, rows], PAIR - ROT_HALF, 1)).astype(BF16)

    class Attention:
        def __init__(self, i):
            p, self.qb = i // 2, i % 2
            self.n, self.slot, self.lanes, self.rows = HALF * (self.qb + 1), self.qb, block(p, PAIR), block(self.qb, HALF)

        def operands(self):
            q, dc = qkv_scr[0, self.rows, self.lanes], dctx_scr[self.rows, self.lanes]
            return q, dc, qkv_scr[1, :self.n, self.lanes], qkv_scr[2, :self.n, self.lanes]

        def one(self):
            q, dc, k, v = self.operands()
            for hh in range(2):
                at = (self.slot, block(hh, HALF), slice(self.n))
                s_scr[at] = dot(only(q, hh), k, NT)
                dp_scr[at] = dot(only(dc, hh), v, NT).astype(BF16)

        def two(self):
            for hh in range(2):
                at = (self.slot, block(hh, HALF), slice(self.n))
                s = s_scr[at]
                diag = jnp.where(causal, s[:, self.n - HALF:], -1e30)
                s = jnp.concatenate([s[:, :HALF], diag], axis=1) if self.qb else diag
                e = jnp.exp2((s - jnp.max(s, axis=-1, keepdims=True)) * (HD ** -0.5 * LOG2E))
                pr = e * (1.0 / jnp.sum(e, axis=-1, keepdims=True))
                pb_scr[at] = pr.astype(BF16)
                dp = dp_scr[at].astype(F32)
                ds_scr[at] = (pr * (dp - jnp.sum(pr * dp, axis=-1, keepdims=True))).astype(BF16)

        def three(self):
            q, dc, k, v = self.operands()
            pb, ds = pb_scr[self.slot, :, :self.n], ds_scr[self.slot, :, :self.n]
            rows, lanes = self.rows, self.lanes
            ctx_scr[rows, lanes] = sum(dot(pb[block(hh, HALF)], only(v, hh)) for hh in range(2)).astype(BF16)
            dqkv_scr[0, rows, lanes] = rope_back(sum(dot(ds[block(hh, HALF)], only(k, hh)) for hh in range(2)), rows)
            dk = dot(ds, jnp.concatenate([only(q, hh) for hh in range(2)], axis=0), TN)
            dv = dot(pb, jnp.concatenate([only(dc, hh) for hh in range(2)], axis=0), TN)
            if not self.qb:
                dk_scr[...] = dk
                dv_scr[...] = dv
                return
            for b in range(2):
                at = block(b, HALF)
                gk, gv = (dk[at], dv[at]) if b else (dk[at] + dk_scr[...], dv[at] + dv_scr[...])
                dqkv_scr[1, at, lanes] = rope_back(gk, at)
                dqkv_scr[2, at, lanes] = gv.astype(BF16)

    class Mlp:
        def __init__(self, i):
            self.i, self.slot, self.cols = i, i % 2, block(i, HALF)

        def one(self):
            a_scr[self.slot] = dot(h2, w1[:, self.cols]) + bias(3, self.i, HALF)
            du_scr[self.slot] = dot(cot, w2[self.cols, :], NT).astype(BF16)

        def two(self):
            u, gp = gelu_parts(rnd(a_scr[self.slot]))
            da = (du_scr[self.slot].astype(F32) * gp).astype(BF16)
            u_scr[self.slot] = u.astype(BF16)
            da_scr[self.slot] = da
            gb1_ref[:, self.cols] += row_sums(da.astype(F32))

        def three(self):
            u, da = u_scr[self.slot], da_scr[self.slot]
            m, d = dot(u, w2[self.cols, :]), dot(da, w1[:, self.cols], NT)
            acc_scr[...] = acc_scr[...] + m if self.i else m
            dh2_scr[...] = dh2_scr[...] + d if self.i else d
            half, part = self.i // RING, 2 * S + self.i % RING * HALF
            gw_ref[:, wcol(half, part, HALF)] += dot(h2t_scr[...], da)
            gw_ref[:, wcol(half, part + 2 * S, HALF)] += dot(cott_scr[...], u)

    units = [u for i in range(2 * PAIRS) for u in (Attention(i), Mlp(i))]
    units[0].one()
    for i, u in enumerate(units):
        if i + 1 < len(units):
            units[i + 1].one()
        u.two()
        if i:
            units[i - 1].three()
    units[-1].three()

    dh1_scr[...] = sum(dot(dqkv_scr[j], wqkv[block(j, S), :]) for j in range(3))
    acc_scr[...] += dot(ctx_scr[...], wd[...])
    for half in range(2):
        hs = block(half, HALF)
        for j in range(3):
            gw_ref[:, wcol(half, j * HALF, HALF)] += dot(h1t_scr[...], dqkv_scr[j, :, hs])
        gw_ref[:, wcol(half, 3 * HALF, HALF)] += dot(cott_scr[...], ctx_scr[:, hs])

    n = n_scr[...]
    d1, d2 = rnd(dh1_scr[...]), rnd(dh2_scr[...])
    for i, v in zip((0, 1, 2, 3, 5, 6, 7), (d1 * n, d1, d2 * n, d2, *(dqkv_scr[j].astype(F32) for j in range(3)))):
        gs_ref[i] += row_sums(v)
    gn = d1 * g1 + d2 * g2
    s_scr[0] = cot.astype(F32) + inv_scr[...] * (
        gn - jnp.mean(gn, axis=-1, keepdims=True) - n * jnp.mean(gn * n, axis=-1, keepdims=True))
    low = (xo_ref[0].astype(F32) + xp_buf[slot] + (acc_scr[...] + bo)).astype(BF16)
    own_low[slot] = low
    out_buf[slot] = low.astype(F32)
    for k in range(RING):
        gx_buf[slot, k] = s_scr[0, :, pl.ds(pl.multiple_of((z + k) % RING * LANES, LANES), LANES)]
    for k in (2, 1, 3, 0):
        gx_copy(step, k).start()
    out_copy(step).start()
    own_store(step).start()

    @pl.when(step > 0)
    def _():
        take_peer(step - 1)

    @pl.when(step == last)
    def _():
        save = pltpu.make_async_copy(gw_ref, gw_out, init_sem.at[0])
        save.start()
        take_peer(step)
        for at in (step - 1, step):
            drain(at)
            peer_store(at).wait()

        @pl.loop(0, last + 1)
        def _(at):
            x_copy(at).wait_send()
            for k in range(1, RING):
                gx_copy(at, k).wait_recv()
        save.wait()


def rope_consts():
    lane = lax.broadcasted_iota(jnp.int32, (S, PAIR), 1) % HD
    inv_freq = ROPE_BASE ** (-(lane % ROT_HALF).astype(F32) / ROT_HALF)
    ang = lax.broadcasted_iota(F32, (S, PAIR), 0) * inv_freq
    sin, low, rot = jnp.sin(ang), lane < ROT_HALF, lane < 2 * ROT_HALF
    return jnp.stack([jnp.where(rot, jnp.cos(ang), 1.0), jnp.where(low, -sin, 0.0), jnp.where(rot & ~low, sin, 0.0)])


def layer_call(*args):
    count = args[0].shape[0]
    vm, hbm = pl.BlockSpec(memory_space=pltpu.VMEM), pl.BlockSpec(memory_space=pl.ANY)
    seq = pl.BlockSpec((1, S, D), lambda i: (i, 0, 0))
    own_seq = pl.BlockSpec((1, S, D), lambda i: (lax.axis_index('tp') * count + i, 0, 0))
    dma = pltpu.SemaphoreType.DMA

    def table(*lead):
        return pltpu.VMEM(lead + (S, D), F32)

    def low(*lead):
        return pltpu.VMEM(lead + (S, D), BF16)
    thin, thin_low, small = pltpu.VMEM((2, S, HALF), F32), pltpu.VMEM((2, S, HALF), BF16), pltpu.VMEM((HALF, PAIR), F32)
    return pl.pallas_call(
        layer_kernel,
        grid=(count,),
        in_specs=[seq, own_seq] + [vm] * 4 + [hbm] * (len(args) - 6),
        out_specs=[hbm] * 4 + [vm] * 2,
        out_shape=[jax.ShapeDtypeStruct((2 * count, S, D), BF16), jax.ShapeDtypeStruct((RING, count * S, LANES), F32), jax.ShapeDtypeStruct((count, S, D), F32),
                   jax.ShapeDtypeStruct((D, 2 * WIDE), F32), jax.ShapeDtypeStruct((ROW, ROW, D), F32), jax.ShapeDtypeStruct((ROW, FF), F32)],
        scratch_shapes=[pltpu.VMEM((D, 2 * WIDE), F32), pltpu.VMEM((3 * S, D), BF16), low(), pltpu.VMEM((D, FF), BF16), pltpu.VMEM((FF, D), BF16)] + [table()] * 4
        + [pltpu.VMEM((S, 1), F32)] + [low()] * 7 + [low(3)] * 2 + [table(2)] + [low(2)] * 3 + [thin] + [thin_low] * 3 + [small] * 2
        + [table(2), pltpu.VMEM((2, RING, S, LANES), F32), table(2), table(count)] + [low(2)] * 2
        + [dma((count,)), dma((count,)), dma((2,)), dma((2, RING)), dma((count, RING)), dma((2,)), dma((2,)), dma((count,)), dma((2,)), dma((2,)), dma((16,))],
        compiler_params=pltpu.CompilerParams(dimension_semantics=("arbitrary",), collective_id=1, has_side_effects=True,
                                             vmem_limit_bytes=VMEM_LIMIT),
        cost_estimate=pl.CostEstimate(flops=count * 30_000_000_000, bytes_accessed=60_000_000, transcendentals=0),
        name="layer",
    )(*args)


STEPS, UNROLL = 8, 8
STEP = PAD // STEPS


def table_kernel(half, ids_ref, rows_hbm, lo_ref, out_ref, lo_out_ref, rows_ref, acc, acc2, stage, lo_buf, sem, lo_in, lo_sent):
    load = pltpu.make_async_copy(rows_hbm, rows_ref, sem.at[0])
    load.start()

    @pl.loop(0, acc.shape[0] // LANES)
    def _(j):
        for a in (acc, acc2):
            a[pl.ds(pl.multiple_of(j * LANES, LANES), LANES), :] = jnp.zeros((LANES, LANES), F32)
    count, blocks = rows_ref.shape[1], lo_ref.shape[0]
    part = RING // 2 * count // blocks
    per = count // part

    def lo_load(i):
        return pltpu.make_async_copy(lo_ref.at[i], lo_buf.at[i % 2], lo_in.at[i % 2])

    def lo_store(i):
        return pltpu.make_async_copy(lo_buf.at[i % 2], lo_out_ref.at[i], lo_sent.at[i % 2])
    lo_load(0).start()
    load.wait()

    @pl.loop(0, blocks)
    def _(i):
        lo_load(i).wait()
        lo_store(i).start()

        @pl.when(i > 0)
        def _():
            lo_store(i - 1).wait()

        @pl.when(i + 1 < blocks)
        def _():
            lo_load(i + 1).start()
        k, first = i // per * 2, i % per * part

        @pl.loop(0, part // UNROLL)
        def _(g):
            t0 = pl.multiple_of(first + g * UNROLL, UNROLL)
            for j in range(UNROLL):
                for a, src in ((acc, k), (acc2, k + 1)):
                    row = pl.ds(ids_ref[src * count + t0 + j], 1)
                    a[row, :] += rows_ref[src, pl.ds(t0 + j, 1), :]
    lo_store(blocks - 1).wait()
    copies = []
    for i in range(2 * STEPS):
        h, c, slot = i // STEPS, i % STEPS, i % 2
        if i > 1:
            copies[i - 2].wait()

        @pl.loop(0, STEP // LANES, unroll=5)
        def _(b):
            at = pl.ds(pl.multiple_of(h * half + c * STEP + b * LANES, ROW), LANES)
            stage[slot, :, pl.ds(pl.multiple_of(b * LANES, LANES), LANES)] = (acc[at, :] + acc2[at, :]).T
        copies.append(pltpu.make_async_copy(stage.at[slot], out_ref.at[h, :, pl.ds(c * STEP, STEP)], sem.at[slot]))
        copies[i].start()
    for c in copies[-2:]:
        c.wait()


def table_call(ids, rows, lo, half):
    hbm, dma = pl.BlockSpec(memory_space=pl.ANY), pltpu.SemaphoreType.DMA((2,))
    return pl.pallas_call(
        functools.partial(table_kernel, half),
        grid_spec=pltpu.PrefetchScalarGridSpec(
            num_scalar_prefetch=1, grid=(), in_specs=[hbm] * 2, out_specs=[hbm] * 2,
            scratch_shapes=[pltpu.VMEM(rows.shape, F32)] + [pltpu.VMEM((half + PAD, LANES), F32)] * 2 + [pltpu.VMEM((2, LANES, STEP), F32), pltpu.VMEM((2, S, D), BF16)]
            + [dma] * 3),
        out_shape=[jax.ShapeDtypeStruct((2, LANES, PAD), F32), jax.ShapeDtypeStruct(lo.shape, lo.dtype)],
        compiler_params=pltpu.CompilerParams(vmem_limit_bytes=VMEM_LIMIT),
        cost_estimate=pl.CostEstimate(flops=4_000_000_000, bytes_accessed=34_000_000, transcendentals=0),
        name="table",
    )(ids, rows, lo)


def cut(lo, n):
    first = n // (2 * LANES) * LANES
    return (lo, first), (lo + first, n - first)


def over(lead, body, at=()):
    if not lead:
        return body(at)

    @pl.loop(0, lead[0])
    def _(i):
        over(lead[1:], body, at + (i,))


def add_into(dst, srcs, lead, lo, n):
    def body(at):
        v = dst[at + (slice(None), pl.ds(lo, n))]
        for s in srcs:
            v = v + s[at + (slice(None), pl.ds(0, n))]
        dst[at + (slice(None), pl.ds(lo, n))] = v
    over(lead, body)


def tail_kernel(t_ref, g_ref, e_ref, oute_ref, outw_ref, *scratch):
    tsum, tpeer, gsum, gpeer, send, recv, local = scratch[:7]
    bufs = list(scratch[7:])
    core, dp = lax.axis_index('tp'), lax.axis_index('dp')
    pos = {'z': dp // (RING * RING), 'y': dp // RING % RING, 'x': dp % RING}
    stride = {'z': RING * RING, 'y': RING, 'x': 1}

    def shift(axis, k):
        return (pos[axis] + k) % RING

    def device(axis, k):
        return (core, dp + (shift(axis, k) - pos[axis]) * stride[axis])
    peer = (1 - core, dp)

    barrier = pltpu.get_barrier_semaphore()
    near = [peer] + [device(axis, k) for axis in 'zyx' for k in (1, RING - 1)]
    for who in near:
        pl.semaphore_signal(barrier, inc=1, device_id=who, device_id_type=MESH)
    pl.semaphore_wait(barrier, len(near))

    used = [0, 0]

    def remote(src, dst, who):
        i = used[0]
        used[0] += 1
        c = pltpu.make_async_remote_copy(src, dst, send.at[i], recv.at[i], device_id=who, device_id_type=MESH)
        c.start()
        return c

    def load(src, dst):
        i = used[1]
        used[1] += 1
        c = pltpu.make_async_copy(src, dst, local.at[i])
        c.start()
        return c
    sent = []

    wide, extra, far = pl.ds(0, WIDE), pl.ds(WIDE, EXTRA), pl.ds(WIDE, WIDE)
    every = slice(None)
    py, px, pz = pos['y'], pos['x'], pos['z']
    width = COLOR // PARTS
    flows = {}
    for q in range(PARTS):
        for axis, lo in (('y', q * width), ('x', COLOR + q * width)):
            flows[lo] = axis
    pend = {}

    def piece(axis, i):
        return (i,) if axis in 'yz' else (every, i)

    def fetch(lo, k):
        axis = flows[lo]
        at = piece(axis, shift(axis, k)) + (every,) * (2 if axis == 'y' else 1) + (pl.ds(lo, width),)
        pend[lo, k] = [remote(t_ref.at[(1,) + at], tpeer.at[at], peer), load(t_ref.at[(0,) + at], tsum.at[at])]

    def fetch_g(k):
        i = shift('z', k)
        pend['g', k] = [remote(g_ref.at[i, every, every, every, far], gpeer.at[i, every, every, every, wide], peer),
                        load(g_ref.at[i, every, every, every, wide], gsum.at[i, every, every, every, wide])]
    order = list(flows)
    for k in (2, 1, RING - 1, 0):
        for n, lo in enumerate(order):
            fetch(lo, k)
            if n == 1:
                if k == 2:
                    pend['e'] = [remote(e_ref.at[1], gpeer.at[every, every, every, every, extra], peer),
                                 load(e_ref.at[0], gsum.at[every, every, every, every, extra])]
                fetch_g(k)

    def arrive(key):
        out, here = pend[key]
        sent.append(out)
        out.wait_recv()
        here.wait()

    def ready(name, k):
        arrive((name, k))
        if name == 'g':
            i = shift('z', k)
            add_into(gsum.at[i], [gpeer.at[i]], (RING, RING), 0, GCOLS)
            return
        axis = flows[name]
        at = piece(axis, shift(axis, k))
        v = at + (every,) * (2 if axis == 'y' else 1) + (pl.ds(name, width),)
        add_into(tsum.at[at], [tpeer.at[v]], (RING,), name, width)

    class Stage:
        def __init__(self, axis, piece, lead, lo, n, need=None):
            self.axis, self.piece, self.lead, self.lo, self.n, self.need = axis, piece, lead, lo, n, need
            self.halves = cut(lo, n)
            self.near = [bufs.pop(0), bufs.pop(0)]
            self.last = [bufs.pop(0), bufs.pop(0)]

        def view(self, k, lo, n):
            return self.piece(shift(self.axis, k)).at[(every,) * (len(self.lead) + 1) + (pl.ds(lo, n),)]

        def want(self, k):
            if self.need is not None:
                ready(self.need, k)

        def first(self):
            self.want(2)
            self.c1 = [remote(self.view(2, *self.halves[s]), self.near[s], device(self.axis, k))
                       for s, k in enumerate((1, RING - 1))]

        def second(self):
            self.want(1)
            self.want(RING - 1)
            self.c2 = []
            for s, k in enumerate((1, RING - 1)):
                self.c1[s].wait_recv()
                add_into(self.piece(shift(self.axis, k)), [self.near[s]], self.lead, *self.halves[s])
                self.c2.append(remote(self.view(k, self.lo, self.n), self.last[s], device(self.axis, k)))

        def finish(self):
            self.want(0)
            for c in self.c2:
                c.wait_recv()
            add_into(self.piece(shift(self.axis, 0)), self.last, self.lead, self.lo, self.n)
            sent.extend(self.c1 + self.c2)

    one, two = (RING,), (RING, RING)
    rows_y, rows_x = (lambda i: tsum.at[i]), (lambda i: tsum.at[:, i])
    last_x, last_y = (lambda i: tsum.at[py, i]), (lambda i: tsum.at[i, px])
    first = [Stage(axis, rows_y if axis == 'y' else rows_x, one, lo, width, lo) for lo, axis in flows.items()]
    g1 = Stage('z', lambda i: gsum.at[i], two, 0, GCOLS, 'g')
    second = [Stage('x' if axis == 'y' else 'y', last_x if axis == 'y' else last_y, (), lo, width) for lo, axis in flows.items()]
    (c0, cn), (d0, dn) = cut(0, GCOLS)
    c1 = Stage('y', lambda i: gsum.at[pz, i], one, c0, cn)
    d1 = Stage('x', lambda i: gsum.at[pz, :, i], one, d0, dn)
    c2 = Stage('x', lambda i: gsum.at[pz, py, i], (), c0, cn)
    d2 = Stage('y', lambda i: gsum.at[pz, i, px], (), d0, dn)

    firsts = first[:2] + [g1] + first[2:]
    after = dict(zip(first, ([s] for s in second)))
    after[g1] = [c1, d1]
    for s in firsts:
        if s is g1:
            arrive('e')
        s.first()
    for s in firsts:
        s.second()
    for s in firsts:
        s.finish()
        for t in after[s]:
            t.first()
    nexts = [t for s in firsts for t in after[s]]
    for s in nexts:
        s.second()
    for s, t in ((c1, c2), (d1, d2)):
        s.finish()
        t.first()
    for s in second:
        s.finish()
    oute_ref[...] = tsum[py, px, :, 0:oute_ref.shape[1]]
    for s in (c2, d2):
        s.second()
    for s in (c2, d2):
        s.finish()
    outw_ref[...] = gsum[pz, py, px]
    for c in sent:
        c.wait_send()


def tail_call(t, g, e, rows):
    def ring_bufs(lead, n):
        (_, p), (_, q) = cut(0, n)
        return [pltpu.VMEM(lead + (ROW, w), F32) for w in (p, q, n, n)]
    (_, cn), (_, dn) = cut(0, GCOLS)
    one, two, three = (RING,), (RING,) * 2, (RING,) * 3
    width = COLOR // PARTS
    bufs = sum((ring_bufs(*b) for b in [(one, width)] * (2 * PARTS) + [(two, GCOLS)] + [((), width)] * (2 * PARTS)
                + [(one, cn), (one, dn), ((), cn), ((), dn)]), [])
    dma = pltpu.SemaphoreType.DMA
    hbm = pl.BlockSpec(memory_space=pl.ANY)
    vm = pl.BlockSpec(memory_space=pltpu.VMEM)
    return pl.pallas_call(
        tail_kernel,
        in_specs=[hbm] * 3, out_specs=[vm] * 2,
        out_shape=[jax.ShapeDtypeStruct((ROW, rows), F32), jax.ShapeDtypeStruct((ROW, GCOLS), F32)],
        scratch_shapes=[pltpu.VMEM(two + (ROW, PAD), F32)] * 2 + [pltpu.VMEM(three + (ROW, GCOLS), F32)] * 2
        + [dma((128,)), dma((128,)), dma((32,))] + bufs,
        compiler_params=pltpu.CompilerParams(collective_id=0, has_side_effects=True, vmem_limit_bytes=VMEM_LIMIT),
        name="tail",
    )(t, g, e)


def solution(mesh):
    tp, dp, no = 'tp', 'dp', None
    one, vec_dp, both = P(no), P(dp), P((tp, dp))
    arg_specs = (P(dp, no), P(tp, no), one, one, one, one, P(no, tp, no, no), P(tp, no, no), P(tp, no, no), one, P(no, tp), P(tp), P(tp, no), one, P(dp, no, no))
    out_specs = (P(dp, no, no), P(tp, dp), vec_dp, vec_dp, vec_dp, vec_dp, P(dp, tp, no, no), both, P(tp, no, dp), vec_dp, P(dp, tp), both, P(tp, dp), vec_dp)
    chips = mesh.shape[dp]
    plane = chips // RING

    def swap(v):
        return lax.ppermute(v, tp, [(0, 1), (1, 0)])

    def z_shift(v, k):
        return lax.ppermute(v, dp, [(i, (i + k * plane) % chips) for i in range(chips)]) if k else v

    def device_step(token_ids, embed_table, ln1_gain, ln1_bias, ln2_gain, ln2_bias, w_qkv, b_qkv, w_dense, b_dense, w_fc1, b_fc1, w_fc2, b_fc2, cotangent):
        core = lax.axis_index(tp)
        vocab_local = embed_table.shape[0]
        seqs = token_ids.shape[0] // 2
        f = lambda v: v.astype(F32)

        wq_own = w_qkv.transpose(2, 1, 3, 0).reshape(3 * HALF, D)
        wd_own = w_dense.reshape(HALF, D)
        rows_peer = swap(f(jnp.concatenate([wq_own, wd_own, w_fc2], axis=0)))
        fc1_peer = swap(f(w_fc1))
        wide = FF // 2
        bias = f(jnp.concatenate([jnp.pad(b_qkv.transpose(1, 0, 2).reshape(3, HALF), ((0, 0), (0, wide - HALF))), b_fc1.reshape(1, wide)], axis=0))
        bias_peer = swap(bias)
        vec = jnp.stack([ln1_gain, ln1_bias, ln2_gain, ln2_bias, b_dense, b_fc2])

        tokens = jnp.where(core == 0, token_ids, jnp.roll(token_ids, seqs, axis=0)).reshape(-1)
        local = tokens - core * vocab_local
        codes = jnp.where((local >= 0) & (local < vocab_local), local, vocab_local)
        x_send, x_own = look_up_call(codes, embed_table)
        flat = tokens[:seqs * S]
        ids = jnp.concatenate([z_shift(flat, k) for k in range(RING)]) - core * vocab_local

        args = (x_own, cotangent, vec, bias, bias_peer, rope_consts(), x_send, wq_own, wd_own, w_fc1, w_fc2, rows_peer, fc1_peer)
        layer_out, rows, _, grad_w, grad_s, grad_b1 = layer_call(*args)

        dense, layer_out = table_call(jnp.where(ids < 0, ids + 2 * vocab_local, ids), rows, layer_out, vocab_local)

        small = jnp.sum(grad_s, axis=1)
        norms = small[:5].reshape(5, chips, ROW).transpose(1, 0, 2).reshape(chips, 5 * ROW)
        grad_bq = small[5:].reshape(3, 2, PAIRS, HD).transpose(1, 2, 0, 3).reshape(2, chips, -1)
        grad_bf = jnp.sum(grad_b1, axis=0).reshape(2, chips, -1)
        extra = jnp.concatenate([jnp.stack([norms, norms]), grad_bq, grad_bf], axis=2)
        ends = (5 * ROW, 5 * ROW + grad_bq.shape[2], extra.shape[2])
        extra = jnp.pad(extra[:, :, None, :], ((0, 0), (0, 0), (0, ROW - 1), (0, EXTRA - ends[2])))
        ring3 = (RING,) * 3
        sum_embed, total = tail_call(dense.reshape(2, RING, RING, ROW, PAD), grad_w.reshape(ring3 + (ROW, 2 * WIDE)),
                                     extra.reshape((2,) + ring3 + (ROW, EXTRA)), vocab_local)
        qkv = 3 * HALF
        sum_wqkv = total[:, :qkv].reshape(ROW, 3, PAIRS, HD).transpose(0, 2, 1, 3)
        sum_wdense = total[:, qkv:wide].reshape(ROW, PAIRS, HD).transpose(1, 2, 0)
        sum_wfc1, sum_wfc2 = total[:, wide:2 * wide], total[:, 2 * wide:WIDE].T
        last = total[0, WIDE:]
        n1g, n1b, n2g, n2b, bias = last[:ends[0]].reshape(5, ROW)
        return (layer_out, sum_embed.T, n1g, n1b, n2g, n2b, sum_wqkv, last[ends[0]:ends[1]], sum_wdense, bias, sum_wfc1,
                last[ends[1]:ends[2]], sum_wfc2, bias)

    return jax.shard_map(device_step, mesh=mesh, in_specs=arg_specs, out_specs=out_specs, check_vma=False)
```

```python
import functools
import math
import jax
import jax.numpy as jnp
from jax import lax
from jax.experimental import pallas as pl
from jax.experimental.pallas import tpu as pltpu
from jax.sharding import PartitionSpec as P

F32, BF16 = jnp.float32, jnp.bfloat16
NN = (((1,), (0,)), ((), ()))
NT = (((1,), (1,)), ((), ()))
TN = (((0,), (0,)), ((), ()))
S, D, FF, HEADS, HD = 512, 512, 2048, 8, 64
PAIR, HALF, PAIRS, FF_STEPS, ROT_HALF = 2 * HD, S // 2, HEADS // 2, FF // S, HD // 8
QKV, BOTH = 3, range(2)
EPS, ROPE_BASE = 1e-5, 10000.0
LOG2E = 1.4426950408889634
SQRT_HALF, INV_SQRT_2PI = 0.7071067811865476, 0.3989422804014327
RB = 128
VMEM_LIMIT = 67_000_000
ROW, LANES, RING = 8, 128, 4
PAD = 25600
COLOR = PAD // 2
PARTS = 2
WIDE, EXTRA = 3072, 128
GCOLS = WIDE + EXTRA
MESH = pl.DeviceIdType.MESH


def dot(a, b, dims=NN):
    return lax.dot_general(a, b, dims, preferred_element_type=F32)


def rnd(v):
    return v.astype(BF16).astype(F32)


def gelu_parts(a):
    phi = 0.5 + 0.5 * lax.erf(a * SQRT_HALF)
    return a * phi, phi + a * jnp.exp2(a * a * (-0.5 * LOG2E)) * INV_SQRT_2PI


def block(i, n):
    return slice(i * n, i * n + n)


def row_sums(v):
    return jnp.sum(v.reshape(v.shape[0] // ROW, ROW, v.shape[1]), axis=0)


def wcol(half, part, width):
    return slice(half * WIDE + part, half * WIDE + part + width)


def look_up_kernel(codes_ref, table_ref, peer_ref, own_ref, table, sem):
    step = pl.program_id(0)
    half = pl.num_programs(0) * S

    @pl.when(step == 0)
    def _():
        tiles = table_ref.shape[0]
        load = pltpu.make_async_copy(table_ref, table.at[:tiles], sem)
        load.start()
        table[tiles] = jnp.zeros((ROW, D), BF16)
        load.wait()
    sub = lax.broadcasted_iota(jnp.int32, (ROW, D), 0)

    def look_up(first):
        got = jnp.zeros((ROW, D), F32)
        for j in range(ROW):
            at = codes_ref[first + j]
            got = jnp.where(sub == j, pltpu.roll(table[at >> 3].astype(F32), at & (ROW - 1), 0), got)
        return got

    for k, dst in enumerate((own_ref, peer_ref)):
        @pl.loop(0, S // ROW, unroll=2)
        def _(g):
            t0 = pl.multiple_of(g * ROW, ROW)
            dst[0, pl.ds(t0, ROW), :] = look_up(k * half + step * S + t0).astype(dst.dtype)


def look_up_call(codes, table):
    seqs = codes.size // (2 * S)
    seq = pl.BlockSpec((1, S, D), lambda i, _: (i, 0, 0))
    return pl.pallas_call(
        look_up_kernel,
        grid_spec=pltpu.PrefetchScalarGridSpec(
            num_scalar_prefetch=1, grid=(seqs,), in_specs=[pl.BlockSpec(memory_space=pl.ANY)], out_specs=[seq] * 2,
            scratch_shapes=[pltpu.VMEM((table.shape[0] + 1, ROW, D), BF16), pltpu.SemaphoreType.DMA]),
        out_shape=[jax.ShapeDtypeStruct((seqs, S, D), t) for t in (F32, BF16)],
        compiler_params=pltpu.CompilerParams(dimension_semantics=("arbitrary",), vmem_limit_bytes=VMEM_LIMIT),
        cost_estimate=pl.CostEstimate(flops=40_000_000_000, bytes_accessed=40_000_000, transcendentals=0),
        name="look_up",
    )(codes, table)


def layer_kernel(xo_ref, cot_ref, g1_ref, b1_ref, g2_ref, b2_ref, bd_ref, bf_ref, bo_ref, bp_ref, rope_ref, xs_ref, ids_ref, qo_ref, do_ref, fo_ref, to_ref, rp_ref, fp_ref,
                 out_ref, rows_ref, xin_ref, idz_ref, gw_out, gs_out, gb1_out,
                 gw_ref, gs_ref, gb1_ref, wqkv, wd, w1, w2, n_scr, acc_scr, dh2_scr, dh1_scr, inv_scr, h1_scr, h2_scr, h1t_scr, h2t_scr, cott_scr, dctx_scr, ctx_scr,
                 qkv_scr, dqkv_scr, s_scr, dp_scr, pb_scr, ds_scr, a_scr, du_scr, u_scr, da_scr, dk_scr, dv_scr,
                 xp_buf, gx_buf, out_buf, peer_buf, own_low, peer_low, x_send, x_recv, x_load, id_send, id_recv, gx_send, gx_recv, gx_local, out_send, out_recv, own_sem, peer_sem, init_sem):
    step, last = pl.program_id(0), pl.num_programs(0) - 1
    slot = step % 2
    core, chip = lax.axis_index('tp'), lax.axis_index('dp')
    chips = lax.axis_size('dp')
    plane = chips // RING
    z, peer = chip // plane, (1 - core, chip)

    def z_device(k):
        return (core, (chip + k * plane) % chips)

    def x_copy(at):
        return pltpu.make_async_remote_copy(xs_ref.at[at], xin_ref.at[at], x_send.at[at], x_recv.at[at], device_id=peer, device_id_type=MESH)

    def x_take(at):
        return pltpu.make_async_copy(xin_ref.at[at], xp_buf.at[at % 2], x_load.at[at % 2])

    def id_copy(k):
        if k:
            return pltpu.make_async_remote_copy(ids_ref, idz_ref.at[k], id_send.at[k], id_recv.at[k], device_id=z_device(k), device_id_type=MESH)
        return pltpu.make_async_copy(ids_ref, idz_ref.at[k], id_send.at[k])

    @pl.when(step == 0)
    def _():
        barrier = pltpu.get_barrier_semaphore()
        near = [peer] + [z_device(k) for k in range(1, RING)]
        for who in near:
            pl.semaphore_signal(barrier, inc=1, device_id=who, device_id_type=MESH)
        pl.semaphore_wait(barrier, len(near))

        @pl.loop(0, last + 1)
        def _(at):
            x_copy(at).start()
        for k in range(RING):
            id_copy(k).start()
        for dst in (gw_ref, gs_ref, gb1_ref):
            dst[...] = jnp.zeros_like(dst)
        n = FF // 2
        moves = [(qo_ref.at[block(j, HALF)], wqkv.at[block(2 * j, HALF)]) for j in range(QKV)]
        moves += [(do_ref, wd.at[:HALF]), (to_ref, w2.at[:n]), (fo_ref, w1.at[:, :n])]
        tables = (n_scr, acc_scr, dh2_scr, dh1_scr, s_scr.at[0], s_scr.at[1])
        parts = [rp_ref.at[block(i, S)] for i in range(RING)] + [fp_ref.at[:, block(i, S)] for i in BOTH]
        copies = [pltpu.make_async_copy(src, dst, init_sem.at[i]) for i, (src, dst) in enumerate(moves + list(zip(parts, tables)))]
        for c in copies:
            c.start()
        for c in copies:
            c.wait()
        for j in range(QKV):
            wqkv[block(2 * j + 1, HALF), :] = tables[j // 2][block(j % 2, HALF), :].astype(BF16)
        wd[HALF:, :] = tables[1][HALF:, :].astype(BF16)
        for i in BOTH:
            w2[block(2 + i, S), :] = tables[2 + i][...].astype(BF16)
            w1[:, block(2 + i, S)] = tables[RING + i][...].astype(BF16)

        x_copy(0).wait_recv()
        x_take(0).start()

    x_take(step).wait()

    @pl.when(step < last)
    def _():
        x_copy(step + 1).wait_recv()
        x_take(step + 1).start()

    def gx_copy(at, k):
        rows = pl.ds(pl.multiple_of(at * S, S), S)
        src, dst = gx_buf.at[at % 2, k], rows_ref.at[k, rows]
        if k:
            return pltpu.make_async_remote_copy(src, dst, gx_send.at[at % 2, k], gx_recv.at[at, k], device_id=z_device(k), device_id_type=MESH)
        return pltpu.make_async_copy(src, dst, gx_local.at[at % 2])

    def out_copy(at):
        return pltpu.make_async_remote_copy(out_buf.at[at % 2], peer_buf.at[at], out_send.at[at % 2], out_recv.at[at], device_id=peer, device_id_type=MESH)

    def own_store(at):
        return pltpu.make_async_copy(own_low.at[at % 2], out_ref.at[core * (last + 1) + at], own_sem.at[at % 2])

    def peer_store(at):
        return pltpu.make_async_copy(peer_low.at[at % 2], out_ref.at[(1 - core) * (last + 1) + at], peer_sem.at[at % 2])

    def drain(at):
        gx_copy(at, 0).wait()
        for k in range(1, RING):
            gx_copy(at, k).wait_send()
        out_copy(at).wait_send()
        own_store(at).wait()

    def take_peer(at):
        out_copy(at).wait_recv()

        @pl.when(at > 1)
        def _():
            peer_store(at - 2).wait()
        peer_low[at % 2] = peer_buf[at].astype(BF16)
        peer_store(at).start()

    @pl.when(step > 1)
    def _():
        drain(step - 2)

    cot = cot_ref[0]
    g1, b1, g2, b2, bd, bf = (v[...].astype(F32).reshape(1, D) for v in (g1_ref, b1_ref, g2_ref, b2_ref, bd_ref, bf_ref))
    bo = bd + bf

    def bias(row, i, n):
        width = HALF if row < 3 else FF // 2
        src, i = (bo_ref, i) if i < width // n else (bp_ref, i - width // n)
        return src[row:row + 1, block(i, n)]

    dctx_scr[...] = dot(cot, wd[...], NT).astype(BF16)
    cott_scr[...] = cot.T
    x = xo_ref[0].astype(F32) + xp_buf[slot]
    cen = x - jnp.mean(x, axis=-1, keepdims=True)
    inv = lax.rsqrt(jnp.mean(cen * cen, axis=-1, keepdims=True) + EPS)
    n = cen * inv
    n_scr[...] = n
    inv_scr[...] = inv
    h1_scr[...] = (n * g1 + b1).astype(BF16)
    h2_scr[...] = (n * g2 + b2).astype(BF16)
    gs_ref[4] += row_sums(cot.astype(F32))
    h1t_scr[...] = h1_scr[...].T
    h2t_scr[...] = h2_scr[...].T
    h1, h2 = h1_scr[...], h2_scr[...]

    for p in range(PAIRS):
        for j in range(QKV):
            v = dot(h1, wqkv[block(j * PAIRS + p, PAIR), :], NT) + bias(j, p, PAIR)
            v = v.astype(BF16)
            if j < 2:
                v = v.astype(F32)
                v = (v * rope_ref[0] + pltpu.roll(v, PAIR - ROT_HALF, 1) * rope_ref[1]
                     + pltpu.roll(v, ROT_HALF, 1) * rope_ref[2]).astype(BF16)
            qkv_scr[j, :, block(p, PAIR)] = v

    lane = lax.broadcasted_iota(jnp.int32, (HALF, PAIR), 1)
    causal = lax.broadcasted_iota(jnp.int32, (HALF, HALF), 0) >= lax.broadcasted_iota(jnp.int32, (HALF, HALF), 1)
    heads = (lane < HD, lane >= HD)
    zero = jnp.zeros((HALF, PAIR), BF16)

    def only(v, hh):
        return jnp.concatenate([jnp.where(heads[hh], v[block(i, HALF)], zero) for i in range(v.shape[0] // HALF)], axis=0)

    def rope_back(g, rows):
        g = rnd(g * HD ** -0.5)
        return (g * rope_ref[0, rows] + pltpu.roll(g * rope_ref[1, rows], ROT_HALF, 1)
                + pltpu.roll(g * rope_ref[2, rows], PAIR - ROT_HALF, 1)).astype(BF16)

    class Attention:
        def __init__(self, i):
            p, self.qb = i // 2, i % 2
            self.n, self.slot, self.lanes, self.rows = HALF * (self.qb + 1), self.qb, block(p, PAIR), block(self.qb, HALF)

        def operands(self):
            q, dc = qkv_scr[0, self.rows, self.lanes], dctx_scr[self.rows, self.lanes]
            return q, dc, qkv_scr[1, :self.n, self.lanes], qkv_scr[2, :self.n, self.lanes]

        def one(self):
            q, dc, k, v = self.operands()
            for hh in BOTH:
                at = (self.slot, block(hh, HALF), slice(self.n))
                s_scr[at] = dot(only(q, hh), k, NT)
                dp_scr[at] = dot(only(dc, hh), v, NT).astype(BF16)

        def two(self):
            for hh in BOTH:
                at = (self.slot, block(hh, HALF), slice(self.n))
                s = s_scr[at]
                diag = jnp.where(causal, s[:, self.n - HALF:], -1e30)
                s = jnp.concatenate([s[:, :HALF], diag], axis=1) if self.qb else diag
                e = jnp.exp2((s - jnp.max(s, axis=-1, keepdims=True)) * (HD ** -0.5 * LOG2E))
                pr = e * (1.0 / jnp.sum(e, axis=-1, keepdims=True))
                pb_scr[at] = pr.astype(BF16)
                dp = dp_scr[at].astype(F32)
                ds_scr[at] = (pr * (dp - jnp.sum(pr * dp, axis=-1, keepdims=True))).astype(BF16)

        def three(self):
            q, dc, k, v = self.operands()
            pb, ds = pb_scr[self.slot, :, :self.n], ds_scr[self.slot, :, :self.n]
            rows, lanes = self.rows, self.lanes
            ctx_scr[rows, lanes] = sum(dot(pb[block(hh, HALF)], only(v, hh)) for hh in BOTH).astype(BF16)
            dqkv_scr[0, rows, lanes] = rope_back(sum(dot(ds[block(hh, HALF)], only(k, hh)) for hh in BOTH), rows)
            dk = dot(ds, jnp.concatenate([only(q, hh) for hh in BOTH], axis=0), TN)
            dv = dot(pb, jnp.concatenate([only(dc, hh) for hh in BOTH], axis=0), TN)
            if not self.qb:
                dk_scr[...] = dk
                dv_scr[...] = dv
                return
            for b in BOTH:
                at = block(b, HALF)
                gk, gv = (dk[at], dv[at]) if b else (dk[at] + dk_scr[...], dv[at] + dv_scr[...])
                dqkv_scr[1, at, lanes] = rope_back(gk, at)
                dqkv_scr[2, at, lanes] = gv.astype(BF16)

    class Mlp:
        def __init__(self, i):
            self.i, self.slot, self.cols = i, i % 2, block(i, HALF)

        def one(self):
            a_scr[self.slot] = dot(h2, w1[:, self.cols]) + bias(3, self.i, HALF)
            du_scr[self.slot] = dot(cot, w2[self.cols, :], NT).astype(BF16)

        def two(self):
            u, gp = gelu_parts(rnd(a_scr[self.slot]))
            da = (du_scr[self.slot].astype(F32) * gp).astype(BF16)
            u_scr[self.slot] = u.astype(BF16)
            da_scr[self.slot] = da
            gb1_ref[:, self.cols] += row_sums(da.astype(F32))

        def three(self):
            u, da = u_scr[self.slot], da_scr[self.slot]
            m, d = dot(u, w2[self.cols, :]), dot(da, w1[:, self.cols], NT)
            acc_scr[...] = acc_scr[...] + m if self.i else m
            dh2_scr[...] = dh2_scr[...] + d if self.i else d
            half, part = self.i // RING, 2 * S + self.i % RING * HALF
            gw_ref[:, wcol(half, part, HALF)] += dot(h2t_scr[...], da)
            gw_ref[:, wcol(half, part + 2 * S, HALF)] += dot(cott_scr[...], u)

    units = [u for i in range(2 * PAIRS) for u in (Attention(i), Mlp(i))]
    units[0].one()
    for i, u in enumerate(units):
        if i + 1 < len(units):
            units[i + 1].one()
        u.two()
        if i:
            units[i - 1].three()
    units[-1].three()

    dh1_scr[...] = sum(dot(dqkv_scr[j], wqkv[block(j, S), :]) for j in range(QKV))
    acc_scr[...] += dot(ctx_scr[...], wd[...])
    for half in BOTH:
        hs = block(half, HALF)
        for j in range(QKV):
            gw_ref[:, wcol(half, j * HALF, HALF)] += dot(h1t_scr[...], dqkv_scr[j, :, hs])
        gw_ref[:, wcol(half, QKV * HALF, HALF)] += dot(cott_scr[...], ctx_scr[:, hs])

    n = n_scr[...]
    d1, d2 = rnd(dh1_scr[...]), rnd(dh2_scr[...])
    for i, v in zip((0, 1, 2, 3, 5, 6, 7), (d1 * n, d1, d2 * n, d2, *(dqkv_scr[j].astype(F32) for j in range(QKV)))):
        gs_ref[i] += row_sums(v)
    gn = d1 * g1 + d2 * g2
    s_scr[0] = cot.astype(F32) + inv_scr[...] * (
        gn - jnp.mean(gn, axis=-1, keepdims=True) - n * jnp.mean(gn * n, axis=-1, keepdims=True))
    low = (xo_ref[0].astype(F32) + xp_buf[slot] + (acc_scr[...] + bo)).astype(BF16)
    own_low[slot] = low
    out_buf[slot] = low.astype(F32)
    for k in range(RING):
        gx_buf[slot, k] = s_scr[0, :, pl.ds(pl.multiple_of((z + k) % RING * LANES, LANES), LANES)]
    for k in (2, 1, 3, 0):
        gx_copy(step, k).start()
    out_copy(step).start()
    own_store(step).start()

    @pl.when(step > 0)
    def _():
        take_peer(step - 1)

    @pl.when(step == last)
    def _():
        save = pltpu.make_async_copy(gw_ref, gw_out, init_sem.at[0])
        save.start()
        gs_out[...] = jnp.sum(gs_ref[...], axis=1)
        gb1_out[...] = jnp.sum(gb1_ref[...], axis=0, keepdims=True)
        take_peer(step)
        for at in (step - 1, step):
            drain(at)
            peer_store(at).wait()

        @pl.loop(0, last + 1)
        def _(at):
            x_copy(at).wait_send()
            for k in range(1, RING):
                gx_copy(at, k).wait_recv()
        save.wait()
        for k in range(RING):
            id_copy(k).wait()


def rope_consts():
    lane = lax.broadcasted_iota(jnp.int32, (S, PAIR), 1) % HD
    inv_freq = ROPE_BASE ** (-(lane % ROT_HALF).astype(F32) / ROT_HALF)
    ang = lax.broadcasted_iota(F32, (S, PAIR), 0) * inv_freq
    sin, low, rot = jnp.sin(ang), lane < ROT_HALF, lane < 2 * ROT_HALF
    return jnp.stack([jnp.where(rot, jnp.cos(ang), 1.0), jnp.where(low, -sin, 0.0), jnp.where(rot & ~low, sin, 0.0)])


def layer_call(*args):
    count = args[0].shape[0]
    vm, hbm = pl.BlockSpec(memory_space=pltpu.VMEM), pl.BlockSpec(memory_space=pl.ANY)
    seq = pl.BlockSpec((1, S, D), lambda i: (i, 0, 0))
    own_seq = pl.BlockSpec((1, S, D), lambda i: (lax.axis_index('tp') * count + i, 0, 0))
    dma = pltpu.SemaphoreType.DMA

    def table(*lead):
        return pltpu.VMEM(lead + (S, D), F32)

    def low(*lead):
        return pltpu.VMEM(lead + (S, D), BF16)
    thin, thin_low, small = pltpu.VMEM((2, S, HALF), F32), pltpu.VMEM((2, S, HALF), BF16), pltpu.VMEM((HALF, PAIR), F32)
    return pl.pallas_call(
        layer_kernel,
        grid=(count,),
        in_specs=[seq, own_seq] + [vm] * 9 + [hbm] * (len(args) - 11),
        out_specs=[hbm] * 5 + [vm] * 2,
        out_shape=[jax.ShapeDtypeStruct((2 * count, S, D), BF16), jax.ShapeDtypeStruct((RING, count * S, LANES), F32), jax.ShapeDtypeStruct((count, S, D), F32), jax.ShapeDtypeStruct((RING, count * S // LANES, LANES), jnp.int32),
                   jax.ShapeDtypeStruct((D, 2 * WIDE), F32), jax.ShapeDtypeStruct((ROW, D), F32), jax.ShapeDtypeStruct((1, FF), F32)],
        scratch_shapes=[pltpu.VMEM((D, 2 * WIDE), F32), pltpu.VMEM((ROW, ROW, D), F32), pltpu.VMEM((ROW, FF), F32), pltpu.VMEM((QKV * S, D), BF16), low(), pltpu.VMEM((D, FF), BF16), pltpu.VMEM((FF, D), BF16)] + [table()] * 4
        + [pltpu.VMEM((S, 1), F32)] + [low()] * 7 + [low(3)] * 2 + [table(2)] + [low(2)] * 3 + [thin] + [thin_low] * 3 + [small] * 2
        + [table(2), pltpu.VMEM((2, RING, S, LANES), F32), table(2), table(count)] + [low(2)] * 2
        + [dma((count,)), dma((count,)), dma((2,)), dma((RING,)), dma((RING,)), dma((2, RING)), dma((count, RING)), dma((2,)), dma((2,)), dma((count,)), dma((2,)), dma((2,)), dma((16,))],
        compiler_params=pltpu.CompilerParams(dimension_semantics=("arbitrary",), collective_id=1, has_side_effects=True,
                                             vmem_limit_bytes=VMEM_LIMIT),
        cost_estimate=pl.CostEstimate(flops=count * 30_000_000_000, bytes_accessed=60_000_000, transcendentals=0),
        name="layer",
    )(*args)


STEPS, UNROLL = 8, 16
STEP = PAD // STEPS


def table_kernel(half, ids_ref, rows_hbm, lo_ref, out_ref, lo_out_ref, rows_ref, acc, acc2, stage, lo_buf, sem, lo_in, lo_sent):
    load = pltpu.make_async_copy(rows_hbm, rows_ref, sem.at[0])
    load.start()

    @pl.loop(0, acc.shape[0] // LANES)
    def _(j):
        for a in (acc, acc2):
            a[pl.ds(pl.multiple_of(j * LANES, LANES), LANES), :] = jnp.zeros((LANES, LANES), F32)
    count, blocks = rows_ref.shape[1], lo_ref.shape[0]
    part = RING // 2 * count // blocks
    per = count // part

    def lo_load(i):
        return pltpu.make_async_copy(lo_ref.at[i], lo_buf.at[i % 2], lo_in.at[i % 2])

    def lo_store(i):
        return pltpu.make_async_copy(lo_buf.at[i % 2], lo_out_ref.at[i], lo_sent.at[i % 2])
    lo_load(0).start()
    load.wait()

    @pl.loop(0, blocks)
    def _(i):
        lo_load(i).wait()
        lo_store(i).start()

        @pl.when(i > 0)
        def _():
            lo_store(i - 1).wait()

        @pl.when(i + 1 < blocks)
        def _():
            lo_load(i + 1).start()
        k, first = i // per * 2, i % per * part

        @pl.loop(0, part // UNROLL)
        def _(g):
            t0 = pl.multiple_of(first + g * UNROLL, UNROLL)
            for j in range(0, UNROLL, 2):
                pairs = []
                for a, src in ((acc, k), (acc2, k + 1)):
                    i0, i1 = (ids_ref[src * count + t0 + j + d] for d in BOTH)
                    x0, x1 = (rows_ref[src, pl.ds(t0 + j + d, 1), :] for d in BOTH)
                    r0, r1 = pl.ds(i0, 1), pl.ds(i1, 1)
                    pairs.append((a, r0, a[r0, :] + x0, r1, a[r1, :] + (x1 + jnp.where(i0 == i1, x0, 0.0))))
                for a, r0, v0, r1, v1 in pairs:
                    a[r0, :] = v0
                    a[r1, :] = v1
    lo_store(blocks - 1).wait()
    copies = []
    for i in range(2 * STEPS):
        h, c, slot = i // STEPS, i % STEPS, i % 2
        if i > 1:
            copies[i - 2].wait()

        @pl.loop(0, STEP // LANES, unroll=5)
        def _(b):
            at = pl.ds(pl.multiple_of(h * half + c * STEP + b * LANES, ROW), LANES)
            stage[slot, :, pl.ds(pl.multiple_of(b * LANES, LANES), LANES)] = (acc[at, :] + acc2[at, :]).T
        copies.append(pltpu.make_async_copy(stage.at[slot], out_ref.at[h, :, pl.ds(c * STEP, STEP)], sem.at[slot]))
        copies[i].start()
    for c in copies[-2:]:
        c.wait()


def table_call(ids, rows, lo, half):
    hbm, dma = pl.BlockSpec(memory_space=pl.ANY), pltpu.SemaphoreType.DMA((2,))
    return pl.pallas_call(
        functools.partial(table_kernel, half),
        grid_spec=pltpu.PrefetchScalarGridSpec(
            num_scalar_prefetch=1, grid=(), in_specs=[hbm] * 2, out_specs=[hbm] * 2,
            scratch_shapes=[pltpu.VMEM(rows.shape, F32)] + [pltpu.VMEM((half + PAD, LANES), F32)] * 2 + [pltpu.VMEM((2, LANES, STEP), F32), pltpu.VMEM((2, S, D), BF16)]
            + [dma] * 3),
        out_shape=[jax.ShapeDtypeStruct((2, LANES, PAD), F32), jax.ShapeDtypeStruct(lo.shape, lo.dtype)],
        compiler_params=pltpu.CompilerParams(vmem_limit_bytes=VMEM_LIMIT),
        cost_estimate=pl.CostEstimate(flops=4_000_000_000, bytes_accessed=34_000_000, transcendentals=0),
        name="table",
    )(ids, rows, lo)


def cut(lo, n):
    first = n // (2 * LANES) * LANES
    return (lo, first), (lo + first, n - first)


def over(lead, body, at=()):
    if not lead:
        return body(at)

    @pl.loop(0, lead[0])
    def _(i):
        over(lead[1:], body, at + (i,))


def add_into(dst, srcs, lead, lo, n):
    def body(at):
        v = dst[at + (slice(None), pl.ds(lo, n))]
        for s in srcs:
            v = v + s[at + (slice(None), pl.ds(0, n))]
        dst[at + (slice(None), pl.ds(lo, n))] = v
    over(lead, body)


def tail_kernel(t_ref, g_ref, e_ref, oute_ref, outw_ref, *scratch):
    tsum, tpeer, gsum, gpeer, send, recv, local = scratch[:7]
    bufs = list(scratch[7:])
    core, dp = lax.axis_index('tp'), lax.axis_index('dp')
    pos = {'z': dp // (RING * RING), 'y': dp // RING % RING, 'x': dp % RING}
    stride = {'z': RING * RING, 'y': RING, 'x': 1}

    def shift(axis, k):
        return (pos[axis] + k) % RING

    def device(axis, k):
        return (core, dp + (shift(axis, k) - pos[axis]) * stride[axis])
    peer = (1 - core, dp)

    barrier = pltpu.get_barrier_semaphore()
    near = [peer] + [device(axis, k) for axis in 'zyx' for k in (1, RING - 1)]
    for who in near:
        pl.semaphore_signal(barrier, inc=1, device_id=who, device_id_type=MESH)
    pl.semaphore_wait(barrier, len(near))

    used = [0, 0]

    def remote(src, dst, who):
        i = used[0]
        used[0] += 1
        c = pltpu.make_async_remote_copy(src, dst, send.at[i], recv.at[i], device_id=who, device_id_type=MESH)
        c.start()
        return c

    def load(src, dst):
        i = used[1]
        used[1] += 1
        c = pltpu.make_async_copy(src, dst, local.at[i])
        c.start()
        return c
    sent = []

    wide, extra, far = pl.ds(0, WIDE), pl.ds(WIDE, EXTRA), pl.ds(WIDE, WIDE)
    every = slice(None)
    py, px, pz = pos['y'], pos['x'], pos['z']
    width = COLOR // PARTS
    flows = {}
    for q in range(PARTS):
        for axis, lo in (('y', q * width), ('x', COLOR + q * width)):
            flows[lo] = axis
    pend = {}

    def piece(axis, i):
        return (i,) if axis in 'yz' else (every, i)

    def fetch(lo, k):
        axis = flows[lo]
        at = piece(axis, shift(axis, k)) + (every,) * (2 if axis == 'y' else 1) + (pl.ds(lo, width),)
        pend[lo, k] = [remote(t_ref.at[(1,) + at], tpeer.at[at], peer), load(t_ref.at[(0,) + at], tsum.at[at])]

    def fetch_g(k):
        i = shift('z', k)
        pend['g', k] = [remote(g_ref.at[i, every, every, every, far], gpeer.at[i, every, every, every, wide], peer),
                        load(g_ref.at[i, every, every, every, wide], gsum.at[i, every, every, every, wide])]
    order = list(flows)
    for k in (2, 1, RING - 1, 0):
        for n, lo in enumerate(order):
            fetch(lo, k)
            if n == 1:
                if k == 2:
                    pend['e'] = [remote(e_ref.at[1], gpeer.at[every, every, every, every, extra], peer),
                                 load(e_ref.at[0], gsum.at[every, every, every, every, extra])]
                fetch_g(k)

    def arrive(key):
        out, here = pend[key]
        sent.append(out)
        out.wait_recv()
        here.wait()

    def ready(name, k):
        arrive((name, k))
        if name == 'g':
            i = shift('z', k)
            add_into(gsum.at[i], [gpeer.at[i]], (RING, RING), 0, GCOLS)
            return
        axis = flows[name]
        at = piece(axis, shift(axis, k))
        v = at + (every,) * (2 if axis == 'y' else 1) + (pl.ds(name, width),)
        add_into(tsum.at[at], [tpeer.at[v]], (RING,), name, width)

    class Stage:
        def __init__(self, axis, piece, lead, lo, n, need=None):
            self.axis, self.piece, self.lead, self.lo, self.n, self.need = axis, piece, lead, lo, n, need
            self.halves = cut(lo, n)
            self.near = [bufs.pop(0), bufs.pop(0)]
            self.last = [bufs.pop(0), bufs.pop(0)]

        def view(self, k, lo, n):
            return self.piece(shift(self.axis, k)).at[(every,) * (len(self.lead) + 1) + (pl.ds(lo, n),)]

        def want(self, k):
            if self.need is not None:
                ready(self.need, k)

        def first(self):
            self.want(2)
            self.c1 = [remote(self.view(2, *self.halves[s]), self.near[s], device(self.axis, k))
                       for s, k in enumerate((1, RING - 1))]

        def second(self):
            self.want(1)
            self.want(RING - 1)
            self.c2 = []
            for s, k in enumerate((1, RING - 1)):
                self.c1[s].wait_recv()
                add_into(self.piece(shift(self.axis, k)), [self.near[s]], self.lead, *self.halves[s])
                self.c2.append(remote(self.view(k, self.lo, self.n), self.last[s], device(self.axis, k)))

        def finish(self):
            self.want(0)
            for c in self.c2:
                c.wait_recv()
            add_into(self.piece(shift(self.axis, 0)), self.last, self.lead, self.lo, self.n)
            sent.extend(self.c1 + self.c2)

    one, two = (RING,), (RING, RING)
    rows_y, rows_x = (lambda i: tsum.at[i]), (lambda i: tsum.at[:, i])
    last_x, last_y = (lambda i: tsum.at[py, i]), (lambda i: tsum.at[i, px])
    first = [Stage(axis, rows_y if axis == 'y' else rows_x, one, lo, width, lo) for lo, axis in flows.items()]
    g1 = Stage('z', lambda i: gsum.at[i], two, 0, GCOLS, 'g')
    second = [Stage('x' if axis == 'y' else 'y', last_x if axis == 'y' else last_y, (), lo, width) for lo, axis in flows.items()]
    (c0, cn), (d0, dn) = cut(0, GCOLS)
    c1 = Stage('y', lambda i: gsum.at[pz, i], one, c0, cn)
    d1 = Stage('x', lambda i: gsum.at[pz, :, i], one, d0, dn)
    c2 = Stage('x', lambda i: gsum.at[pz, py, i], (), c0, cn)
    d2 = Stage('y', lambda i: gsum.at[pz, i, px], (), d0, dn)

    firsts = first[:2] + [g1] + first[2:]
    after = dict(zip(first, ([s] for s in second)))
    after[g1] = [c1, d1]
    for s in firsts:
        if s is g1:
            arrive('e')
        s.first()
    for s in firsts:
        s.second()
    for s in firsts:
        s.finish()
        for t in after[s]:
            t.first()
    nexts = [t for s in firsts for t in after[s]]
    for s in nexts:
        s.second()
    for s, t in ((c1, c2), (d1, d2)):
        s.finish()
        t.first()
    for s in second:
        s.finish()
    oute_ref[...] = tsum[py, px, :, 0:oute_ref.shape[1]]
    for s in (c2, d2):
        s.second()
    for s in (c2, d2):
        s.finish()
    outw_ref[...] = gsum[pz, py, px]
    for c in sent:
        c.wait_send()


def tail_call(t, g, e, rows):
    def ring_bufs(lead, n):
        (_, p), (_, q) = cut(0, n)
        return [pltpu.VMEM(lead + (ROW, w), F32) for w in (p, q, n, n)]
    (_, cn), (_, dn) = cut(0, GCOLS)
    one, two, three = (RING,), (RING,) * 2, (RING,) * 3
    width = COLOR // PARTS
    bufs = sum((ring_bufs(*b) for b in [(one, width)] * (2 * PARTS) + [(two, GCOLS)] + [((), width)] * (2 * PARTS)
                + [(one, cn), (one, dn), ((), cn), ((), dn)]), [])
    dma = pltpu.SemaphoreType.DMA
    hbm = pl.BlockSpec(memory_space=pl.ANY)
    vm = pl.BlockSpec(memory_space=pltpu.VMEM)
    return pl.pallas_call(
        tail_kernel,
        in_specs=[hbm] * 3, out_specs=[vm] * 2,
        out_shape=[jax.ShapeDtypeStruct((ROW, rows), F32), jax.ShapeDtypeStruct((ROW, GCOLS), F32)],
        scratch_shapes=[pltpu.VMEM(two + (ROW, PAD), F32)] * 2 + [pltpu.VMEM(three + (ROW, GCOLS), F32)] * 2
        + [dma((128,)), dma((128,)), dma((32,))] + bufs,
        compiler_params=pltpu.CompilerParams(collective_id=0, has_side_effects=True, vmem_limit_bytes=VMEM_LIMIT),
        name="tail",
    )(t, g, e)


def solution(mesh):
    tp, dp, no = 'tp', 'dp', None
    one, vec_dp, both = P(no), P(dp), P((tp, dp))
    arg_specs = (P(dp, no), P(tp, no), one, one, one, one, P(no, tp, no, no), P(tp, no, no), P(tp, no, no), one, P(no, tp), P(tp), P(tp, no), one, P(dp, no, no))
    out_specs = (P(dp, no, no), P(tp, dp), vec_dp, vec_dp, vec_dp, vec_dp, P(dp, tp, no, no), both, P(tp, no, dp), vec_dp, P(dp, tp), both, P(tp, dp), vec_dp)
    chips = mesh.shape[dp]

    def swap(v):
        return lax.ppermute(v, tp, [(0, 1), (1, 0)])

    def device_step(token_ids, embed_table, ln1_gain, ln1_bias, ln2_gain, ln2_bias, w_qkv, b_qkv, w_dense, b_dense, w_fc1, b_fc1, w_fc2, b_fc2, cotangent):
        core = lax.axis_index(tp)
        vocab_local = embed_table.shape[0]
        seqs = token_ids.shape[0] // 2
        f = lambda v: v.astype(F32)

        wq_own = w_qkv.transpose(2, 1, 3, 0).reshape(QKV * HALF, D)
        wd_own = w_dense.reshape(HALF, D)
        rows_peer = swap(f(jnp.concatenate([wq_own, wd_own, w_fc2], axis=0)))
        fc1_peer = swap(f(w_fc1))
        wide = FF // 2
        bias = f(jnp.concatenate([jnp.pad(b_qkv.transpose(1, 0, 2).reshape(3, HALF), ((0, 0), (0, wide - HALF))), b_fc1.reshape(1, wide)], axis=0))
        bias_peer = swap(bias)

        tokens = jnp.where(core == 0, token_ids, jnp.roll(token_ids, seqs, axis=0)).reshape(-1)
        local = tokens - core * vocab_local
        row = jnp.where((local >= 0) & (local < vocab_local), local, vocab_local)
        codes = (row & -ROW) | ((lax.iota(jnp.int32, tokens.size) - row) & (ROW - 1))
        x_send, x_own = look_up_call(codes, embed_table.reshape(-1, ROW, D))
        ids = jnp.where(local < 0, local + 2 * vocab_local, local)[:seqs * S].reshape(-1, LANES)

        args = (x_own, cotangent, ln1_gain, ln1_bias, ln2_gain, ln2_bias, b_dense, b_fc2, bias, bias_peer, rope_consts(), x_send, ids, wq_own, wd_own, w_fc1, w_fc2, rows_peer, fc1_peer)
        layer_out, rows, _, ids, grad_w, small, grad_b1 = layer_call(*args)

        dense, layer_out = table_call(ids.reshape(-1), rows, layer_out, vocab_local)

        norms = small[:5].reshape(5, chips, ROW).transpose(1, 0, 2).reshape(chips, 5 * ROW)
        grad_bq = small[5:].reshape(3, 2, PAIRS, HD).transpose(1, 2, 0, 3).reshape(2, chips, -1)
        grad_bf = grad_b1.reshape(2, chips, -1)
        extra = jnp.concatenate([jnp.stack([norms, norms]), grad_bq, grad_bf], axis=2)
        ends = (5 * ROW, 5 * ROW + grad_bq.shape[2], extra.shape[2])
        extra = jnp.pad(extra[:, :, None, :], ((0, 0), (0, 0), (0, ROW - 1), (0, EXTRA - ends[2])))
        ring3 = (RING,) * 3
        sum_embed, total = tail_call(dense.reshape(2, RING, RING, ROW, PAD), grad_w.reshape(ring3 + (ROW, 2 * WIDE)),
                                     extra.reshape((2,) + ring3 + (ROW, EXTRA)), vocab_local)
        qkv = QKV * HALF
        sum_wqkv = total[:, :qkv].reshape(ROW, 3, PAIRS, HD).transpose(0, 2, 1, 3)
        sum_wdense = total[:, qkv:wide].reshape(ROW, PAIRS, HD).transpose(1, 2, 0)
        sum_wfc1, sum_wfc2 = total[:, wide:2 * wide], total[:, 2 * wide:WIDE].T
        last = total[0, WIDE:]
        n1g, n1b, n2g, n2b, bias = last[:ends[0]].reshape(5, ROW)
        return (layer_out, sum_embed.T, n1g, n1b, n2g, n2b, sum_wqkv, last[ends[0]:ends[1]], sum_wdense, bias, sum_wfc1,
                last[ends[1]:ends[2]], sum_wfc2, bias)

    return jax.shard_map(device_step, mesh=mesh, in_specs=arg_specs, out_specs=out_specs, check_vma=False)
```

```python
import functools
import math
import jax
import jax.numpy as jnp
from jax import lax
from jax.experimental import pallas as pl
from jax.experimental.pallas import tpu as pltpu
from jax.sharding import PartitionSpec as P

F32, BF16 = jnp.float32, jnp.bfloat16
NN = (((1,), (0,)), ((), ()))
NT = (((1,), (1,)), ((), ()))
TN = (((0,), (0,)), ((), ()))
S, D, FF, HEADS, HD = 512, 512, 2048, 8, 64
PAIR, HALF, PAIRS, FF_STEPS, ROT_HALF = 2 * HD, S // 2, HEADS // 2, FF // S, HD // 8
QKV, BOTH = 3, range(2)
EPS, ROPE_BASE = 1e-5, 10000.0
LOG2E = 1.4426950408889634
SQRT_HALF, INV_SQRT_2PI = 0.7071067811865476, 0.3989422804014327
RB = 128
VMEM_LIMIT = 67_000_000
ROW, LANES, RING = 8, 128, 4
PAD = 25600
COLOR = PAD // 2
PARTS = 2
WIDE, EXTRA = 3072, 128
GCOLS = WIDE + EXTRA
MESH = pl.DeviceIdType.MESH


def dot(a, b, dims=NN):
    return lax.dot_general(a, b, dims, preferred_element_type=F32)


def rnd(v):
    return v.astype(BF16).astype(F32)


def gelu_parts(a):
    phi = 0.5 + 0.5 * lax.erf(a * SQRT_HALF)
    return a * phi, phi + a * jnp.exp2(a * a * (-0.5 * LOG2E)) * INV_SQRT_2PI


def block(i, n):
    return slice(i * n, i * n + n)


def row_sums(v):
    return jnp.sum(v.reshape(v.shape[0] // ROW, ROW, v.shape[1]), axis=0)


def wcol(half, part, width):
    return slice(half * WIDE + part, half * WIDE + part + width)


def look_up_kernel(codes_ref, table_ref, peer_ref, own_ref, table, sem):
    step = pl.program_id(0)
    half = pl.num_programs(0) * S

    @pl.when(step == 0)
    def _():
        tiles = table_ref.shape[0]
        load = pltpu.make_async_copy(table_ref, table.at[:tiles], sem)
        load.start()
        table[tiles] = jnp.zeros((ROW, D), BF16)
        load.wait()
    sub = lax.broadcasted_iota(jnp.int32, (ROW, D), 0)

    def look_up(first):
        got = jnp.zeros((ROW, D), F32)
        for j in range(ROW):
            at = codes_ref[first + j]
            got = jnp.where(sub == j, pltpu.roll(table[at >> 3].astype(F32), at & (ROW - 1), 0), got)
        return got

    for k, dst in enumerate((own_ref, peer_ref)):
        @pl.loop(0, S // ROW, unroll=2)
        def _(g):
            t0 = pl.multiple_of(g * ROW, ROW)
            dst[0, pl.ds(t0, ROW), :] = look_up(k * half + step * S + t0).astype(dst.dtype)


def look_up_call(codes, table):
    seqs = codes.size // (2 * S)
    seq = pl.BlockSpec((1, S, D), lambda i, _: (i, 0, 0))
    return pl.pallas_call(
        look_up_kernel,
        grid_spec=pltpu.PrefetchScalarGridSpec(
            num_scalar_prefetch=1, grid=(seqs,), in_specs=[pl.BlockSpec(memory_space=pl.ANY)], out_specs=[seq] * 2,
            scratch_shapes=[pltpu.VMEM((table.shape[0] + 1, ROW, D), BF16), pltpu.SemaphoreType.DMA]),
        out_shape=[jax.ShapeDtypeStruct((seqs, S, D), t) for t in (F32, BF16)],
        compiler_params=pltpu.CompilerParams(dimension_semantics=("arbitrary",), vmem_limit_bytes=VMEM_LIMIT),
        cost_estimate=pl.CostEstimate(flops=40_000_000_000, bytes_accessed=40_000_000, transcendentals=0),
        name="look_up",
    )(codes, table)


def layer_kernel(xo_ref, cot_ref, g1_ref, b1_ref, g2_ref, b2_ref, bd_ref, bf_ref, bq_ref, bf1_ref, rope_ref, xs_ref, ids_ref, qo_ref, do_ref, fo_ref, to_ref, rp_ref, fp_ref,
                 out_ref, rows_ref, xin_ref, idz_ref, gw_out, gs_out, gb1_out,
                 bo_scr, bp_scr, gw_ref, gs_ref, gb1_ref, wqkv, wd, w1, w2, n_scr, acc_scr, dh2_scr, dh1_scr, inv_scr, h1_scr, h2_scr, h1t_scr, h2t_scr, cott_scr, dctx_scr, ctx_scr,
                 qkv_scr, dqkv_scr, s_scr, dp_scr, pb_scr, ds_scr, a_scr, du_scr, u_scr, da_scr, dk_scr, dv_scr,
                 xp_buf, gx_buf, out_buf, peer_buf, own_low, peer_low, x_send, x_recv, x_load, id_send, id_recv, gx_send, gx_recv, gx_local, out_send, out_recv, own_sem, peer_sem, init_sem):
    step, last = pl.program_id(0), pl.num_programs(0) - 1
    slot = step % 2
    core, chip = lax.axis_index('tp'), lax.axis_index('dp')
    chips = lax.axis_size('dp')
    plane = chips // RING
    z, peer = chip // plane, (1 - core, chip)

    def z_device(k):
        return (core, (chip + k * plane) % chips)

    def x_copy(at):
        return pltpu.make_async_remote_copy(xs_ref.at[at], xin_ref.at[at], x_send.at[at], x_recv.at[at], device_id=peer, device_id_type=MESH)

    def x_take(at):
        return pltpu.make_async_copy(xin_ref.at[at], xp_buf.at[at % 2], x_load.at[at % 2])

    def id_copy(k):
        if k:
            return pltpu.make_async_remote_copy(ids_ref, idz_ref.at[k], id_send.at[k], id_recv.at[k], device_id=z_device(k), device_id_type=MESH)
        return pltpu.make_async_copy(ids_ref, idz_ref.at[k], id_send.at[RING])

    @pl.when(step == 0)
    def _():
        barrier = pltpu.get_barrier_semaphore()
        near = [peer] + [z_device(k) for k in range(1, RING)]
        for who in near:
            pl.semaphore_signal(barrier, inc=1, device_id=who, device_id_type=MESH)
        pl.semaphore_wait(barrier, len(near))

        @pl.loop(0, last + 1)
        def _(at):
            x_copy(at).start()
        for k in range(RING):
            id_copy(k).start()
        for dst in (gw_ref, gs_ref, gb1_ref):
            dst[...] = jnp.zeros_like(dst)
        n = FF // 2
        bo_scr[...] = jnp.zeros_like(bo_scr)
        bo_scr[QKV:, :] = bf1_ref[...].astype(F32).reshape(1, n)
        for j in range(QKV):
            for h in range(RING):
                bo_scr[j:j + 1, block(h, HD)] = bq_ref[j, h:h + 1, :].astype(F32)
        moves = [(qo_ref.at[block(j, HALF)], wqkv.at[block(2 * j, HALF)]) for j in range(QKV)]
        moves += [(do_ref, wd.at[:HALF]), (to_ref, w2.at[:n]), (fo_ref, w1.at[:, :n])]
        tables = (n_scr, acc_scr, dh2_scr, dh1_scr, s_scr.at[0], s_scr.at[1])
        parts = [rp_ref.at[block(i, S)] for i in range(RING)] + [fp_ref.at[:, block(i, S)] for i in BOTH]
        copies = [pltpu.make_async_copy(src, dst, init_sem.at[i]) for i, (src, dst) in enumerate(moves + list(zip(parts, tables)))]
        for c in copies:
            c.start()
        biases = pltpu.make_async_remote_copy(bo_scr, bp_scr, id_send.at[0], id_recv.at[0], device_id=peer, device_id_type=MESH)
        for c in copies:
            c.wait()
        biases.start()
        biases.wait()
        for j in range(QKV):
            wqkv[block(2 * j + 1, HALF), :] = tables[j // 2][block(j % 2, HALF), :].astype(BF16)
        wd[HALF:, :] = tables[1][HALF:, :].astype(BF16)
        for i in BOTH:
            w2[block(2 + i, S), :] = tables[2 + i][...].astype(BF16)
            w1[:, block(2 + i, S)] = tables[RING + i][...].astype(BF16)

        x_copy(0).wait_recv()
        x_take(0).start()

    x_take(step).wait()

    @pl.when(step < last)
    def _():
        x_copy(step + 1).wait_recv()
        x_take(step + 1).start()

    def gx_copy(at, k):
        rows = pl.ds(pl.multiple_of(at * S, S), S)
        src, dst = gx_buf.at[at % 2, k], rows_ref.at[k, rows]
        if k:
            return pltpu.make_async_remote_copy(src, dst, gx_send.at[at % 2, k], gx_recv.at[at, k], device_id=z_device(k), device_id_type=MESH)
        return pltpu.make_async_copy(src, dst, gx_local.at[at % 2])

    def out_copy(at):
        return pltpu.make_async_remote_copy(out_buf.at[at % 2], peer_buf.at[at], out_send.at[at % 2], out_recv.at[at], device_id=peer, device_id_type=MESH)

    def own_store(at):
        return pltpu.make_async_copy(own_low.at[at % 2], out_ref.at[core * (last + 1) + at], own_sem.at[at % 2])

    def peer_store(at):
        return pltpu.make_async_copy(peer_low.at[at % 2], out_ref.at[(1 - core) * (last + 1) + at], peer_sem.at[at % 2])

    def drain(at):
        gx_copy(at, 0).wait()
        for k in range(1, RING):
            gx_copy(at, k).wait_send()
        out_copy(at).wait_send()
        own_store(at).wait()

    def take_peer(at):
        out_copy(at).wait_recv()

        @pl.when(at > 1)
        def _():
            peer_store(at - 2).wait()
        peer_low[at % 2] = peer_buf[at].astype(BF16)
        peer_store(at).start()

    @pl.when(step > 1)
    def _():
        drain(step - 2)

    cot = cot_ref[0]
    g1, b1, g2, b2, bd, bf = (v[...].astype(F32).reshape(1, D) for v in (g1_ref, b1_ref, g2_ref, b2_ref, bd_ref, bf_ref))
    bo = bd + bf

    def bias(row, i, n):
        width = HALF if row < 3 else FF // 2
        src, i = (bo_scr, i) if i < width // n else (bp_scr, i - width // n)
        return src[row:row + 1, block(i, n)]

    dctx_scr[...] = dot(cot, wd[...], NT).astype(BF16)
    cott_scr[...] = cot.T
    x = xo_ref[0].astype(F32) + xp_buf[slot]
    cen = x - jnp.mean(x, axis=-1, keepdims=True)
    inv = lax.rsqrt(jnp.mean(cen * cen, axis=-1, keepdims=True) + EPS)
    n = cen * inv
    n_scr[...] = n
    inv_scr[...] = inv
    h1_scr[...] = (n * g1 + b1).astype(BF16)
    h2_scr[...] = (n * g2 + b2).astype(BF16)
    gs_ref[4] += row_sums(cot.astype(F32))
    h1t_scr[...] = h1_scr[...].T
    h2t_scr[...] = h2_scr[...].T
    h1, h2 = h1_scr[...], h2_scr[...]

    for p in range(PAIRS):
        for j in range(QKV):
            v = dot(h1, wqkv[block(j * PAIRS + p, PAIR), :], NT) + bias(j, p, PAIR)
            v = v.astype(BF16)
            if j < 2:
                v = v.astype(F32)
                v = (v * rope_ref[0] + pltpu.roll(v, PAIR - ROT_HALF, 1) * rope_ref[1]
                     + pltpu.roll(v, ROT_HALF, 1) * rope_ref[2]).astype(BF16)
            qkv_scr[j, :, block(p, PAIR)] = v

    lane = lax.broadcasted_iota(jnp.int32, (HALF, PAIR), 1)
    causal = lax.broadcasted_iota(jnp.int32, (HALF, HALF), 0) >= lax.broadcasted_iota(jnp.int32, (HALF, HALF), 1)
    heads = (lane < HD, lane >= HD)
    zero = jnp.zeros((HALF, PAIR), BF16)

    def only(v, hh):
        return jnp.concatenate([jnp.where(heads[hh], v[block(i, HALF)], zero) for i in range(v.shape[0] // HALF)], axis=0)

    def rope_back(g, rows):
        g = rnd(g * HD ** -0.5)
        return (g * rope_ref[0, rows] + pltpu.roll(g * rope_ref[1, rows], ROT_HALF, 1)
                + pltpu.roll(g * rope_ref[2, rows], PAIR - ROT_HALF, 1)).astype(BF16)

    class Attention:
        def __init__(self, i):
            p, self.qb = i // 2, i % 2
            self.n, self.slot, self.lanes, self.rows = HALF * (self.qb + 1), self.qb, block(p, PAIR), block(self.qb, HALF)

        def operands(self):
            q, dc = qkv_scr[0, self.rows, self.lanes], dctx_scr[self.rows, self.lanes]
            return q, dc, qkv_scr[1, :self.n, self.lanes], qkv_scr[2, :self.n, self.lanes]

        def one(self):
            q, dc, k, v = self.operands()
            for hh in BOTH:
                at = (self.slot, block(hh, HALF), slice(self.n))
                s_scr[at] = dot(only(q, hh), k, NT)
                dp_scr[at] = dot(only(dc, hh), v, NT).astype(BF16)

        def two(self):
            for hh in BOTH:
                at = (self.slot, block(hh, HALF), slice(self.n))
                s = s_scr[at]
                diag = jnp.where(causal, s[:, self.n - HALF:], -1e30)
                s = jnp.concatenate([s[:, :HALF], diag], axis=1) if self.qb else diag
                e = jnp.exp2((s - jnp.max(s, axis=-1, keepdims=True)) * (HD ** -0.5 * LOG2E))
                pr = e * (1.0 / jnp.sum(e, axis=-1, keepdims=True))
                pb_scr[at] = pr.astype(BF16)
                dp = dp_scr[at].astype(F32)
                ds_scr[at] = (pr * (dp - jnp.sum(pr * dp, axis=-1, keepdims=True))).astype(BF16)

        def three(self):
            q, dc, k, v = self.operands()
            pb, ds = pb_scr[self.slot, :, :self.n], ds_scr[self.slot, :, :self.n]
            rows, lanes = self.rows, self.lanes
            ctx_scr[rows, lanes] = sum(dot(pb[block(hh, HALF)], only(v, hh)) for hh in BOTH).astype(BF16)
            dqkv_scr[0, rows, lanes] = rope_back(sum(dot(ds[block(hh, HALF)], only(k, hh)) for hh in BOTH), rows)
            dk = dot(ds, jnp.concatenate([only(q, hh) for hh in BOTH], axis=0), TN)
            dv = dot(pb, jnp.concatenate([only(dc, hh) for hh in BOTH], axis=0), TN)
            if not self.qb:
                dk_scr[...] = dk
                dv_scr[...] = dv
                return
            for b in BOTH:
                at = block(b, HALF)
                gk, gv = (dk[at], dv[at]) if b else (dk[at] + dk_scr[...], dv[at] + dv_scr[...])
                dqkv_scr[1, at, lanes] = rope_back(gk, at)
                dqkv_scr[2, at, lanes] = gv.astype(BF16)

    class Mlp:
        def __init__(self, i):
            self.i, self.slot, self.cols = i, i % 2, block(i, HALF)

        def one(self):
            a_scr[self.slot] = dot(h2, w1[:, self.cols]) + bias(3, self.i, HALF)
            du_scr[self.slot] = dot(cot, w2[self.cols, :], NT).astype(BF16)

        def two(self):
            u, gp = gelu_parts(rnd(a_scr[self.slot]))
            da = (du_scr[self.slot].astype(F32) * gp).astype(BF16)
            u_scr[self.slot] = u.astype(BF16)
            da_scr[self.slot] = da
            gb1_ref[:, self.cols] += row_sums(da.astype(F32))

        def three(self):
            u, da = u_scr[self.slot], da_scr[self.slot]
            m, d = dot(u, w2[self.cols, :]), dot(da, w1[:, self.cols], NT)
            acc_scr[...] = acc_scr[...] + m if self.i else m
            dh2_scr[...] = dh2_scr[...] + d if self.i else d
            half, part = self.i // RING, 2 * S + self.i % RING * HALF
            gw_ref[:, wcol(half, part, HALF)] += dot(h2t_scr[...], da)
            gw_ref[:, wcol(half, part + 2 * S, HALF)] += dot(cott_scr[...], u)

    units = [u for i in range(2 * PAIRS) for u in (Attention(i), Mlp(i))]
    units[0].one()
    for i, u in enumerate(units):
        if i + 1 < len(units):
            units[i + 1].one()
        u.two()
        if i:
            units[i - 1].three()
    units[-1].three()

    dh1_scr[...] = sum(dot(dqkv_scr[j], wqkv[block(j, S), :]) for j in range(QKV))
    acc_scr[...] += dot(ctx_scr[...], wd[...])
    for half in BOTH:
        hs = block(half, HALF)
        for j in range(QKV):
            gw_ref[:, wcol(half, j * HALF, HALF)] += dot(h1t_scr[...], dqkv_scr[j, :, hs])
        gw_ref[:, wcol(half, QKV * HALF, HALF)] += dot(cott_scr[...], ctx_scr[:, hs])

    n = n_scr[...]
    d1, d2 = rnd(dh1_scr[...]), rnd(dh2_scr[...])
    for i, v in zip((0, 1, 2, 3, 5, 6, 7), (d1 * n, d1, d2 * n, d2, *(dqkv_scr[j].astype(F32) for j in range(QKV)))):
        gs_ref[i] += row_sums(v)
    gn = d1 * g1 + d2 * g2
    s_scr[0] = cot.astype(F32) + inv_scr[...] * (
        gn - jnp.mean(gn, axis=-1, keepdims=True) - n * jnp.mean(gn * n, axis=-1, keepdims=True))
    low = (xo_ref[0].astype(F32) + xp_buf[slot] + (acc_scr[...] + bo)).astype(BF16)
    own_low[slot] = low
    out_buf[slot] = low.astype(F32)
    for k in range(RING):
        gx_buf[slot, k] = s_scr[0, :, pl.ds(pl.multiple_of((z + k) % RING * LANES, LANES), LANES)]
    for k in (2, 1, 3, 0):
        gx_copy(step, k).start()
    out_copy(step).start()
    own_store(step).start()

    @pl.when(step > 0)
    def _():
        take_peer(step - 1)

    @pl.when(step == last)
    def _():
        save = pltpu.make_async_copy(gw_ref, gw_out, init_sem.at[0])
        save.start()
        gs_out[...] = jnp.sum(gs_ref[...], axis=1)
        gb1_out[...] = jnp.sum(gb1_ref[...], axis=0)
        take_peer(step)
        for at in (step - 1, step):
            drain(at)
            peer_store(at).wait()

        @pl.loop(0, last + 1)
        def _(at):
            x_copy(at).wait_send()
            for k in range(1, RING):
                gx_copy(at, k).wait_recv()
        save.wait()
        for k in range(RING):
            id_copy(k).wait()


def rope_consts():
    lane = lax.broadcasted_iota(jnp.int32, (S, PAIR), 1) % HD
    inv_freq = ROPE_BASE ** (-(lane % ROT_HALF).astype(F32) / ROT_HALF)
    ang = lax.broadcasted_iota(F32, (S, PAIR), 0) * inv_freq
    sin, low, rot = jnp.sin(ang), lane < ROT_HALF, lane < 2 * ROT_HALF
    return jnp.stack([jnp.where(rot, jnp.cos(ang), 1.0), jnp.where(low, -sin, 0.0), jnp.where(rot & ~low, sin, 0.0)])


def layer_call(*args):
    count = args[0].shape[0]
    vm, hbm = pl.BlockSpec(memory_space=pltpu.VMEM), pl.BlockSpec(memory_space=pl.ANY)
    seq = pl.BlockSpec((1, S, D), lambda i: (i, 0, 0))
    own_seq = pl.BlockSpec((1, S, D), lambda i: (lax.axis_index('tp') * count + i, 0, 0))
    dma = pltpu.SemaphoreType.DMA

    def table(*lead):
        return pltpu.VMEM(lead + (S, D), F32)

    def low(*lead):
        return pltpu.VMEM(lead + (S, D), BF16)
    thin, thin_low, small = pltpu.VMEM((2, S, HALF), F32), pltpu.VMEM((2, S, HALF), BF16), pltpu.VMEM((HALF, PAIR), F32)
    return pl.pallas_call(
        layer_kernel,
        grid=(count,),
        in_specs=[seq, own_seq] + [vm] * 9 + [hbm] * (len(args) - 11),
        out_specs=[hbm] * 5 + [vm] * 2,
        out_shape=[jax.ShapeDtypeStruct((2 * count, S, D), BF16), jax.ShapeDtypeStruct((RING, count * S, LANES), F32), jax.ShapeDtypeStruct((count, S, D), F32), jax.ShapeDtypeStruct((RING, count * S // LANES, LANES), jnp.int32),
                   jax.ShapeDtypeStruct((D, 2 * WIDE), F32), jax.ShapeDtypeStruct((ROW, D), F32), jax.ShapeDtypeStruct((FF,), F32)],
        scratch_shapes=[pltpu.VMEM((RING, FF // 2), F32)] * 2 + [pltpu.VMEM((D, 2 * WIDE), F32), pltpu.VMEM((ROW, ROW, D), F32), pltpu.VMEM((ROW, FF), F32), pltpu.VMEM((QKV * S, D), BF16), low(), pltpu.VMEM((D, FF), BF16), pltpu.VMEM((FF, D), BF16)] + [table()] * 4
        + [pltpu.VMEM((S, 1), F32)] + [low()] * 7 + [low(3)] * 2 + [table(2)] + [low(2)] * 3 + [thin] + [thin_low] * 3 + [small] * 2
        + [table(2), pltpu.VMEM((2, RING, S, LANES), F32), table(2), table(count)] + [low(2)] * 2
        + [dma((count,)), dma((count,)), dma((2,)), dma((RING + 1,)), dma((RING,)), dma((2, RING)), dma((count, RING)), dma((2,)), dma((2,)), dma((count,)), dma((2,)), dma((2,)), dma((16,))],
        compiler_params=pltpu.CompilerParams(dimension_semantics=("arbitrary",), collective_id=1, has_side_effects=True,
                                             vmem_limit_bytes=VMEM_LIMIT),
        cost_estimate=pl.CostEstimate(flops=count * 30_000_000_000, bytes_accessed=60_000_000, transcendentals=0),
        name="layer",
    )(*args)


STEPS, UNROLL = 8, 16
STEP = PAD // STEPS


def table_kernel(half, ids_ref, rows_hbm, lo_ref, out_ref, lo_out_ref, rows_ref, acc, acc2, stage, lo_buf, sem, lo_in, lo_sent):
    load = pltpu.make_async_copy(rows_hbm, rows_ref, sem.at[0])
    load.start()

    @pl.loop(0, acc.shape[0] // LANES)
    def _(j):
        for a in (acc, acc2):
            a[pl.ds(pl.multiple_of(j * LANES, LANES), LANES), :] = jnp.zeros((LANES, LANES), F32)
    count, blocks = rows_ref.shape[1], lo_ref.shape[0]
    part = RING // 2 * count // blocks
    per = count // part

    def lo_load(i):
        return pltpu.make_async_copy(lo_ref.at[i], lo_buf.at[i % 2], lo_in.at[i % 2])

    def lo_store(i):
        return pltpu.make_async_copy(lo_buf.at[i % 2], lo_out_ref.at[i], lo_sent.at[i % 2])
    lo_load(0).start()
    load.wait()

    @pl.loop(0, blocks)
    def _(i):
        lo_load(i).wait()
        lo_store(i).start()

        @pl.when(i > 0)
        def _():
            lo_store(i - 1).wait()

        @pl.when(i + 1 < blocks)
        def _():
            lo_load(i + 1).start()
        k, first = i // per * 2, i % per * part

        @pl.loop(0, part // UNROLL)
        def _(g):
            t0 = pl.multiple_of(first + g * UNROLL, UNROLL)
            for j in range(0, UNROLL, 2):
                pairs = []
                for a, src in ((acc, k), (acc2, k + 1)):
                    i0, i1 = (ids_ref[src * count + t0 + j + d] for d in BOTH)
                    x0, x1 = (rows_ref[src, pl.ds(t0 + j + d, 1), :] for d in BOTH)
                    r0, r1 = pl.ds(i0, 1), pl.ds(i1, 1)
                    pairs.append((a, r0, a[r0, :] + x0, r1, a[r1, :] + (x1 + jnp.where(i0 == i1, x0, 0.0))))
                for a, r0, v0, r1, v1 in pairs:
                    a[r0, :] = v0
                    a[r1, :] = v1
    lo_store(blocks - 1).wait()
    copies = []
    for i in range(2 * STEPS):
        h, c, slot = i // STEPS, i % STEPS, i % 2
        if i > 1:
            copies[i - 2].wait()

        @pl.loop(0, STEP // LANES, unroll=5)
        def _(b):
            at = pl.ds(pl.multiple_of(h * half + c * STEP + b * LANES, ROW), LANES)
            stage[slot, :, pl.ds(pl.multiple_of(b * LANES, LANES), LANES)] = (acc[at, :] + acc2[at, :]).T
        copies.append(pltpu.make_async_copy(stage.at[slot], out_ref.at[h, :, pl.ds(c * STEP, STEP)], sem.at[slot]))
        copies[i].start()
    for c in copies[-2:]:
        c.wait()


def table_call(ids, rows, lo, half):
    hbm, dma = pl.BlockSpec(memory_space=pl.ANY), pltpu.SemaphoreType.DMA((2,))
    return pl.pallas_call(
        functools.partial(table_kernel, half),
        grid_spec=pltpu.PrefetchScalarGridSpec(
            num_scalar_prefetch=1, grid=(), in_specs=[hbm] * 2, out_specs=[hbm] * 2,
            scratch_shapes=[pltpu.VMEM(rows.shape, F32)] + [pltpu.VMEM((half + PAD, LANES), F32)] * 2 + [pltpu.VMEM((2, LANES, STEP), F32), pltpu.VMEM((2, S, D), BF16)]
            + [dma] * 3),
        out_shape=[jax.ShapeDtypeStruct((2, LANES, PAD), F32), jax.ShapeDtypeStruct(lo.shape, lo.dtype)],
        compiler_params=pltpu.CompilerParams(vmem_limit_bytes=VMEM_LIMIT),
        cost_estimate=pl.CostEstimate(flops=4_000_000_000, bytes_accessed=34_000_000, transcendentals=0),
        name="table",
    )(ids, rows, lo)


def cut(lo, n):
    first = n // (2 * LANES) * LANES
    return (lo, first), (lo + first, n - first)


def over(lead, body, at=()):
    if not lead:
        return body(at)

    @pl.loop(0, lead[0])
    def _(i):
        over(lead[1:], body, at + (i,))


def add_into(dst, srcs, lead, lo, n):
    def body(at):
        v = dst[at + (slice(None), pl.ds(lo, n))]
        for s in srcs:
            v = v + s[at + (slice(None), pl.ds(0, n))]
        dst[at + (slice(None), pl.ds(lo, n))] = v
    over(lead, body)


def tail_kernel(t_ref, g_ref, e_ref, oute_ref, outw_ref, *scratch):
    tsum, tpeer, gsum, gpeer, send, recv, local = scratch[:7]
    bufs = list(scratch[7:])
    core, dp = lax.axis_index('tp'), lax.axis_index('dp')
    pos = {'z': dp // (RING * RING), 'y': dp // RING % RING, 'x': dp % RING}
    stride = {'z': RING * RING, 'y': RING, 'x': 1}

    def shift(axis, k):
        return (pos[axis] + k) % RING

    def device(axis, k):
        return (core, dp + (shift(axis, k) - pos[axis]) * stride[axis])
    peer = (1 - core, dp)

    barrier = pltpu.get_barrier_semaphore()
    near = [peer] + [device(axis, k) for axis in 'zyx' for k in (1, RING - 1)]
    for who in near:
        pl.semaphore_signal(barrier, inc=1, device_id=who, device_id_type=MESH)
    pl.semaphore_wait(barrier, len(near))

    used = [0, 0]

    def remote(src, dst, who):
        i = used[0]
        used[0] += 1
        c = pltpu.make_async_remote_copy(src, dst, send.at[i], recv.at[i], device_id=who, device_id_type=MESH)
        c.start()
        return c

    def load(src, dst):
        i = used[1]
        used[1] += 1
        c = pltpu.make_async_copy(src, dst, local.at[i])
        c.start()
        return c
    sent = []

    wide, extra, far = pl.ds(0, WIDE), pl.ds(WIDE, EXTRA), pl.ds(WIDE, WIDE)
    every = slice(None)
    py, px, pz = pos['y'], pos['x'], pos['z']
    width = COLOR // PARTS
    flows = {}
    for q in range(PARTS):
        for axis, lo in (('y', q * width), ('x', COLOR + q * width)):
            flows[lo] = axis
    pend = {}

    def piece(axis, i):
        return (i,) if axis in 'yz' else (every, i)

    def fetch(lo, k):
        axis = flows[lo]
        at = piece(axis, shift(axis, k)) + (every,) * (2 if axis == 'y' else 1) + (pl.ds(lo, width),)
        pend[lo, k] = [remote(t_ref.at[(1,) + at], tpeer.at[at], peer), load(t_ref.at[(0,) + at], tsum.at[at])]

    def fetch_g(k):
        i = shift('z', k)
        pend['g', k] = [remote(g_ref.at[i, every, every, every, far], gpeer.at[i, every, every, every, wide], peer),
                        load(g_ref.at[i, every, every, every, wide], gsum.at[i, every, every, every, wide])]
    order = list(flows)
    for k in (2, 1, RING - 1, 0):
        for n, lo in enumerate(order):
            fetch(lo, k)
            if n == 1:
                if k == 2:
                    pend['e'] = [remote(e_ref.at[1], gpeer.at[every, every, every, every, extra], peer),
                                 load(e_ref.at[0], gsum.at[every, every, every, every, extra])]
                fetch_g(k)

    def arrive(key):
        out, here = pend[key]
        sent.append(out)
        out.wait_recv()
        here.wait()

    def ready(name, k):
        arrive((name, k))
        if name == 'g':
            i = shift('z', k)
            add_into(gsum.at[i], [gpeer.at[i]], (RING, RING), 0, GCOLS)
            return
        axis = flows[name]
        at = piece(axis, shift(axis, k))
        v = at + (every,) * (2 if axis == 'y' else 1) + (pl.ds(name, width),)
        add_into(tsum.at[at], [tpeer.at[v]], (RING,), name, width)

    class Stage:
        def __init__(self, axis, piece, lead, lo, n, need=None):
            self.axis, self.piece, self.lead, self.lo, self.n, self.need = axis, piece, lead, lo, n, need
            self.halves = cut(lo, n)
            self.near = [bufs.pop(0), bufs.pop(0)]
            self.last = [bufs.pop(0), bufs.pop(0)]

        def view(self, k, lo, n):
            return self.piece(shift(self.axis, k)).at[(every,) * (len(self.lead) + 1) + (pl.ds(lo, n),)]

        def want(self, k):
            if self.need is not None:
                ready(self.need, k)

        def first(self):
            self.want(2)
            self.c1 = [remote(self.view(2, *self.halves[s]), self.near[s], device(self.axis, k))
                       for s, k in enumerate((1, RING - 1))]

        def second(self):
            self.want(1)
            self.want(RING - 1)
            self.c2 = []
            for s, k in enumerate((1, RING - 1)):
                self.c1[s].wait_recv()
                add_into(self.piece(shift(self.axis, k)), [self.near[s]], self.lead, *self.halves[s])
                self.c2.append(remote(self.view(k, self.lo, self.n), self.last[s], device(self.axis, k)))

        def finish(self):
            self.want(0)
            for c in self.c2:
                c.wait_recv()
            add_into(self.piece(shift(self.axis, 0)), self.last, self.lead, self.lo, self.n)
            sent.extend(self.c1 + self.c2)

    one, two = (RING,), (RING, RING)
    rows_y, rows_x = (lambda i: tsum.at[i]), (lambda i: tsum.at[:, i])
    last_x, last_y = (lambda i: tsum.at[py, i]), (lambda i: tsum.at[i, px])
    first = [Stage(axis, rows_y if axis == 'y' else rows_x, one, lo, width, lo) for lo, axis in flows.items()]
    g1 = Stage('z', lambda i: gsum.at[i], two, 0, GCOLS, 'g')
    second = [Stage('x' if axis == 'y' else 'y', last_x if axis == 'y' else last_y, (), lo, width) for lo, axis in flows.items()]
    (c0, cn), (d0, dn) = cut(0, GCOLS)
    c1 = Stage('y', lambda i: gsum.at[pz, i], one, c0, cn)
    d1 = Stage('x', lambda i: gsum.at[pz, :, i], one, d0, dn)
    c2 = Stage('x', lambda i: gsum.at[pz, py, i], (), c0, cn)
    d2 = Stage('y', lambda i: gsum.at[pz, i, px], (), d0, dn)

    firsts = first[:2] + [g1] + first[2:]
    after = dict(zip(first, ([s] for s in second)))
    after[g1] = [c1, d1]
    for s in firsts:
        if s is g1:
            arrive('e')
        s.first()
    for s in firsts:
        s.second()
    for s in firsts:
        s.finish()
        for t in after[s]:
            t.first()
    nexts = [t for s in firsts for t in after[s]]
    for s in nexts:
        s.second()
    for s, t in ((c1, c2), (d1, d2)):
        s.finish()
        t.first()
    for s in second:
        s.finish()
    oute_ref[...] = tsum[py, px, :, 0:oute_ref.shape[1]]
    for s in (c2, d2):
        s.second()
    for s in (c2, d2):
        s.finish()
    outw_ref[...] = gsum[pz, py, px]
    for c in sent:
        c.wait_send()


def tail_call(t, g, e, rows):
    def ring_bufs(lead, n):
        (_, p), (_, q) = cut(0, n)
        return [pltpu.VMEM(lead + (ROW, w), F32) for w in (p, q, n, n)]
    (_, cn), (_, dn) = cut(0, GCOLS)
    one, two, three = (RING,), (RING,) * 2, (RING,) * 3
    width = COLOR // PARTS
    bufs = sum((ring_bufs(*b) for b in [(one, width)] * (2 * PARTS) + [(two, GCOLS)] + [((), width)] * (2 * PARTS)
                + [(one, cn), (one, dn), ((), cn), ((), dn)]), [])
    dma = pltpu.SemaphoreType.DMA
    hbm = pl.BlockSpec(memory_space=pl.ANY)
    vm = pl.BlockSpec(memory_space=pltpu.VMEM)
    return pl.pallas_call(
        tail_kernel,
        in_specs=[hbm] * 3, out_specs=[vm] * 2,
        out_shape=[jax.ShapeDtypeStruct((ROW, rows), F32), jax.ShapeDtypeStruct((ROW, GCOLS), F32)],
        scratch_shapes=[pltpu.VMEM(two + (ROW, PAD), F32)] * 2 + [pltpu.VMEM(three + (ROW, GCOLS), F32)] * 2
        + [dma((128,)), dma((128,)), dma((32,))] + bufs,
        compiler_params=pltpu.CompilerParams(collective_id=0, has_side_effects=True, vmem_limit_bytes=VMEM_LIMIT),
        name="tail",
    )(t, g, e)


def finish_kernel(e_ref, w_ref, oe, o1, o2, oq, od, *small):
    oe[...] = e_ref[...]
    wide = RING * HALF
    for dst, at in ((o1, wide), (o2, 2 * wide)):
        dst[...] = w_ref[:, at:at + wide]
    for h in range(RING):
        for j in range(QKV):
            oq[:, j, h, :] = w_ref[:, j * HALF + h * HD:j * HALF + (h + 1) * HD]
        od[h] = w_ref[:, block(QKV * RING + h, HD)]
    at = WIDE
    for dst in small:
        n = dst.shape[0]
        dst[...] = w_ref[0, at:at + n]
        at += n


def finish_call(e, w, small):
    shape = jax.ShapeDtypeStruct
    vm = pl.BlockSpec(memory_space=pltpu.VMEM)
    outs = [shape(e.shape, F32)] + [shape((ROW, RING * HALF), F32)] * 2 + [shape((ROW, QKV, RING, HD), F32), shape((RING, ROW, HD), F32)]
    outs += [shape((n,), F32) for n in small]
    return pl.pallas_call(finish_kernel, in_specs=[vm] * 2, out_specs=[vm] * len(outs), out_shape=outs, name="finish")(e, w)


def solution(mesh):
    tp, dp, no = 'tp', 'dp', None
    one, vec_dp, both = P(no), P(dp), P((tp, dp))
    arg_specs = (P(dp, no), P(tp, no), one, one, one, one, P(no, tp, no, no), P(tp, no, no), P(tp, no, no), one, P(no, tp), P(tp), P(tp, no), one, P(dp, no, no))
    out_specs = (P(dp, no, no), P(tp, dp), vec_dp, vec_dp, vec_dp, vec_dp, P(dp, tp, no, no), both, P(tp, no, dp), vec_dp, P(dp, tp), both, P(tp, dp), vec_dp)
    chips = mesh.shape[dp]

    def swap(v):
        return lax.ppermute(v, tp, [(0, 1), (1, 0)])

    def device_step(token_ids, embed_table, ln1_gain, ln1_bias, ln2_gain, ln2_bias, w_qkv, b_qkv, w_dense, b_dense, w_fc1, b_fc1, w_fc2, b_fc2, cotangent):
        core = lax.axis_index(tp)
        vocab_local = embed_table.shape[0]
        seqs = token_ids.shape[0] // 2
        f = lambda v: v.astype(F32)

        wq_own = w_qkv.transpose(2, 1, 3, 0).reshape(QKV * HALF, D)
        wd_own = w_dense.reshape(HALF, D)
        rows_peer = swap(f(jnp.concatenate([wq_own, wd_own, w_fc2], axis=0)))
        fc1_peer = swap(f(w_fc1))

        tokens = jnp.where(core == 0, token_ids, jnp.roll(token_ids, seqs, axis=0)).reshape(-1)
        local = tokens - core * vocab_local
        row = jnp.where((local >= 0) & (local < vocab_local), local, vocab_local)
        codes = (row & -ROW) | ((lax.iota(jnp.int32, tokens.size) - row) & (ROW - 1))
        x_send, x_own = look_up_call(codes, embed_table.reshape(-1, ROW, D))
        ids = jnp.where(local < 0, local + 2 * vocab_local, local)[:seqs * S].reshape(-1, LANES)

        args = (x_own, cotangent, ln1_gain, ln1_bias, ln2_gain, ln2_bias, b_dense, b_fc2, b_qkv.transpose(1, 0, 2), b_fc1, rope_consts(), x_send, ids, wq_own, wd_own, w_fc1, w_fc2, rows_peer, fc1_peer)
        layer_out, rows, _, ids, grad_w, small, grad_b1 = layer_call(*args)

        dense, layer_out = table_call(ids.reshape(-1), rows, layer_out, vocab_local)

        norms = small[:5].reshape(5, chips, ROW).transpose(1, 0, 2).reshape(chips, 5 * ROW)
        norms = jnp.concatenate([norms, norms[:, -ROW:]], axis=1)
        grad_bq = small[5:].reshape(3, 2, PAIRS, HD).transpose(1, 2, 0, 3).reshape(2, chips, -1)
        grad_bf = grad_b1.reshape(2, chips, -1)
        extra = jnp.concatenate([jnp.stack([norms, norms]), grad_bq, grad_bf], axis=2)
        extra = jnp.pad(extra[:, :, None, :], ((0, 0), (0, 0), (0, ROW - 1), (0, EXTRA - extra.shape[2])))
        ring3 = (RING,) * 3
        sum_embed, total = tail_call(dense.reshape(2, RING, RING, ROW, PAD), grad_w.reshape(ring3 + (ROW, 2 * WIDE)),
                                     extra.reshape((2,) + ring3 + (ROW, EXTRA)), vocab_local)
        small = [ROW] * 6 + [grad_bq.shape[2], grad_bf.shape[2]]
        sum_embed, sum_wfc1, sum_wfc2, sum_wqkv, sum_wdense, n1g, n1b, n2g, n2b, bias, bias2, bq, bf1 = finish_call(sum_embed, total, small)
        return (layer_out, sum_embed.T, n1g, n1b, n2g, n2b, sum_wqkv.transpose(0, 2, 1, 3), bq, sum_wdense.transpose(0, 2, 1), bias, sum_wfc1,
                bf1, sum_wfc2.T, bias2)

    return jax.shard_map(device_step, mesh=mesh, in_specs=arg_specs, out_specs=out_specs, check_vma=False)
```

```python
import functools
import math
import jax
import jax.numpy as jnp
from jax import lax
from jax.experimental import pallas as pl
from jax.experimental.pallas import tpu as pltpu
from jax.sharding import PartitionSpec as P

F32, BF16 = jnp.float32, jnp.bfloat16
NN = (((1,), (0,)), ((), ()))
NT = (((1,), (1,)), ((), ()))
TN = (((0,), (0,)), ((), ()))
S, D, FF, HEADS, HD = 512, 512, 2048, 8, 64
PAIR, HALF, PAIRS, FF_STEPS, ROT_HALF = 2 * HD, S // 2, HEADS // 2, FF // S, HD // 8
QKV, BOTH = 3, range(2)
EPS, ROPE_BASE = 1e-5, 10000.0
LOG2E = 1.4426950408889634
SQRT_HALF, INV_SQRT_2PI = 0.7071067811865476, 0.3989422804014327
RB = 128
VMEM_LIMIT = 67_000_000
ROW, LANES, RING = 8, 128, 4
PAD = 25600
COLOR = PAD // 2
PARTS = 2
WIDE, EXTRA = 3072, 128
GCOLS = WIDE + EXTRA
MESH = pl.DeviceIdType.MESH


def dot(a, b, dims=NN):
    return lax.dot_general(a, b, dims, preferred_element_type=F32)


def rnd(v):
    return v.astype(BF16).astype(F32)


def gelu_parts(a):
    phi = 0.5 + 0.5 * lax.erf(a * SQRT_HALF)
    return a * phi, phi + a * jnp.exp2(a * a * (-0.5 * LOG2E)) * INV_SQRT_2PI


def block(i, n):
    return slice(i * n, i * n + n)


def row_sums(v):
    return jnp.sum(v.reshape(v.shape[0] // ROW, ROW, v.shape[1]), axis=0)


def wcol(half, part, width):
    return slice(half * WIDE + part, half * WIDE + part + width)


def look_up_kernel(codes_ref, table_ref, peer_ref, own_ref, table, sem):
    step = pl.program_id(0)
    half = pl.num_programs(0) * S

    @pl.when(step == 0)
    def _():
        tiles = table_ref.shape[0]
        load = pltpu.make_async_copy(table_ref, table.at[:tiles], sem)
        load.start()
        table[tiles] = jnp.zeros((ROW, D), BF16)
        load.wait()
    sub = lax.broadcasted_iota(jnp.int32, (ROW, D), 0)

    def look_up(first):
        got = jnp.zeros((ROW, D), F32)
        for j in range(ROW):
            at = codes_ref[first + j]
            got = jnp.where(sub == j, pltpu.roll(table[at >> 3].astype(F32), at & (ROW - 1), 0), got)
        return got

    for k, dst in enumerate((own_ref, peer_ref)):
        @pl.loop(0, S // ROW, unroll=2)
        def _(g):
            t0 = pl.multiple_of(g * ROW, ROW)
            dst[0, pl.ds(t0, ROW), :] = look_up(k * half + step * S + t0).astype(dst.dtype)


def look_up_call(codes, table):
    seqs = codes.size // (2 * S)
    seq = pl.BlockSpec((1, S, D), lambda i, _: (i, 0, 0))
    return pl.pallas_call(
        look_up_kernel,
        grid_spec=pltpu.PrefetchScalarGridSpec(
            num_scalar_prefetch=1, grid=(seqs,), in_specs=[pl.BlockSpec(memory_space=pl.ANY)], out_specs=[seq] * 2,
            scratch_shapes=[pltpu.VMEM((table.shape[0] + 1, ROW, D), BF16), pltpu.SemaphoreType.DMA]),
        out_shape=[jax.ShapeDtypeStruct((seqs, S, D), t) for t in (F32, BF16)],
        compiler_params=pltpu.CompilerParams(dimension_semantics=("arbitrary",), vmem_limit_bytes=VMEM_LIMIT),
        cost_estimate=pl.CostEstimate(flops=40_000_000_000, bytes_accessed=40_000_000, transcendentals=0),
        name="look_up",
    )(codes, table)


def layer_kernel(xo_ref, cot_ref, g1_ref, b1_ref, g2_ref, b2_ref, bd_ref, bf_ref, bo_ref, bp_ref, rope_ref, xs_ref, ids_ref, qo_ref, do_ref, fo_ref, to_ref, rp_ref, fp_ref,
                 out_ref, rows_ref, xin_ref, idz_ref, gw_out, gs_out, gb1_out,
                 gw_ref, gs_ref, gb1_ref, wqkv, wd, w1, w2, n_scr, acc_scr, dh2_scr, dh1_scr, inv_scr, h1_scr, h2_scr, h1t_scr, h2t_scr, cott_scr, dctx_scr, ctx_scr,
                 qkv_scr, dqkv_scr, s_scr, dp_scr, pb_scr, ds_scr, a_scr, du_scr, u_scr, da_scr, dk_scr, dv_scr,
                 xp_buf, gx_buf, out_buf, peer_buf, own_low, peer_low, x_send, x_recv, x_load, id_send, id_recv, gx_send, gx_recv, gx_local, out_send, out_recv, own_sem, peer_sem, init_sem):
    step, last = pl.program_id(0), pl.num_programs(0) - 1
    slot = step % 2
    core, chip = lax.axis_index('tp'), lax.axis_index('dp')
    chips = lax.axis_size('dp')
    plane = chips // RING
    z, peer = chip // plane, (1 - core, chip)

    def z_device(k):
        return (core, (chip + k * plane) % chips)

    def x_copy(at):
        return pltpu.make_async_remote_copy(xs_ref.at[at], xin_ref.at[at], x_send.at[at], x_recv.at[at], device_id=peer, device_id_type=MESH)

    def x_take(at):
        return pltpu.make_async_copy(xin_ref.at[at], xp_buf.at[at % 2], x_load.at[at % 2])

    def id_copy(k):
        if k:
            return pltpu.make_async_remote_copy(ids_ref, idz_ref.at[k], id_send.at[k], id_recv.at[k], device_id=z_device(k), device_id_type=MESH)
        return pltpu.make_async_copy(ids_ref, idz_ref.at[k], id_send.at[k])

    @pl.when(step == 0)
    def _():
        barrier = pltpu.get_barrier_semaphore()
        near = [peer] + [z_device(k) for k in range(1, RING)]
        for who in near:
            pl.semaphore_signal(barrier, inc=1, device_id=who, device_id_type=MESH)
        pl.semaphore_wait(barrier, len(near))

        @pl.loop(0, last + 1)
        def _(at):
            x_copy(at).start()
        for k in range(RING):
            id_copy(k).start()
        for dst in (gw_ref, gs_ref, gb1_ref):
            dst[...] = jnp.zeros_like(dst)
        n = FF // 2
        moves = [(qo_ref.at[block(j, HALF)], wqkv.at[block(2 * j, HALF)]) for j in range(QKV)]
        moves += [(do_ref, wd.at[:HALF]), (to_ref, w2.at[:n]), (fo_ref, w1.at[:, :n])]
        tables = (n_scr, acc_scr, dh2_scr, dh1_scr, s_scr.at[0], s_scr.at[1])
        parts = [rp_ref.at[block(i, S)] for i in range(RING)] + [fp_ref.at[:, block(i, S)] for i in BOTH]
        copies = [pltpu.make_async_copy(src, dst, init_sem.at[i]) for i, (src, dst) in enumerate(moves + list(zip(parts, tables)))]
        for c in copies:
            c.start()
        for c in copies:
            c.wait()
        for j in range(QKV):
            wqkv[block(2 * j + 1, HALF), :] = tables[j // 2][block(j % 2, HALF), :].astype(BF16)
        wd[HALF:, :] = tables[1][HALF:, :].astype(BF16)
        for i in BOTH:
            w2[block(2 + i, S), :] = tables[2 + i][...].astype(BF16)
            w1[:, block(2 + i, S)] = tables[RING + i][...].astype(BF16)

        x_copy(0).wait_recv()
        x_take(0).start()

    x_take(step).wait()

    @pl.when(step < last)
    def _():
        x_copy(step + 1).wait_recv()
        x_take(step + 1).start()

    def gx_copy(at, k):
        rows = pl.ds(pl.multiple_of(at * S, S), S)
        src, dst = gx_buf.at[at % 2, k], rows_ref.at[k, rows]
        if k:
            return pltpu.make_async_remote_copy(src, dst, gx_send.at[at % 2, k], gx_recv.at[at, k], device_id=z_device(k), device_id_type=MESH)
        return pltpu.make_async_copy(src, dst, gx_local.at[at % 2])

    def out_copy(at):
        return pltpu.make_async_remote_copy(out_buf.at[at % 2], peer_buf.at[at], out_send.at[at % 2], out_recv.at[at], device_id=peer, device_id_type=MESH)

    def own_store(at):
        return pltpu.make_async_copy(own_low.at[at % 2], out_ref.at[core * (last + 1) + at], own_sem.at[at % 2])

    def peer_store(at):
        return pltpu.make_async_copy(peer_low.at[at % 2], out_ref.at[(1 - core) * (last + 1) + at], peer_sem.at[at % 2])

    def drain(at):
        gx_copy(at, 0).wait()
        for k in range(1, RING):
            gx_copy(at, k).wait_send()
        out_copy(at).wait_send()
        own_store(at).wait()

    def take_peer(at):
        out_copy(at).wait_recv()

        @pl.when(at > 1)
        def _():
            peer_store(at - 2).wait()
        peer_low[at % 2] = peer_buf[at].astype(BF16)
        peer_store(at).start()

    @pl.when(step > 1)
    def _():
        drain(step - 2)

    cot = cot_ref[0]
    g1, b1, g2, b2, bd, bf = (v[...].astype(F32).reshape(1, D) for v in (g1_ref, b1_ref, g2_ref, b2_ref, bd_ref, bf_ref))
    bo = bd + bf

    def bias(row, i, n):
        width = HALF if row < 3 else FF // 2
        src, i = (bo_ref, i) if i < width // n else (bp_ref, i - width // n)
        return src[row:row + 1, block(i, n)]

    dctx_scr[...] = dot(cot, wd[...], NT).astype(BF16)
    cott_scr[...] = cot.T
    x = xo_ref[0].astype(F32) + xp_buf[slot]
    cen = x - jnp.mean(x, axis=-1, keepdims=True)
    inv = lax.rsqrt(jnp.mean(cen * cen, axis=-1, keepdims=True) + EPS)
    n = cen * inv
    n_scr[...] = n
    inv_scr[...] = inv
    h1_scr[...] = (n * g1 + b1).astype(BF16)
    h2_scr[...] = (n * g2 + b2).astype(BF16)
    gs_ref[4] += row_sums(cot.astype(F32))
    h1t_scr[...] = h1_scr[...].T
    h2t_scr[...] = h2_scr[...].T
    h1, h2 = h1_scr[...], h2_scr[...]

    for p in range(PAIRS):
        for j in range(QKV):
            v = dot(h1, wqkv[block(j * PAIRS + p, PAIR), :], NT) + bias(j, p, PAIR)
            v = v.astype(BF16)
            if j < 2:
                v = v.astype(F32)
                v = (v * rope_ref[0] + pltpu.roll(v, PAIR - ROT_HALF, 1) * rope_ref[1]
                     + pltpu.roll(v, ROT_HALF, 1) * rope_ref[2]).astype(BF16)
            qkv_scr[j, :, block(p, PAIR)] = v

    lane = lax.broadcasted_iota(jnp.int32, (HALF, PAIR), 1)
    causal = lax.broadcasted_iota(jnp.int32, (HALF, HALF), 0) >= lax.broadcasted_iota(jnp.int32, (HALF, HALF), 1)
    heads = (lane < HD, lane >= HD)
    zero = jnp.zeros((HALF, PAIR), BF16)

    def only(v, hh):
        return jnp.concatenate([jnp.where(heads[hh], v[block(i, HALF)], zero) for i in range(v.shape[0] // HALF)], axis=0)

    def rope_back(g, rows):
        g = rnd(g * HD ** -0.5)
        return (g * rope_ref[0, rows] + pltpu.roll(g * rope_ref[1, rows], ROT_HALF, 1)
                + pltpu.roll(g * rope_ref[2, rows], PAIR - ROT_HALF, 1)).astype(BF16)

    class Attention:
        def __init__(self, i):
            p, self.qb = i // 2, i % 2
            self.n, self.slot, self.lanes, self.rows = HALF * (self.qb + 1), self.qb, block(p, PAIR), block(self.qb, HALF)

        def operands(self):
            q, dc = qkv_scr[0, self.rows, self.lanes], dctx_scr[self.rows, self.lanes]
            return q, dc, qkv_scr[1, :self.n, self.lanes], qkv_scr[2, :self.n, self.lanes]

        def one(self):
            q, dc, k, v = self.operands()
            for hh in BOTH:
                at = (self.slot, block(hh, HALF), slice(self.n))
                s_scr[at] = dot(only(q, hh), k, NT)
                dp_scr[at] = dot(only(dc, hh), v, NT).astype(BF16)

        def two(self):
            for hh in BOTH:
                at = (self.slot, block(hh, HALF), slice(self.n))
                s = s_scr[at]
                diag = jnp.where(causal, s[:, self.n - HALF:], -1e30)
                s = jnp.concatenate([s[:, :HALF], diag], axis=1) if self.qb else diag
                e = jnp.exp2((s - jnp.max(s, axis=-1, keepdims=True)) * (HD ** -0.5 * LOG2E))
                pr = e * (1.0 / jnp.sum(e, axis=-1, keepdims=True))
                pb_scr[at] = pr.astype(BF16)
                dp = dp_scr[at].astype(F32)
                ds_scr[at] = (pr * (dp - jnp.sum(pr * dp, axis=-1, keepdims=True))).astype(BF16)

        def three(self):
            q, dc, k, v = self.operands()
            pb, ds = pb_scr[self.slot, :, :self.n], ds_scr[self.slot, :, :self.n]
            rows, lanes = self.rows, self.lanes
            ctx_scr[rows, lanes] = sum(dot(pb[block(hh, HALF)], only(v, hh)) for hh in BOTH).astype(BF16)
            dqkv_scr[0, rows, lanes] = rope_back(sum(dot(ds[block(hh, HALF)], only(k, hh)) for hh in BOTH), rows)
            dk = dot(ds, jnp.concatenate([only(q, hh) for hh in BOTH], axis=0), TN)
            dv = dot(pb, jnp.concatenate([only(dc, hh) for hh in BOTH], axis=0), TN)
            if not self.qb:
                dk_scr[...] = dk
                dv_scr[...] = dv
                return
            for b in BOTH:
                at = block(b, HALF)
                gk, gv = (dk[at], dv[at]) if b else (dk[at] + dk_scr[...], dv[at] + dv_scr[...])
                dqkv_scr[1, at, lanes] = rope_back(gk, at)
                dqkv_scr[2, at, lanes] = gv.astype(BF16)

    class Mlp:
        def __init__(self, i):
            self.i, self.slot, self.cols = i, i % 2, block(i, HALF)

        def one(self):
            a_scr[self.slot] = dot(h2, w1[:, self.cols]) + bias(3, self.i, HALF)
            du_scr[self.slot] = dot(cot, w2[self.cols, :], NT).astype(BF16)

        def two(self):
            u, gp = gelu_parts(rnd(a_scr[self.slot]))
            da = (du_scr[self.slot].astype(F32) * gp).astype(BF16)
            u_scr[self.slot] = u.astype(BF16)
            da_scr[self.slot] = da
            gb1_ref[:, self.cols] += row_sums(da.astype(F32))

        def three(self):
            u, da = u_scr[self.slot], da_scr[self.slot]
            m, d = dot(u, w2[self.cols, :]), dot(da, w1[:, self.cols], NT)
            acc_scr[...] = acc_scr[...] + m if self.i else m
            dh2_scr[...] = dh2_scr[...] + d if self.i else d
            half, part = self.i // RING, 2 * S + self.i % RING * HALF
            gw_ref[:, wcol(half, part, HALF)] += dot(h2t_scr[...], da)
            gw_ref[:, wcol(half, part + 2 * S, HALF)] += dot(cott_scr[...], u)

    units = [u for i in range(2 * PAIRS) for u in (Attention(i), Mlp(i))]
    units[0].one()
    for i, u in enumerate(units):
        if i + 1 < len(units):
            units[i + 1].one()
        u.two()
        if i:
            units[i - 1].three()
    units[-1].three()

    dh1_scr[...] = sum(dot(dqkv_scr[j], wqkv[block(j, S), :]) for j in range(QKV))
    acc_scr[...] += dot(ctx_scr[...], wd[...])
    for half in BOTH:
        hs = block(half, HALF)
        for j in range(QKV):
            gw_ref[:, wcol(half, j * HALF, HALF)] += dot(h1t_scr[...], dqkv_scr[j, :, hs])
        gw_ref[:, wcol(half, QKV * HALF, HALF)] += dot(cott_scr[...], ctx_scr[:, hs])

    n = n_scr[...]
    d1, d2 = rnd(dh1_scr[...]), rnd(dh2_scr[...])
    for i, v in zip((0, 1, 2, 3, 5, 6, 7), (d1 * n, d1, d2 * n, d2, *(dqkv_scr[j].astype(F32) for j in range(QKV)))):
        gs_ref[i] += row_sums(v)
    gn = d1 * g1 + d2 * g2
    s_scr[0] = cot.astype(F32) + inv_scr[...] * (
        gn - jnp.mean(gn, axis=-1, keepdims=True) - n * jnp.mean(gn * n, axis=-1, keepdims=True))
    low = (xo_ref[0].astype(F32) + xp_buf[slot] + (acc_scr[...] + bo)).astype(BF16)
    own_low[slot] = low
    out_buf[slot] = low.astype(F32)
    for k in range(RING):
        gx_buf[slot, k] = s_scr[0, :, pl.ds(pl.multiple_of((z + k) % RING * LANES, LANES), LANES)]
    for k in (2, 1, 3, 0):
        gx_copy(step, k).start()
    out_copy(step).start()
    own_store(step).start()

    @pl.when(step > 0)
    def _():
        take_peer(step - 1)

    @pl.when(step == last)
    def _():
        save = pltpu.make_async_copy(gw_ref, gw_out, init_sem.at[0])
        save.start()
        gs_out[...] = jnp.sum(gs_ref[...], axis=1)
        gb1_out[...] = jnp.sum(gb1_ref[...], axis=0, keepdims=True)
        take_peer(step)
        for at in (step - 1, step):
            drain(at)
            peer_store(at).wait()

        @pl.loop(0, last + 1)
        def _(at):
            x_copy(at).wait_send()
            for k in range(1, RING):
                gx_copy(at, k).wait_recv()
        save.wait()
        for k in range(RING):
            id_copy(k).wait()


def rope_consts():
    lane = lax.broadcasted_iota(jnp.int32, (S, PAIR), 1) % HD
    inv_freq = ROPE_BASE ** (-(lane % ROT_HALF).astype(F32) / ROT_HALF)
    ang = lax.broadcasted_iota(F32, (S, PAIR), 0) * inv_freq
    sin, low, rot = jnp.sin(ang), lane < ROT_HALF, lane < 2 * ROT_HALF
    return jnp.stack([jnp.where(rot, jnp.cos(ang), 1.0), jnp.where(low, -sin, 0.0), jnp.where(rot & ~low, sin, 0.0)])


def layer_call(*args):
    count = args[0].shape[0]
    vm, hbm = pl.BlockSpec(memory_space=pltpu.VMEM), pl.BlockSpec(memory_space=pl.ANY)
    seq = pl.BlockSpec((1, S, D), lambda i: (i, 0, 0))
    own_seq = pl.BlockSpec((1, S, D), lambda i: (lax.axis_index('tp') * count + i, 0, 0))
    dma = pltpu.SemaphoreType.DMA

    def table(*lead):
        return pltpu.VMEM(lead + (S, D), F32)

    def low(*lead):
        return pltpu.VMEM(lead + (S, D), BF16)
    thin, thin_low, small = pltpu.VMEM((2, S, HALF), F32), pltpu.VMEM((2, S, HALF), BF16), pltpu.VMEM((HALF, PAIR), F32)
    return pl.pallas_call(
        layer_kernel,
        grid=(count,),
        in_specs=[seq, own_seq] + [vm] * 9 + [hbm] * (len(args) - 11),
        out_specs=[hbm] * 5 + [vm] * 2,
        out_shape=[jax.ShapeDtypeStruct((2 * count, S, D), BF16), jax.ShapeDtypeStruct((RING, count * S, LANES), F32), jax.ShapeDtypeStruct((count, S, D), F32), jax.ShapeDtypeStruct((RING, count * S // LANES, LANES), jnp.int32),
                   jax.ShapeDtypeStruct((D, 2 * WIDE), F32), jax.ShapeDtypeStruct((ROW, D), F32), jax.ShapeDtypeStruct((1, FF), F32)],
        scratch_shapes=[pltpu.VMEM((D, 2 * WIDE), F32), pltpu.VMEM((ROW, ROW, D), F32), pltpu.VMEM((ROW, FF), F32), pltpu.VMEM((QKV * S, D), BF16), low(), pltpu.VMEM((D, FF), BF16), pltpu.VMEM((FF, D), BF16)] + [table()] * 4
        + [pltpu.VMEM((S, 1), F32)] + [low()] * 7 + [low(3)] * 2 + [table(2)] + [low(2)] * 3 + [thin] + [thin_low] * 3 + [small] * 2
        + [table(2), pltpu.VMEM((2, RING, S, LANES), F32), table(2), table(count)] + [low(2)] * 2
        + [dma((count,)), dma((count,)), dma((2,)), dma((RING,)), dma((RING,)), dma((2, RING)), dma((count, RING)), dma((2,)), dma((2,)), dma((count,)), dma((2,)), dma((2,)), dma((16,))],
        compiler_params=pltpu.CompilerParams(dimension_semantics=("arbitrary",), collective_id=1, has_side_effects=True,
                                             vmem_limit_bytes=VMEM_LIMIT),
        cost_estimate=pl.CostEstimate(flops=count * 30_000_000_000, bytes_accessed=60_000_000, transcendentals=0),
        name="layer",
    )(*args)


STEPS, UNROLL = 8, 16
STEP = PAD // STEPS


def table_kernel(half, ids_ref, rows_hbm, lo_ref, out_ref, lo_out_ref, rows_ref, acc, acc2, stage, lo_buf, sem, lo_in, lo_sent):
    load = pltpu.make_async_copy(rows_hbm, rows_ref, sem.at[0])
    load.start()

    @pl.loop(0, acc.shape[0] // LANES)
    def _(j):
        for a in (acc, acc2):
            a[pl.ds(pl.multiple_of(j * LANES, LANES), LANES), :] = jnp.zeros((LANES, LANES), F32)
    count, blocks = rows_ref.shape[1], lo_ref.shape[0]
    part = RING // 2 * count // blocks
    per = count // part

    def lo_load(i):
        return pltpu.make_async_copy(lo_ref.at[i], lo_buf.at[i % 2], lo_in.at[i % 2])

    def lo_store(i):
        return pltpu.make_async_copy(lo_buf.at[i % 2], lo_out_ref.at[i], lo_sent.at[i % 2])
    lo_load(0).start()
    load.wait()

    @pl.loop(0, blocks)
    def _(i):
        lo_load(i).wait()
        lo_store(i).start()

        @pl.when(i > 0)
        def _():
            lo_store(i - 1).wait()

        @pl.when(i + 1 < blocks)
        def _():
            lo_load(i + 1).start()
        k, first = i // per * 2, i % per * part

        @pl.loop(0, part // UNROLL)
        def _(g):
            t0 = pl.multiple_of(first + g * UNROLL, UNROLL)
            for j in range(0, UNROLL, 2):
                pairs = []
                for a, src in ((acc, k), (acc2, k + 1)):
                    i0, i1 = (ids_ref[src * count + t0 + j + d] for d in BOTH)
                    x0, x1 = (rows_ref[src, pl.ds(t0 + j + d, 1), :] for d in BOTH)
                    r0, r1 = pl.ds(i0, 1), pl.ds(i1, 1)
                    pairs.append((a, r0, a[r0, :] + x0, r1, a[r1, :] + (x1 + jnp.where(i0 == i1, x0, 0.0))))
                for a, r0, v0, r1, v1 in pairs:
                    a[r0, :] = v0
                    a[r1, :] = v1
    lo_store(blocks - 1).wait()
    copies = []
    for i in range(2 * STEPS):
        h, c, slot = i // STEPS, i % STEPS, i % 2
        if i > 1:
            copies[i - 2].wait()

        @pl.loop(0, STEP // LANES, unroll=5)
        def _(b):
            at = pl.ds(pl.multiple_of(h * half + c * STEP + b * LANES, ROW), LANES)
            stage[slot, :, pl.ds(pl.multiple_of(b * LANES, LANES), LANES)] = (acc[at, :] + acc2[at, :]).T
        copies.append(pltpu.make_async_copy(stage.at[slot], out_ref.at[h, :, pl.ds(c * STEP, STEP)], sem.at[slot]))
        copies[i].start()
    for c in copies[-2:]:
        c.wait()


def table_call(ids, rows, lo, half):
    hbm, dma = pl.BlockSpec(memory_space=pl.ANY), pltpu.SemaphoreType.DMA((2,))
    return pl.pallas_call(
        functools.partial(table_kernel, half),
        grid_spec=pltpu.PrefetchScalarGridSpec(
            num_scalar_prefetch=1, grid=(), in_specs=[hbm] * 2, out_specs=[hbm] * 2,
            scratch_shapes=[pltpu.VMEM(rows.shape, F32)] + [pltpu.VMEM((half + PAD, LANES), F32)] * 2 + [pltpu.VMEM((2, LANES, STEP), F32), pltpu.VMEM((2, S, D), BF16)]
            + [dma] * 3),
        out_shape=[jax.ShapeDtypeStruct((2, LANES, PAD), F32), jax.ShapeDtypeStruct(lo.shape, lo.dtype)],
        compiler_params=pltpu.CompilerParams(vmem_limit_bytes=VMEM_LIMIT),
        cost_estimate=pl.CostEstimate(flops=4_000_000_000, bytes_accessed=34_000_000, transcendentals=0),
        name="table",
    )(ids, rows, lo)


def cut(lo, n):
    first = n // (2 * LANES) * LANES
    return (lo, first), (lo + first, n - first)


def over(lead, body, at=()):
    if not lead:
        return body(at)

    @pl.loop(0, lead[0])
    def _(i):
        over(lead[1:], body, at + (i,))


def add_into(dst, srcs, lead, lo, n):
    def body(at):
        v = dst[at + (slice(None), pl.ds(lo, n))]
        for s in srcs:
            v = v + s[at + (slice(None), pl.ds(0, n))]
        dst[at + (slice(None), pl.ds(lo, n))] = v
    over(lead, body)


def tail_kernel(t_ref, g_ref, e_ref, oute_ref, outw_ref, *scratch):
    tsum, tpeer, gsum, gpeer, send, recv, local = scratch[:7]
    bufs = list(scratch[7:])
    core, dp = lax.axis_index('tp'), lax.axis_index('dp')
    pos = {'z': dp // (RING * RING), 'y': dp // RING % RING, 'x': dp % RING}
    stride = {'z': RING * RING, 'y': RING, 'x': 1}

    def shift(axis, k):
        return (pos[axis] + k) % RING

    def device(axis, k):
        return (core, dp + (shift(axis, k) - pos[axis]) * stride[axis])
    peer = (1 - core, dp)

    barrier = pltpu.get_barrier_semaphore()
    near = [peer] + [device(axis, k) for axis in 'zyx' for k in (1, RING - 1)]
    for who in near:
        pl.semaphore_signal(barrier, inc=1, device_id=who, device_id_type=MESH)
    pl.semaphore_wait(barrier, len(near))

    used = [0, 0]

    def remote(src, dst, who):
        i = used[0]
        used[0] += 1
        c = pltpu.make_async_remote_copy(src, dst, send.at[i], recv.at[i], device_id=who, device_id_type=MESH)
        c.start()
        return c

    def load(src, dst):
        i = used[1]
        used[1] += 1
        c = pltpu.make_async_copy(src, dst, local.at[i])
        c.start()
        return c
    sent = []

    wide, extra, far = pl.ds(0, WIDE), pl.ds(WIDE, EXTRA), pl.ds(WIDE, WIDE)
    every = slice(None)
    py, px, pz = pos['y'], pos['x'], pos['z']
    width = COLOR // PARTS
    flows = {}
    for q in range(PARTS):
        for axis, lo in (('y', q * width), ('x', COLOR + q * width)):
            flows[lo] = axis
    pend = {}

    def piece(axis, i):
        return (i,) if axis in 'yz' else (every, i)

    def fetch(lo, k):
        axis = flows[lo]
        at = piece(axis, shift(axis, k)) + (every,) * (2 if axis == 'y' else 1) + (pl.ds(lo, width),)
        pend[lo, k] = [remote(t_ref.at[(1,) + at], tpeer.at[at], peer), load(t_ref.at[(0,) + at], tsum.at[at])]

    def fetch_g(k):
        i = shift('z', k)
        pend['g', k] = [remote(g_ref.at[i, every, every, every, far], gpeer.at[i, every, every, every, wide], peer),
                        load(g_ref.at[i, every, every, every, wide], gsum.at[i, every, every, every, wide])]
    order = list(flows)
    for k in (2, 1, RING - 1, 0):
        for n, lo in enumerate(order):
            fetch(lo, k)
            if n == 1:
                if k == 2:
                    pend['e'] = [remote(e_ref.at[1], gpeer.at[every, every, every, every, extra], peer),
                                 load(e_ref.at[0], gsum.at[every, every, every, every, extra])]
                fetch_g(k)

    def arrive(key):
        out, here = pend[key]
        sent.append(out)
        out.wait_recv()
        here.wait()

    def ready(name, k):
        arrive((name, k))
        if name == 'g':
            i = shift('z', k)
            add_into(gsum.at[i], [gpeer.at[i]], (RING, RING), 0, GCOLS)
            return
        axis = flows[name]
        at = piece(axis, shift(axis, k))
        v = at + (every,) * (2 if axis == 'y' else 1) + (pl.ds(name, width),)
        add_into(tsum.at[at], [tpeer.at[v]], (RING,), name, width)

    class Stage:
        def __init__(self, axis, piece, lead, lo, n, need=None):
            self.axis, self.piece, self.lead, self.lo, self.n, self.need = axis, piece, lead, lo, n, need
            self.halves = cut(lo, n)
            self.near = [bufs.pop(0), bufs.pop(0)]
            self.last = [bufs.pop(0), bufs.pop(0)]

        def view(self, k, lo, n):
            return self.piece(shift(self.axis, k)).at[(every,) * (len(self.lead) + 1) + (pl.ds(lo, n),)]

        def want(self, k):
            if self.need is not None:
                ready(self.need, k)

        def first(self):
            self.want(2)
            self.c1 = [remote(self.view(2, *self.halves[s]), self.near[s], device(self.axis, k))
                       for s, k in enumerate((1, RING - 1))]

        def second(self):
            self.want(1)
            self.want(RING - 1)
            self.c2 = []
            for s, k in enumerate((1, RING - 1)):
                self.c1[s].wait_recv()
                add_into(self.piece(shift(self.axis, k)), [self.near[s]], self.lead, *self.halves[s])
                self.c2.append(remote(self.view(k, self.lo, self.n), self.last[s], device(self.axis, k)))

        def finish(self):
            self.want(0)
            for c in self.c2:
                c.wait_recv()
            add_into(self.piece(shift(self.axis, 0)), self.last, self.lead, self.lo, self.n)
            sent.extend(self.c1 + self.c2)

    one, two = (RING,), (RING, RING)
    rows_y, rows_x = (lambda i: tsum.at[i]), (lambda i: tsum.at[:, i])
    last_x, last_y = (lambda i: tsum.at[py, i]), (lambda i: tsum.at[i, px])
    first = [Stage(axis, rows_y if axis == 'y' else rows_x, one, lo, width, lo) for lo, axis in flows.items()]
    g1 = Stage('z', lambda i: gsum.at[i], two, 0, GCOLS, 'g')
    second = [Stage('x' if axis == 'y' else 'y', last_x if axis == 'y' else last_y, (), lo, width) for lo, axis in flows.items()]
    (c0, cn), (d0, dn) = cut(0, GCOLS)
    c1 = Stage('y', lambda i: gsum.at[pz, i], one, c0, cn)
    d1 = Stage('x', lambda i: gsum.at[pz, :, i], one, d0, dn)
    c2 = Stage('x', lambda i: gsum.at[pz, py, i], (), c0, cn)
    d2 = Stage('y', lambda i: gsum.at[pz, i, px], (), d0, dn)

    firsts = first[:2] + [g1] + first[2:]
    after = dict(zip(first, ([s] for s in second)))
    after[g1] = [c1, d1]
    for s in firsts:
        if s is g1:
            arrive('e')
        s.first()
    for s in firsts:
        s.second()
    for s in firsts:
        s.finish()
        for t in after[s]:
            t.first()
    nexts = [t for s in firsts for t in after[s]]
    for s in nexts:
        s.second()
    for s, t in ((c1, c2), (d1, d2)):
        s.finish()
        t.first()
    for s in second:
        s.finish()
    oute_ref[...] = tsum[py, px, :, 0:oute_ref.shape[1]]
    for s in (c2, d2):
        s.second()
    for s in (c2, d2):
        s.finish()
    outw_ref[...] = gsum[pz, py, px]
    for c in sent:
        c.wait_send()


def tail_call(t, g, e, rows):
    def ring_bufs(lead, n):
        (_, p), (_, q) = cut(0, n)
        return [pltpu.VMEM(lead + (ROW, w), F32) for w in (p, q, n, n)]
    (_, cn), (_, dn) = cut(0, GCOLS)
    one, two, three = (RING,), (RING,) * 2, (RING,) * 3
    width = COLOR // PARTS
    bufs = sum((ring_bufs(*b) for b in [(one, width)] * (2 * PARTS) + [(two, GCOLS)] + [((), width)] * (2 * PARTS)
                + [(one, cn), (one, dn), ((), cn), ((), dn)]), [])
    dma = pltpu.SemaphoreType.DMA
    hbm = pl.BlockSpec(memory_space=pl.ANY)
    vm = pl.BlockSpec(memory_space=pltpu.VMEM)
    return pl.pallas_call(
        tail_kernel,
        in_specs=[hbm] * 3, out_specs=[vm] * 2,
        out_shape=[jax.ShapeDtypeStruct((ROW, rows), F32), jax.ShapeDtypeStruct((ROW, GCOLS), F32)],
        scratch_shapes=[pltpu.VMEM(two + (ROW, PAD), F32)] * 2 + [pltpu.VMEM(three + (ROW, GCOLS), F32)] * 2
        + [dma((128,)), dma((128,)), dma((32,))] + bufs,
        compiler_params=pltpu.CompilerParams(collective_id=0, has_side_effects=True, vmem_limit_bytes=VMEM_LIMIT),
        name="tail",
    )(t, g, e)


def finish_kernel(e_ref, w_ref, oe, o1, o2, oq, od, *small):
    oe[...] = e_ref[...]
    wide = RING * HALF
    for dst, at in ((o1, wide), (o2, 2 * wide)):
        dst[...] = w_ref[:, at:at + wide]
    for h in range(RING):
        for j in range(QKV):
            oq[:, j, h, :] = w_ref[:, j * HALF + h * HD:j * HALF + (h + 1) * HD]
        od[h] = w_ref[:, block(QKV * RING + h, HD)]
    at = WIDE
    for dst in small:
        n = dst.shape[0]
        dst[...] = w_ref[0, at:at + n]
        at += n


def finish_call(e, w, small):
    shape = jax.ShapeDtypeStruct
    vm = pl.BlockSpec(memory_space=pltpu.VMEM)
    outs = [shape(e.shape, F32)] + [shape((ROW, RING * HALF), F32)] * 2 + [shape((ROW, QKV, RING, HD), F32), shape((RING, ROW, HD), F32)]
    outs += [shape((n,), F32) for n in small]
    return pl.pallas_call(finish_kernel, in_specs=[vm] * 2, out_specs=[vm] * len(outs), out_shape=outs, name="finish")(e, w)


def solution(mesh):
    tp, dp, no = 'tp', 'dp', None
    one, vec_dp, both = P(no), P(dp), P((tp, dp))
    arg_specs = (P(dp, no), P(tp, no), one, one, one, one, P(no, tp, no, no), P(tp, no, no), P(tp, no, no), one, P(no, tp), P(tp), P(tp, no), one, P(dp, no, no))
    out_specs = (P(dp, no, no), P(tp, dp), vec_dp, vec_dp, vec_dp, vec_dp, P(dp, tp, no, no), both, P(tp, no, dp), vec_dp, P(dp, tp), both, P(tp, dp), vec_dp)
    chips = mesh.shape[dp]

    def swap(v):
        return lax.ppermute(v, tp, [(0, 1), (1, 0)])

    def device_step(token_ids, embed_table, ln1_gain, ln1_bias, ln2_gain, ln2_bias, w_qkv, b_qkv, w_dense, b_dense, w_fc1, b_fc1, w_fc2, b_fc2, cotangent):
        core = lax.axis_index(tp)
        vocab_local = embed_table.shape[0]
        seqs = token_ids.shape[0] // 2
        f = lambda v: v.astype(F32)

        wq_own = w_qkv.transpose(2, 1, 3, 0).reshape(QKV * HALF, D)
        wd_own = w_dense.reshape(HALF, D)
        rows_peer = swap(f(jnp.concatenate([wq_own, wd_own, w_fc2], axis=0)))
        fc1_peer = swap(f(w_fc1))
        wide = FF // 2
        bias = f(jnp.concatenate([jnp.pad(b_qkv.transpose(1, 0, 2).reshape(3, HALF), ((0, 0), (0, wide - HALF))), b_fc1.reshape(1, wide)], axis=0))
        bias_peer = swap(bias)

        tokens = jnp.where(core == 0, token_ids, jnp.roll(token_ids, seqs, axis=0)).reshape(-1)
        local = tokens - core * vocab_local
        row = jnp.where((local >= 0) & (local < vocab_local), local, vocab_local)
        codes = (row & -ROW) | ((lax.iota(jnp.int32, tokens.size) - row) & (ROW - 1))
        x_send, x_own = look_up_call(codes, embed_table.reshape(-1, ROW, D))
        ids = jnp.where(local < 0, local + 2 * vocab_local, local)[:seqs * S].reshape(-1, LANES)

        args = (x_own, cotangent, ln1_gain, ln1_bias, ln2_gain, ln2_bias, b_dense, b_fc2, bias, bias_peer, rope_consts(), x_send, ids, wq_own, wd_own, w_fc1, w_fc2, rows_peer, fc1_peer)
        layer_out, rows, _, ids, grad_w, small, grad_b1 = layer_call(*args)

        dense, layer_out = table_call(ids.reshape(-1), rows, layer_out, vocab_local)

        norms = small[:5].reshape(5, chips, ROW).transpose(1, 0, 2).reshape(chips, 5 * ROW)
        norms = jnp.concatenate([norms, norms[:, -ROW:]], axis=1)
        grad_bq = small[5:].reshape(3, 2, PAIRS, HD).transpose(1, 2, 0, 3).reshape(2, chips, -1)
        grad_bf = grad_b1.reshape(2, chips, -1)
        extra = jnp.concatenate([jnp.stack([norms, norms]), grad_bq, grad_bf], axis=2)
        extra = jnp.pad(extra[:, :, None, :], ((0, 0), (0, 0), (0, ROW - 1), (0, EXTRA - extra.shape[2])))
        ring3 = (RING,) * 3
        sum_embed, total = tail_call(dense.reshape(2, RING, RING, ROW, PAD), grad_w.reshape(ring3 + (ROW, 2 * WIDE)),
                                     extra.reshape((2,) + ring3 + (ROW, EXTRA)), vocab_local)
        small = [ROW] * 6 + [grad_bq.shape[2], grad_bf.shape[2]]
        sum_embed, sum_wfc1, sum_wfc2, sum_wqkv, sum_wdense, n1g, n1b, n2g, n2b, bias, bias2, bq, bf1 = finish_call(sum_embed, total, small)
        return (layer_out, sum_embed.T, n1g, n1b, n2g, n2b, sum_wqkv.transpose(0, 2, 1, 3), bq, sum_wdense.transpose(0, 2, 1), bias, sum_wfc1,
                bf1, sum_wfc2.T, bias2)

    return jax.shard_map(device_step, mesh=mesh, in_specs=arg_specs, out_specs=out_specs, check_vma=False)
```

```python
import functools
import math
import jax
import jax.numpy as jnp
from jax import lax
from jax.experimental import pallas as pl
from jax.experimental.pallas import tpu as pltpu
from jax.sharding import PartitionSpec as P

F32, BF16 = jnp.float32, jnp.bfloat16
NN = (((1,), (0,)), ((), ()))
NT = (((1,), (1,)), ((), ()))
TN = (((0,), (0,)), ((), ()))
S, D, FF, HEADS, HD = 512, 512, 2048, 8, 64
PAIR, HALF, PAIRS, FF_STEPS, ROT_HALF = 2 * HD, S // 2, HEADS // 2, FF // S, HD // 8
QKV, BOTH = 3, range(2)
EPS, ROPE_BASE = 1e-5, 10000.0
LOG2E = 1.4426950408889634
SQRT_HALF, INV_SQRT_2PI = 0.7071067811865476, 0.3989422804014327
RB = 128
VMEM_LIMIT = 67_000_000
ROW, LANES, RING = 8, 128, 4
PAD = 25600
COLOR = PAD // 2
PARTS = 2
WIDE, EXTRA = 3072, 128
GCOLS = WIDE + EXTRA
MESH = pl.DeviceIdType.MESH


def dot(a, b, dims=NN):
    return lax.dot_general(a, b, dims, preferred_element_type=F32)


def rnd(v):
    return v.astype(BF16).astype(F32)


def gelu_parts(a):
    phi = 0.5 + 0.5 * lax.erf(a * SQRT_HALF)
    return a * phi, phi + a * jnp.exp2(a * a * (-0.5 * LOG2E)) * INV_SQRT_2PI


def block(i, n):
    return slice(i * n, i * n + n)


def row_sums(v):
    return jnp.sum(v.reshape(v.shape[0] // ROW, ROW, v.shape[1]), axis=0)


def wcol(half, part, width):
    return slice(half * WIDE + part, half * WIDE + part + width)


def look_up_kernel(codes_ref, table_ref, peer_ref, own_ref, table, sem):
    step = pl.program_id(0)
    half = pl.num_programs(0) * S

    @pl.when(step == 0)
    def _():
        tiles = table_ref.shape[0]
        load = pltpu.make_async_copy(table_ref, table.at[:tiles], sem)
        load.start()
        table[tiles] = jnp.zeros((ROW, D), BF16)
        load.wait()
    sub = lax.broadcasted_iota(jnp.int32, (ROW, D), 0)

    def look_up(first):
        got = jnp.zeros((ROW, D), F32)
        for j in range(ROW):
            at = codes_ref[first + j]
            got = jnp.where(sub == j, pltpu.roll(table[at >> 3].astype(F32), at & (ROW - 1), 0), got)
        return got

    for k, dst in enumerate((own_ref, peer_ref)):
        @pl.loop(0, S // ROW, unroll=8)
        def _(g):
            t0 = pl.multiple_of(g * ROW, ROW)
            dst[0, pl.ds(t0, ROW), :] = look_up(k * half + step * S + t0).astype(dst.dtype)


def look_up_call(codes, table):
    seqs = codes.size // (2 * S)
    seq = pl.BlockSpec((1, S, D), lambda i, _: (i, 0, 0))
    return pl.pallas_call(
        look_up_kernel,
        grid_spec=pltpu.PrefetchScalarGridSpec(
            num_scalar_prefetch=1, grid=(seqs,), in_specs=[pl.BlockSpec(memory_space=pl.ANY)], out_specs=[seq] * 2,
            scratch_shapes=[pltpu.VMEM((table.shape[0] + 1, ROW, D), BF16), pltpu.SemaphoreType.DMA]),
        out_shape=[jax.ShapeDtypeStruct((seqs, S, D), t) for t in (F32, BF16)],
        compiler_params=pltpu.CompilerParams(dimension_semantics=("arbitrary",), vmem_limit_bytes=VMEM_LIMIT),
        cost_estimate=pl.CostEstimate(flops=40_000_000_000, bytes_accessed=40_000_000, transcendentals=0),
        name="look_up",
    )(codes, table)


def layer_kernel(xo_ref, cot_ref, g1_ref, b1_ref, g2_ref, b2_ref, bd_ref, bf_ref, bo_ref, bp_ref, rope_ref, xs_ref, ids_ref, qo_ref, do_ref, fo_ref, to_ref, rp_ref, fp_ref,
                 out_ref, rows_ref, xin_ref, idz_ref, gw_out, gs_out, gb1_out,
                 gw_ref, gs_ref, gb1_ref, wqkv, wd, w1, w2, n_scr, acc_scr, dh2_scr, dh1_scr, inv_scr, h1_scr, h2_scr, h1t_scr, h2t_scr, cott_scr, dctx_scr, ctx_scr,
                 qkv_scr, dqkv_scr, s_scr, dp_scr, pb_scr, ds_scr, a_scr, du_scr, u_scr, da_scr, dk_scr, dv_scr,
                 xp_buf, gx_buf, out_buf, peer_buf, own_low, peer_low, x_send, x_recv, x_load, id_send, id_recv, gx_send, gx_recv, gx_local, out_send, out_recv, own_sem, peer_sem, init_sem):
    step, last = pl.program_id(0), pl.num_programs(0) - 1
    slot = step % 2
    core, chip = lax.axis_index('tp'), lax.axis_index('dp')
    chips = lax.axis_size('dp')
    plane = chips // RING
    z, peer = chip // plane, (1 - core, chip)

    def z_device(k):
        return (core, (chip + k * plane) % chips)

    def x_copy(at):
        return pltpu.make_async_remote_copy(xs_ref.at[at], xin_ref.at[at], x_send.at[at], x_recv.at[at], device_id=peer, device_id_type=MESH)

    def x_take(at):
        return pltpu.make_async_copy(xin_ref.at[at], xp_buf.at[at % 2], x_load.at[at % 2])

    def id_copy(k):
        if k:
            return pltpu.make_async_remote_copy(ids_ref, idz_ref.at[k], id_send.at[k], id_recv.at[k], device_id=z_device(k), device_id_type=MESH)
        return pltpu.make_async_copy(ids_ref, idz_ref.at[k], id_send.at[k])

    @pl.when(step == 0)
    def _():
        barrier = pltpu.get_barrier_semaphore()
        near = [peer] + [z_device(k) for k in range(1, RING)]
        for who in near:
            pl.semaphore_signal(barrier, inc=1, device_id=who, device_id_type=MESH)
        pl.semaphore_wait(barrier, len(near))

        @pl.loop(0, last + 1)
        def _(at):
            x_copy(at).start()
        for k in range(RING):
            id_copy(k).start()
        for dst in (gw_ref, gs_ref, gb1_ref):
            dst[...] = jnp.zeros_like(dst)
        n = FF // 2
        moves = [(qo_ref.at[block(j, HALF)], wqkv.at[block(2 * j, HALF)]) for j in range(QKV)]
        moves += [(do_ref, wd.at[:HALF]), (to_ref, w2.at[:n]), (fo_ref, w1.at[:, :n])]
        tables = (n_scr, acc_scr, dh2_scr, dh1_scr, s_scr.at[0], s_scr.at[1])
        parts = [rp_ref.at[block(i, S)] for i in range(RING)] + [fp_ref.at[:, block(i, S)] for i in BOTH]
        copies = [pltpu.make_async_copy(src, dst, init_sem.at[i]) for i, (src, dst) in enumerate(moves + list(zip(parts, tables)))]
        for c in copies:
            c.start()
        for c in copies:
            c.wait()
        for j in range(QKV):
            wqkv[block(2 * j + 1, HALF), :] = tables[j // 2][block(j % 2, HALF), :].astype(BF16)
        wd[HALF:, :] = tables[1][HALF:, :].astype(BF16)
        for i in BOTH:
            w2[block(2 + i, S), :] = tables[2 + i][...].astype(BF16)
            w1[:, block(2 + i, S)] = tables[RING + i][...].astype(BF16)

        x_copy(0).wait_recv()
        x_take(0).start()

    x_take(step).wait()

    @pl.when(step < last)
    def _():
        x_copy(step + 1).wait_recv()
        x_take(step + 1).start()

    def gx_copy(at, k):
        rows = pl.ds(pl.multiple_of(at * S, S), S)
        src, dst = gx_buf.at[at % 2, k], rows_ref.at[k, rows]
        if k:
            return pltpu.make_async_remote_copy(src, dst, gx_send.at[at % 2, k], gx_recv.at[at, k], device_id=z_device(k), device_id_type=MESH)
        return pltpu.make_async_copy(src, dst, gx_local.at[at % 2])

    def out_copy(at):
        return pltpu.make_async_remote_copy(out_buf.at[at % 2], peer_buf.at[at], out_send.at[at % 2], out_recv.at[at], device_id=peer, device_id_type=MESH)

    def own_store(at):
        return pltpu.make_async_copy(own_low.at[at % 2], out_ref.at[core * (last + 1) + at], own_sem.at[at % 2])

    def peer_store(at):
        return pltpu.make_async_copy(peer_low.at[at % 2], out_ref.at[(1 - core) * (last + 1) + at], peer_sem.at[at % 2])

    def drain(at):
        gx_copy(at, 0).wait()
        for k in range(1, RING):
            gx_copy(at, k).wait_send()
        out_copy(at).wait_send()
        own_store(at).wait()

    def take_peer(at):
        out_copy(at).wait_recv()

        @pl.when(at > 1)
        def _():
            peer_store(at - 2).wait()
        peer_low[at % 2] = peer_buf[at].astype(BF16)
        peer_store(at).start()

    @pl.when(step > 1)
    def _():
        drain(step - 2)

    cot = cot_ref[0]
    g1, b1, g2, b2, bd, bf = (v[...].astype(F32).reshape(1, D) for v in (g1_ref, b1_ref, g2_ref, b2_ref, bd_ref, bf_ref))
    bo = bd + bf

    def bias(row, i, n):
        width = HALF if row < 3 else FF // 2
        src, i = (bo_ref, i) if i < width // n else (bp_ref, i - width // n)
        return src[row:row + 1, block(i, n)]

    dctx_scr[...] = dot(cot, wd[...], NT).astype(BF16)
    cott_scr[...] = cot.T
    x = xo_ref[0].astype(F32) + xp_buf[slot]
    cen = x - jnp.mean(x, axis=-1, keepdims=True)
    inv = lax.rsqrt(jnp.mean(cen * cen, axis=-1, keepdims=True) + EPS)
    n = cen * inv
    n_scr[...] = n
    inv_scr[...] = inv
    h1_scr[...] = (n * g1 + b1).astype(BF16)
    h2_scr[...] = (n * g2 + b2).astype(BF16)
    gs_ref[4] += row_sums(cot.astype(F32))
    h1t_scr[...] = h1_scr[...].T
    h2t_scr[...] = h2_scr[...].T
    h1, h2 = h1_scr[...], h2_scr[...]

    for p in range(PAIRS):
        for j in range(QKV):
            v = dot(h1, wqkv[block(j * PAIRS + p, PAIR), :], NT) + bias(j, p, PAIR)
            v = v.astype(BF16)
            if j < 2:
                v = v.astype(F32)
                v = (v * rope_ref[0] + pltpu.roll(v, PAIR - ROT_HALF, 1) * rope_ref[1]
                     + pltpu.roll(v, ROT_HALF, 1) * rope_ref[2]).astype(BF16)
            qkv_scr[j, :, block(p, PAIR)] = v

    lane = lax.broadcasted_iota(jnp.int32, (HALF, PAIR), 1)
    causal = lax.broadcasted_iota(jnp.int32, (HALF, HALF), 0) >= lax.broadcasted_iota(jnp.int32, (HALF, HALF), 1)
    heads = (lane < HD, lane >= HD)
    zero = jnp.zeros((HALF, PAIR), BF16)

    def only(v, hh):
        return jnp.concatenate([jnp.where(heads[hh], v[block(i, HALF)], zero) for i in range(v.shape[0] // HALF)], axis=0)

    def rope_back(g, rows):
        g = rnd(g * HD ** -0.5)
        return (g * rope_ref[0, rows] + pltpu.roll(g * rope_ref[1, rows], ROT_HALF, 1)
                + pltpu.roll(g * rope_ref[2, rows], PAIR - ROT_HALF, 1)).astype(BF16)

    class Attention:
        def __init__(self, i):
            p, self.qb = i // 2, i % 2
            self.n, self.slot, self.lanes, self.rows = HALF * (self.qb + 1), self.qb, block(p, PAIR), block(self.qb, HALF)

        def operands(self):
            q, dc = qkv_scr[0, self.rows, self.lanes], dctx_scr[self.rows, self.lanes]
            return q, dc, qkv_scr[1, :self.n, self.lanes], qkv_scr[2, :self.n, self.lanes]

        def one(self):
            q, dc, k, v = self.operands()
            for hh in BOTH:
                at = (self.slot, block(hh, HALF), slice(self.n))
                s_scr[at] = dot(only(q, hh), k, NT)
                dp_scr[at] = dot(only(dc, hh), v, NT).astype(BF16)

        def two(self):
            for hh in BOTH:
                at = (self.slot, block(hh, HALF), slice(self.n))
                s = s_scr[at]
                diag = jnp.where(causal, s[:, self.n - HALF:], -1e30)
                s = jnp.concatenate([s[:, :HALF], diag], axis=1) if self.qb else diag
                e = jnp.exp2((s - jnp.max(s, axis=-1, keepdims=True)) * (HD ** -0.5 * LOG2E))
                pr = e * (1.0 / jnp.sum(e, axis=-1, keepdims=True))
                pb_scr[at] = pr.astype(BF16)
                dp = dp_scr[at].astype(F32)
                ds_scr[at] = (pr * (dp - jnp.sum(pr * dp, axis=-1, keepdims=True))).astype(BF16)

        def three(self):
            q, dc, k, v = self.operands()
            pb, ds = pb_scr[self.slot, :, :self.n], ds_scr[self.slot, :, :self.n]
            rows, lanes = self.rows, self.lanes
            ctx_scr[rows, lanes] = sum(dot(pb[block(hh, HALF)], only(v, hh)) for hh in BOTH).astype(BF16)
            dqkv_scr[0, rows, lanes] = rope_back(sum(dot(ds[block(hh, HALF)], only(k, hh)) for hh in BOTH), rows)
            dk = dot(ds, jnp.concatenate([only(q, hh) for hh in BOTH], axis=0), TN)
            dv = dot(pb, jnp.concatenate([only(dc, hh) for hh in BOTH], axis=0), TN)
            if not self.qb:
                dk_scr[...] = dk
                dv_scr[...] = dv
                return
            for b in BOTH:
                at = block(b, HALF)
                gk, gv = (dk[at], dv[at]) if b else (dk[at] + dk_scr[...], dv[at] + dv_scr[...])
                dqkv_scr[1, at, lanes] = rope_back(gk, at)
                dqkv_scr[2, at, lanes] = gv.astype(BF16)

    class Mlp:
        def __init__(self, i):
            self.i, self.slot, self.cols = i, i % 2, block(i, HALF)

        def one(self):
            a_scr[self.slot] = dot(h2, w1[:, self.cols]) + bias(3, self.i, HALF)
            du_scr[self.slot] = dot(cot, w2[self.cols, :], NT).astype(BF16)

        def two(self):
            u, gp = gelu_parts(rnd(a_scr[self.slot]))
            da = (du_scr[self.slot].astype(F32) * gp).astype(BF16)
            u_scr[self.slot] = u.astype(BF16)
            da_scr[self.slot] = da
            gb1_ref[:, self.cols] += row_sums(da.astype(F32))

        def three(self):
            u, da = u_scr[self.slot], da_scr[self.slot]
            m, d = dot(u, w2[self.cols, :]), dot(da, w1[:, self.cols], NT)
            acc_scr[...] = acc_scr[...] + m if self.i else m
            dh2_scr[...] = dh2_scr[...] + d if self.i else d
            half, part = self.i // RING, 2 * S + self.i % RING * HALF
            gw_ref[:, wcol(half, part, HALF)] += dot(h2t_scr[...], da)
            gw_ref[:, wcol(half, part + 2 * S, HALF)] += dot(cott_scr[...], u)

    units = [u for i in range(2 * PAIRS) for u in (Attention(i), Mlp(i))]
    units[0].one()
    for i, u in enumerate(units):
        if i + 1 < len(units):
            units[i + 1].one()
        u.two()
        if i:
            units[i - 1].three()
    units[-1].three()

    dh1_scr[...] = sum(dot(dqkv_scr[j], wqkv[block(j, S), :]) for j in range(QKV))
    acc_scr[...] += dot(ctx_scr[...], wd[...])
    for half in BOTH:
        hs = block(half, HALF)
        for j in range(QKV):
            gw_ref[:, wcol(half, j * HALF, HALF)] += dot(h1t_scr[...], dqkv_scr[j, :, hs])
        gw_ref[:, wcol(half, QKV * HALF, HALF)] += dot(cott_scr[...], ctx_scr[:, hs])

    n = n_scr[...]
    d1, d2 = rnd(dh1_scr[...]), rnd(dh2_scr[...])
    for i, v in zip((0, 1, 2, 3, 5, 6, 7), (d1 * n, d1, d2 * n, d2, *(dqkv_scr[j].astype(F32) for j in range(QKV)))):
        gs_ref[i] += row_sums(v)
    gn = d1 * g1 + d2 * g2
    s_scr[0] = cot.astype(F32) + inv_scr[...] * (
        gn - jnp.mean(gn, axis=-1, keepdims=True) - n * jnp.mean(gn * n, axis=-1, keepdims=True))
    low = (xo_ref[0].astype(F32) + xp_buf[slot] + (acc_scr[...] + bo)).astype(BF16)
    own_low[slot] = low
    out_buf[slot] = low.astype(F32)
    for k in range(RING):
        gx_buf[slot, k] = s_scr[0, :, pl.ds(pl.multiple_of((z + k) % RING * LANES, LANES), LANES)]
    for k in (2, 1, 3, 0):
        gx_copy(step, k).start()
    out_copy(step).start()
    own_store(step).start()

    @pl.when(step > 0)
    def _():
        take_peer(step - 1)

    @pl.when(step == last)
    def _():
        save = pltpu.make_async_copy(gw_ref, gw_out, init_sem.at[0])
        save.start()
        gs_out[...] = jnp.sum(gs_ref[...], axis=1)
        gb1_out[...] = jnp.sum(gb1_ref[...], axis=0, keepdims=True)
        take_peer(step)
        for at in (step - 1, step):
            drain(at)
            peer_store(at).wait()

        @pl.loop(0, last + 1)
        def _(at):
            x_copy(at).wait_send()
            for k in range(1, RING):
                gx_copy(at, k).wait_recv()
        save.wait()
        for k in range(RING):
            id_copy(k).wait()


def rope_consts():
    lane = lax.broadcasted_iota(jnp.int32, (S, PAIR), 1) % HD
    inv_freq = ROPE_BASE ** (-(lane % ROT_HALF).astype(F32) / ROT_HALF)
    ang = lax.broadcasted_iota(F32, (S, PAIR), 0) * inv_freq
    sin, low, rot = jnp.sin(ang), lane < ROT_HALF, lane < 2 * ROT_HALF
    return jnp.stack([jnp.where(rot, jnp.cos(ang), 1.0), jnp.where(low, -sin, 0.0), jnp.where(rot & ~low, sin, 0.0)])


def layer_call(*args):
    count = args[0].shape[0]
    vm, hbm = pl.BlockSpec(memory_space=pltpu.VMEM), pl.BlockSpec(memory_space=pl.ANY)
    seq = pl.BlockSpec((1, S, D), lambda i: (i, 0, 0))
    own_seq = pl.BlockSpec((1, S, D), lambda i: (lax.axis_index('tp') * count + i, 0, 0))
    dma = pltpu.SemaphoreType.DMA

    def table(*lead):
        return pltpu.VMEM(lead + (S, D), F32)

    def low(*lead):
        return pltpu.VMEM(lead + (S, D), BF16)
    thin, thin_low, small = pltpu.VMEM((2, S, HALF), F32), pltpu.VMEM((2, S, HALF), BF16), pltpu.VMEM((HALF, PAIR), F32)
    return pl.pallas_call(
        layer_kernel,
        grid=(count,),
        in_specs=[seq, own_seq] + [vm] * 9 + [hbm] * (len(args) - 11),
        out_specs=[hbm] * 5 + [vm] * 2,
        out_shape=[jax.ShapeDtypeStruct((2 * count, S, D), BF16), jax.ShapeDtypeStruct((RING, count * S, LANES), F32), jax.ShapeDtypeStruct((count, S, D), F32), jax.ShapeDtypeStruct((RING, count * S // LANES, LANES), jnp.int32),
                   jax.ShapeDtypeStruct((D, 2 * WIDE), F32), jax.ShapeDtypeStruct((ROW, D), F32), jax.ShapeDtypeStruct((1, FF), F32)],
        scratch_shapes=[pltpu.VMEM((D, 2 * WIDE), F32), pltpu.VMEM((ROW, ROW, D), F32), pltpu.VMEM((ROW, FF), F32), pltpu.VMEM((QKV * S, D), BF16), low(), pltpu.VMEM((D, FF), BF16), pltpu.VMEM((FF, D), BF16)] + [table()] * 4
        + [pltpu.VMEM((S, 1), F32)] + [low()] * 7 + [low(3)] * 2 + [table(2)] + [low(2)] * 3 + [thin] + [thin_low] * 3 + [small] * 2
        + [table(2), pltpu.VMEM((2, RING, S, LANES), F32), table(2), table(count)] + [low(2)] * 2
        + [dma((count,)), dma((count,)), dma((2,)), dma((RING,)), dma((RING,)), dma((2, RING)), dma((count, RING)), dma((2,)), dma((2,)), dma((count,)), dma((2,)), dma((2,)), dma((16,))],
        compiler_params=pltpu.CompilerParams(dimension_semantics=("arbitrary",), collective_id=1, has_side_effects=True,
                                             vmem_limit_bytes=VMEM_LIMIT),
        cost_estimate=pl.CostEstimate(flops=count * 30_000_000_000, bytes_accessed=60_000_000, transcendentals=0),
        name="layer",
    )(*args)


STEPS, UNROLL = 8, 32
STEP = PAD // STEPS


def table_kernel(half, ids_ref, rows_hbm, lo_ref, out_ref, lo_out_ref, rows_ref, acc, acc2, stage, lo_buf, sem, lo_in, lo_sent):
    load = pltpu.make_async_copy(rows_hbm, rows_ref, sem.at[0])
    load.start()

    @pl.loop(0, acc.shape[0] // LANES)
    def _(j):
        for a in (acc, acc2):
            a[pl.ds(pl.multiple_of(j * LANES, LANES), LANES), :] = jnp.zeros((LANES, LANES), F32)
    count, blocks = rows_ref.shape[1], lo_ref.shape[0]
    part = RING // 2 * count // blocks
    per = count // part

    def lo_load(i):
        return pltpu.make_async_copy(lo_ref.at[i], lo_buf.at[i % 2], lo_in.at[i % 2])

    def lo_store(i):
        return pltpu.make_async_copy(lo_buf.at[i % 2], lo_out_ref.at[i], lo_sent.at[i % 2])
    lo_load(0).start()
    load.wait()

    @pl.loop(0, blocks)
    def _(i):
        lo_load(i).wait()
        lo_store(i).start()

        @pl.when(i > 0)
        def _():
            lo_store(i - 1).wait()

        @pl.when(i + 1 < blocks)
        def _():
            lo_load(i + 1).start()
        k, first = i // per * 2, i % per * part

        @pl.loop(0, part // UNROLL)
        def _(g):
            t0 = pl.multiple_of(first + g * UNROLL, UNROLL)
            for j in range(0, UNROLL, 2):
                pairs = []
                for a, src in ((acc, k), (acc2, k + 1)):
                    i0, i1 = (ids_ref[src * count + t0 + j + d] for d in BOTH)
                    x0, x1 = (rows_ref[src, pl.ds(t0 + j + d, 1), :] for d in BOTH)
                    r0, r1 = pl.ds(i0, 1), pl.ds(i1, 1)
                    pairs.append((a, r0, a[r0, :] + x0, r1, a[r1, :] + (x1 + jnp.where(i0 == i1, x0, 0.0))))
                for a, r0, v0, r1, v1 in pairs:
                    a[r0, :] = v0
                    a[r1, :] = v1
    lo_store(blocks - 1).wait()
    copies = []
    for i in range(2 * STEPS):
        h, c, slot = i // STEPS, i % STEPS, i % 2
        if i > 1:
            copies[i - 2].wait()

        @pl.loop(0, STEP // LANES, unroll=True)
        def _(b):
            at = pl.ds(pl.multiple_of(h * half + c * STEP + b * LANES, ROW), LANES)
            stage[slot, :, pl.ds(pl.multiple_of(b * LANES, LANES), LANES)] = (acc[at, :] + acc2[at, :]).T
        copies.append(pltpu.make_async_copy(stage.at[slot], out_ref.at[h, :, pl.ds(c * STEP, STEP)], sem.at[slot]))
        copies[i].start()
    for c in copies[-2:]:
        c.wait()


def table_call(ids, rows, lo, half):
    hbm, dma = pl.BlockSpec(memory_space=pl.ANY), pltpu.SemaphoreType.DMA((2,))
    return pl.pallas_call(
        functools.partial(table_kernel, half),
        grid_spec=pltpu.PrefetchScalarGridSpec(
            num_scalar_prefetch=1, grid=(), in_specs=[hbm] * 2, out_specs=[hbm] * 2,
            scratch_shapes=[pltpu.VMEM(rows.shape, F32)] + [pltpu.VMEM((half + PAD, LANES), F32)] * 2 + [pltpu.VMEM((2, LANES, STEP), F32), pltpu.VMEM((2, S, D), BF16)]
            + [dma] * 3),
        out_shape=[jax.ShapeDtypeStruct((2, LANES, PAD), F32), jax.ShapeDtypeStruct(lo.shape, lo.dtype)],
        compiler_params=pltpu.CompilerParams(vmem_limit_bytes=VMEM_LIMIT),
        cost_estimate=pl.CostEstimate(flops=4_000_000_000, bytes_accessed=34_000_000, transcendentals=0),
        name="table",
    )(ids, rows, lo)


def cut(lo, n):
    first = n // (2 * LANES) * LANES
    return (lo, first), (lo + first, n - first)


def over(lead, body, at=()):
    if not lead:
        return body(at)

    @pl.loop(0, lead[0])
    def _(i):
        over(lead[1:], body, at + (i,))


def add_into(dst, srcs, lead, lo, n):
    def body(at):
        v = dst[at + (slice(None), pl.ds(lo, n))]
        for s in srcs:
            v = v + s[at + (slice(None), pl.ds(0, n))]
        dst[at + (slice(None), pl.ds(lo, n))] = v
    over(lead, body)


def tail_kernel(t_ref, g_ref, e_ref, oute_ref, outw_ref, *scratch):
    tsum, tpeer, gsum, gpeer, send, recv, local = scratch[:7]
    bufs = list(scratch[7:])
    core, dp = lax.axis_index('tp'), lax.axis_index('dp')
    pos = {'z': dp // (RING * RING), 'y': dp // RING % RING, 'x': dp % RING}
    stride = {'z': RING * RING, 'y': RING, 'x': 1}

    def shift(axis, k):
        return (pos[axis] + k) % RING

    def device(axis, k):
        return (core, dp + (shift(axis, k) - pos[axis]) * stride[axis])
    peer = (1 - core, dp)

    barrier = pltpu.get_barrier_semaphore()
    near = [peer] + [device(axis, k) for axis in 'zyx' for k in (1, RING - 1)]
    for who in near:
        pl.semaphore_signal(barrier, inc=1, device_id=who, device_id_type=MESH)
    pl.semaphore_wait(barrier, len(near))

    used = [0, 0]

    def remote(src, dst, who):
        i = used[0]
        used[0] += 1
        c = pltpu.make_async_remote_copy(src, dst, send.at[i], recv.at[i], device_id=who, device_id_type=MESH)
        c.start()
        return c

    def load(src, dst):
        i = used[1]
        used[1] += 1
        c = pltpu.make_async_copy(src, dst, local.at[i])
        c.start()
        return c
    sent = []

    wide, extra, far = pl.ds(0, WIDE), pl.ds(WIDE, EXTRA), pl.ds(WIDE, WIDE)
    every = slice(None)
    py, px, pz = pos['y'], pos['x'], pos['z']
    width = COLOR // PARTS
    flows = {}
    for q in range(PARTS):
        for axis, lo in (('y', q * width), ('x', COLOR + q * width)):
            flows[lo] = axis
    pend = {}

    def piece(axis, i):
        return (i,) if axis in 'yz' else (every, i)

    def fetch(lo, k):
        axis = flows[lo]
        at = piece(axis, shift(axis, k)) + (every,) * (2 if axis == 'y' else 1) + (pl.ds(lo, width),)
        pend[lo, k] = [remote(t_ref.at[(1,) + at], tpeer.at[at], peer), load(t_ref.at[(0,) + at], tsum.at[at])]

    def fetch_g(k):
        i = shift('z', k)
        pend['g', k] = [remote(g_ref.at[i, every, every, every, far], gpeer.at[i, every, every, every, wide], peer),
                        load(g_ref.at[i, every, every, every, wide], gsum.at[i, every, every, every, wide])]
    order = list(flows)
    for k in (2, 1, RING - 1, 0):
        for n, lo in enumerate(order):
            fetch(lo, k)
            if n == 1:
                if k == 2:
                    pend['e'] = [remote(e_ref.at[1], gpeer.at[every, every, every, every, extra], peer),
                                 load(e_ref.at[0], gsum.at[every, every, every, every, extra])]
                fetch_g(k)

    def arrive(key):
        out, here = pend[key]
        sent.append(out)
        out.wait_recv()
        here.wait()

    def ready(name, k):
        arrive((name, k))
        if name == 'g':
            i = shift('z', k)
            add_into(gsum.at[i], [gpeer.at[i]], (RING, RING), 0, GCOLS)
            return
        axis = flows[name]
        at = piece(axis, shift(axis, k))
        v = at + (every,) * (2 if axis == 'y' else 1) + (pl.ds(name, width),)
        add_into(tsum.at[at], [tpeer.at[v]], (RING,), name, width)

    class Stage:
        def __init__(self, axis, piece, lead, lo, n, need=None):
            self.axis, self.piece, self.lead, self.lo, self.n, self.need = axis, piece, lead, lo, n, need
            self.halves = cut(lo, n)
            self.near = [bufs.pop(0), bufs.pop(0)]
            self.last = [bufs.pop(0), bufs.pop(0)]

        def view(self, k, lo, n):
            return self.piece(shift(self.axis, k)).at[(every,) * (len(self.lead) + 1) + (pl.ds(lo, n),)]

        def want(self, k):
            if self.need is not None:
                ready(self.need, k)

        def first(self):
            self.want(2)
            self.c1 = [remote(self.view(2, *self.halves[s]), self.near[s], device(self.axis, k))
                       for s, k in enumerate((1, RING - 1))]

        def second(self):
            self.want(1)
            self.want(RING - 1)
            self.c2 = []
            for s, k in enumerate((1, RING - 1)):
                self.c1[s].wait_recv()
                add_into(self.piece(shift(self.axis, k)), [self.near[s]], self.lead, *self.halves[s])
                self.c2.append(remote(self.view(k, self.lo, self.n), self.last[s], device(self.axis, k)))

        def finish(self):
            self.want(0)
            for c in self.c2:
                c.wait_recv()
            add_into(self.piece(shift(self.axis, 0)), self.last, self.lead, self.lo, self.n)
            sent.extend(self.c1 + self.c2)

    one, two = (RING,), (RING, RING)
    rows_y, rows_x = (lambda i: tsum.at[i]), (lambda i: tsum.at[:, i])
    last_x, last_y = (lambda i: tsum.at[py, i]), (lambda i: tsum.at[i, px])
    first = [Stage(axis, rows_y if axis == 'y' else rows_x, one, lo, width, lo) for lo, axis in flows.items()]
    g1 = Stage('z', lambda i: gsum.at[i], two, 0, GCOLS, 'g')
    second = [Stage('x' if axis == 'y' else 'y', last_x if axis == 'y' else last_y, (), lo, width) for lo, axis in flows.items()]
    (c0, cn), (d0, dn) = cut(0, GCOLS)
    c1 = Stage('y', lambda i: gsum.at[pz, i], one, c0, cn)
    d1 = Stage('x', lambda i: gsum.at[pz, :, i], one, d0, dn)
    c2 = Stage('x', lambda i: gsum.at[pz, py, i], (), c0, cn)
    d2 = Stage('y', lambda i: gsum.at[pz, i, px], (), d0, dn)

    firsts = first[:2] + [g1] + first[2:]
    after = dict(zip(first, ([s] for s in second)))
    after[g1] = [c1, d1]
    for s in firsts:
        if s is g1:
            arrive('e')
        s.first()
    for s in firsts:
        s.second()
    for s in firsts:
        s.finish()
        for t in after[s]:
            t.first()
    nexts = [t for s in firsts for t in after[s]]
    for s in nexts:
        s.second()
    for s, t in ((c1, c2), (d1, d2)):
        s.finish()
        t.first()
    for s in second:
        s.finish()
    oute_ref[...] = tsum[py, px, :, 0:oute_ref.shape[1]]
    for s in (c2, d2):
        s.second()
    for s in (c2, d2):
        s.finish()
    outw_ref[...] = gsum[pz, py, px]
    for c in sent:
        c.wait_send()


def tail_call(t, g, e, rows):
    def ring_bufs(lead, n):
        (_, p), (_, q) = cut(0, n)
        return [pltpu.VMEM(lead + (ROW, w), F32) for w in (p, q, n, n)]
    (_, cn), (_, dn) = cut(0, GCOLS)
    one, two, three = (RING,), (RING,) * 2, (RING,) * 3
    width = COLOR // PARTS
    bufs = sum((ring_bufs(*b) for b in [(one, width)] * (2 * PARTS) + [(two, GCOLS)] + [((), width)] * (2 * PARTS)
                + [(one, cn), (one, dn), ((), cn), ((), dn)]), [])
    dma = pltpu.SemaphoreType.DMA
    hbm = pl.BlockSpec(memory_space=pl.ANY)
    vm = pl.BlockSpec(memory_space=pltpu.VMEM)
    return pl.pallas_call(
        tail_kernel,
        in_specs=[hbm] * 3, out_specs=[vm] * 2,
        out_shape=[jax.ShapeDtypeStruct((ROW, rows), F32), jax.ShapeDtypeStruct((ROW, GCOLS), F32)],
        scratch_shapes=[pltpu.VMEM(two + (ROW, PAD), F32)] * 2 + [pltpu.VMEM(three + (ROW, GCOLS), F32)] * 2
        + [dma((128,)), dma((128,)), dma((32,))] + bufs,
        compiler_params=pltpu.CompilerParams(collective_id=0, has_side_effects=True, vmem_limit_bytes=VMEM_LIMIT),
        name="tail",
    )(t, g, e)


def finish_kernel(e_ref, w_ref, oe, o1, o2, oq, od, *small):
    oe[...] = e_ref[...]
    wide = RING * HALF
    for dst, at in ((o1, wide), (o2, 2 * wide)):
        dst[...] = w_ref[:, at:at + wide]
    for h in range(RING):
        for j in range(QKV):
            oq[:, j, h, :] = w_ref[:, j * HALF + h * HD:j * HALF + (h + 1) * HD]
        od[h] = w_ref[:, block(QKV * RING + h, HD)]
    at = WIDE
    for dst in small:
        n = dst.shape[0]
        dst[...] = w_ref[0, at:at + n]
        at += n


def finish_call(e, w, small):
    shape = jax.ShapeDtypeStruct
    vm = pl.BlockSpec(memory_space=pltpu.VMEM)
    outs = [shape(e.shape, F32)] + [shape((ROW, RING * HALF), F32)] * 2 + [shape((ROW, QKV, RING, HD), F32), shape((RING, ROW, HD), F32)]
    outs += [shape((n,), F32) for n in small]
    return pl.pallas_call(finish_kernel, in_specs=[vm] * 2, out_specs=[vm] * len(outs), out_shape=outs, name="finish")(e, w)


def solution(mesh):
    tp, dp, no = 'tp', 'dp', None
    one, vec_dp, both = P(no), P(dp), P((tp, dp))
    arg_specs = (P(dp, no), P(tp, no), one, one, one, one, P(no, tp, no, no), P(tp, no, no), P(tp, no, no), one, P(no, tp), P(tp), P(tp, no), one, P(dp, no, no))
    out_specs = (P(dp, no, no), P(tp, dp), vec_dp, vec_dp, vec_dp, vec_dp, P(dp, tp, no, no), both, P(tp, no, dp), vec_dp, P(dp, tp), both, P(tp, dp), vec_dp)
    chips = mesh.shape[dp]

    def swap(v):
        return lax.ppermute(v, tp, [(0, 1), (1, 0)])

    def device_step(token_ids, embed_table, ln1_gain, ln1_bias, ln2_gain, ln2_bias, w_qkv, b_qkv, w_dense, b_dense, w_fc1, b_fc1, w_fc2, b_fc2, cotangent):
        core = lax.axis_index(tp)
        vocab_local = embed_table.shape[0]
        seqs = token_ids.shape[0] // 2
        f = lambda v: v.astype(F32)

        wq_own = w_qkv.transpose(2, 1, 3, 0).reshape(QKV * HALF, D)
        wd_own = w_dense.reshape(HALF, D)
        rows_peer = swap(f(jnp.concatenate([wq_own, wd_own, w_fc2], axis=0)))
        fc1_peer = swap(f(w_fc1))
        wide = FF // 2
        bias = f(jnp.concatenate([jnp.pad(b_qkv.transpose(1, 0, 2).reshape(3, HALF), ((0, 0), (0, wide - HALF))), b_fc1.reshape(1, wide)], axis=0))
        bias_peer = swap(bias)

        tokens = jnp.where(core == 0, token_ids, jnp.roll(token_ids, seqs, axis=0)).reshape(-1)
        local = tokens - core * vocab_local
        row = jnp.where((local >= 0) & (local < vocab_local), local, vocab_local)
        codes = (row & -ROW) | ((lax.iota(jnp.int32, tokens.size) - row) & (ROW - 1))
        x_send, x_own = look_up_call(codes, embed_table.reshape(-1, ROW, D))
        ids = jnp.where(local < 0, local + 2 * vocab_local, local)[:seqs * S].reshape(-1, LANES)

        args = (x_own, cotangent, ln1_gain, ln1_bias, ln2_gain, ln2_bias, b_dense, b_fc2, bias, bias_peer, rope_consts(), x_send, ids, wq_own, wd_own, w_fc1, w_fc2, rows_peer, fc1_peer)
        layer_out, rows, _, ids, grad_w, small, grad_b1 = layer_call(*args)

        dense, layer_out = table_call(ids.reshape(-1), rows, layer_out, vocab_local)

        norms = small[:5].reshape(5, chips, ROW).transpose(1, 0, 2).reshape(chips, 5 * ROW)
        norms = jnp.concatenate([norms, norms[:, -ROW:]], axis=1)
        grad_bq = small[5:].reshape(3, 2, PAIRS, HD).transpose(1, 2, 0, 3).reshape(2, chips, -1)
        grad_bf = grad_b1.reshape(2, chips, -1)
        extra = jnp.concatenate([jnp.stack([norms, norms]), grad_bq, grad_bf], axis=2)
        extra = jnp.pad(extra[:, :, None, :], ((0, 0), (0, 0), (0, ROW - 1), (0, EXTRA - extra.shape[2])))
        ring3 = (RING,) * 3
        sum_embed, total = tail_call(dense.reshape(2, RING, RING, ROW, PAD), grad_w.reshape(ring3 + (ROW, 2 * WIDE)),
                                     extra.reshape((2,) + ring3 + (ROW, EXTRA)), vocab_local)
        small = [ROW] * 6 + [grad_bq.shape[2], grad_bf.shape[2]]
        sum_embed, sum_wfc1, sum_wfc2, sum_wqkv, sum_wdense, n1g, n1b, n2g, n2b, bias, bias2, bq, bf1 = finish_call(sum_embed, total, small)
        return (layer_out, sum_embed.T, n1g, n1b, n2g, n2b, sum_wqkv.transpose(0, 2, 1, 3), bq, sum_wdense.transpose(0, 2, 1), bias, sum_wfc1,
                bf1, sum_wfc2.T, bias2)

    return jax.shard_map(device_step, mesh=mesh, in_specs=arg_specs, out_specs=out_specs, check_vma=False)
```
